16 devices in a mesh: ty: 2 (over z), tx: 8 (over y, x, core).
Axes of the slice: x: 2, y: 2, z: 2, core: 2. Of those that a mesh axis runs over, the one named last changes fastest.
Arguments:
- x_tok: bfloat16 [256, 4096], P('ty', 'tx')
- dy_tok: bfloat16 [256, 4096], P('ty', 'tx')
- ln_gain: float32 [4096], P('tx')
- w_gate: bfloat16 [4096, 16384], P('tx', 'ty')
- w_up: bfloat16 [4096, 16384], P('tx', 'ty')
- w_down: bfloat16 [16384, 4096], P('ty', 'tx')
Outputs:
- output 1: bfloat16 [256, 4096], P('ty', 'tx')
- output 2: bfloat16 [256, 4096], P('ty', 'tx')
- output 3: float32 [4096, 16384], P('tx', 'ty')
- output 4: float32 [4096, 16384], P('tx', 'ty')
- output 5: float32 [16384, 4096], P('ty', 'tx')
- output 6: float32 [4096], P('tx')
All inputs are finite; a program needn't handle non-finite values.
Results may differ from the reference program's by a relative error of at most 0.00184539.
Values are sent between devices in bfloat16 or wider.
A program may use at most 1 GiB of HBM per device.

```python
import jax
import jax.numpy as jnp
from jax import lax

TOKENS = 256
D_MODEL = 4096
D_FF = 16384
LN_EPS = 1e-6


def setup_inputs(seed: int = 0) -> dict:
    key_list = jax.random.split(jax.random.key(seed), 9)
    x_tok = (jax.random.normal(key_list[0], (TOKENS, D_MODEL), jnp.float32)
             + 1.5 * jax.random.normal(key_list[1], (TOKENS, 1), jnp.float32)).astype(jnp.bfloat16)
    dy_tok = jax.random.normal(key_list[2], (TOKENS, D_MODEL), jnp.float32).astype(jnp.bfloat16)
    ln_gain = 1.0 + 0.5 * jax.random.normal(key_list[3], (D_MODEL,), jnp.float32)
    in_scale = D_MODEL ** -0.5
    w_gate = ((jax.random.normal(key_list[4], (D_MODEL, D_FF), jnp.float32)
               + jax.random.normal(key_list[5], (1, D_FF), jnp.float32)) * in_scale).astype(jnp.bfloat16)
    w_up = ((jax.random.normal(key_list[6], (D_MODEL, D_FF), jnp.float32)
             + jax.random.normal(key_list[7], (1, D_FF), jnp.float32)) * in_scale).astype(jnp.bfloat16)
    w_down = (jax.random.normal(key_list[8], (D_FF, D_MODEL), jnp.float32) * D_FF ** -0.5).astype(jnp.bfloat16)
    return {"x_tok": x_tok, "dy_tok": dy_tok, "ln_gain": ln_gain,
            "w_gate": w_gate, "w_up": w_up, "w_down": w_down}


def reference(x_tok, dy_tok, ln_gain, w_gate, w_up, w_down):
    x_float = x_tok.astype(jnp.float32)
    mean_x = jnp.mean(x_float, axis=1, keepdims=True)
    mean_sq = jnp.mean(x_float * x_float, axis=1, keepdims=True)
    inv_std = lax.rsqrt(mean_sq - mean_x * mean_x + LN_EPS)
    x_hat = (x_float - mean_x) * inv_std
    h_norm = (ln_gain * x_hat).astype(jnp.bfloat16)
    gate_pre = jnp.dot(h_norm, w_gate, preferred_element_type=jnp.float32)
    up_pre = jnp.dot(h_norm, w_up, preferred_element_type=jnp.float32)
    gate_sig = jax.nn.sigmoid(gate_pre)
    gate_swish = gate_pre * gate_sig
    act_out = (gate_swish * up_pre).astype(jnp.bfloat16)
    mlp_out = jnp.dot(act_out, w_down, preferred_element_type=jnp.float32)
    y_tok = (x_float + mlp_out).astype(jnp.bfloat16)
    dw_down = jnp.dot(act_out.T, dy_tok, preferred_element_type=jnp.float32)
    d_act = jnp.dot(dy_tok, w_down.T, preferred_element_type=jnp.float32)
    d_gate = (d_act * up_pre * gate_sig * (1.0 + gate_pre * (1.0 - gate_sig))).astype(jnp.bfloat16)
    d_up = (d_act * gate_swish).astype(jnp.bfloat16)
    dw_gate = jnp.dot(h_norm.T, d_gate, preferred_element_type=jnp.float32)
    dw_up = jnp.dot(h_norm.T, d_up, preferred_element_type=jnp.float32)
    d_hnorm = (jnp.dot(d_gate, w_gate.T, preferred_element_type=jnp.float32)
               + jnp.dot(d_up, w_up.T, preferred_element_type=jnp.float32))
    d_gain = jnp.sum(d_hnorm * x_hat, axis=0)
    d_xhat = d_hnorm * ln_gain
    dx_ln = inv_std * (d_xhat - jnp.mean(d_xhat, axis=1, keepdims=True)
                       - x_hat * jnp.mean(d_xhat * x_hat, axis=1, keepdims=True))
    dx_tok = (dy_tok.astype(jnp.float32) + dx_ln).astype(jnp.bfloat16)
    return (y_tok, dx_tok, dw_gate, dw_up, dw_down, d_gain)
```

```python
import functools

import jax
import jax.numpy as jnp
from jax import lax
from jax.experimental import pallas as pl
from jax.experimental.pallas import tpu as pltpu
from jax.sharding import PartitionSpec as P

LN_EPS = 1e-6
MESH = pl.DeviceIdType.MESH
FC = 512
P_SLOTS = 3
D_SLOTS = 4


def contract_rows(left_op, right_op):
    return lax.dot_general(left_op, right_op, (((0,), (0,)), ((), ())), preferred_element_type=jnp.float32)


def contract_cols(left_op, right_op):
    return lax.dot_general(left_op, right_op, (((1,), (1,)), ((), ())), preferred_element_type=jnp.float32)


def mo(value, multiple):
    return pl.multiple_of(value, multiple)


def branch_kernel(d_model, n_steps,
                  x_ref, dy_ref, gain_ref, wg_hbm, wu_hbm, wd_hbm,
                  a_hbm, du_hbm, dv_hbm, h_ref, dya_ref, m_own_ref, m_oth_ref, dh_own_ref, dh_oth_ref, dg_ref, cols_ref,
                  wg, wu, wd, xa, xh, part, dsum, r1, r2, gat, m_acc, dh_acc, st, sb, rb,
                  wsem, zs, zr, ss, sr, bs, br, ds, dr, p1s, p1r, p2s, p2r, g1s, g1r, g2s, g2r, gds, gdr, osem):
    half = FC // 2
    rows = x_ref.shape[0]
    tok = 2 * rows
    q1, q2, q3 = tok // 2, tok // 4, tok // 8

    ty = lax.axis_index("ty")
    t = lax.axis_index("tx")
    c = lax.rem(t, 2)
    xc = lax.rem(lax.div(t, 2), 2)
    yc = lax.div(t, 4)
    me = ty * 8 + t
    dev_c = (ty, t + 1 - 2 * c)
    dev_x = (ty, t + 2 - 4 * xc)
    dev_y = (ty, t + 4 - 8 * yc)
    dev_z = (1 - ty, t)

    def remote(src, dst, ssem, rsem, dev):
        return pltpu.make_async_remote_copy(src_ref=src, dst_ref=dst, send_sem=ssem, recv_sem=rsem,
                                            device_id=dev, device_id_type=MESH)

    def wcopy(k, i):
        cs = pl.ds(mo(i * FC, FC), FC)
        if k == 0:
            return pltpu.make_async_copy(wg_hbm.at[:, cs], wg.at[:, cs], wsem.at[0, i])
        if k == 1:
            return pltpu.make_async_copy(wu_hbm.at[:, cs], wu.at[:, cs], wsem.at[1, i])
        return pltpu.make_async_copy(wd_hbm.at[cs, :], wd.at[cs, :], wsem.at[2, i])

    def start_w(i, carry):
        for k in range(3):
            wcopy(k, i).start()
        return carry

    lax.fori_loop(0, n_steps, start_w, 0)

    barrier = pltpu.get_barrier_semaphore()
    for o in range(1, 16):
        q = lax.rem(me + o, 16)
        pl.semaphore_signal(barrier, inc=1, device_id=(lax.div(q, 8), lax.rem(q, 8)), device_id_type=MESH)
    pl.semaphore_wait(barrier, 15)

    own = pl.ds(mo(ty * rows, rows), rows)
    oth = pl.ds(mo((1 - ty) * rows, rows), rows)

    zx = remote(x_ref, xa.at[own, :], zs.at[0], zr.at[0], dev_z)
    zx.start()
    zdy = remote(dy_ref, dya_ref.at[own, :], zs.at[1], zr.at[1], dev_z)
    zdy.start()

    lane = lax.broadcasted_iota(jnp.int32, (rows, 128), 1)

    def pack_cols(c0, c1):
        both = jnp.where(lane == 0, c0, jnp.where(lane == 1, c1, 0.0))
        return both.T[0:8, :]

    def unpack_cols(packed):
        full = jnp.concatenate([packed, jnp.zeros((rows - 8, 128), jnp.float32)], axis=0).T
        return full[:, 0:1], full[:, 1:2]

    x_own = x_ref[...].astype(jnp.float32)
    st[me] = pack_cols(jnp.sum(x_own, axis=1, keepdims=True), jnp.sum(x_own * x_own, axis=1, keepdims=True))
    for o in range(1, 16):
        q = lax.rem(me + o, 16)
        remote(st.at[me], st.at[me], ss.at[o], sr.at[o], (lax.div(q, 8), lax.rem(q, 8))).start()

    xa[own, :] = x_ref[...]
    dya_ref[own, :] = dy_ref[...]
    for o in range(1, 16):
        q = lax.rem(me + 16 - o, 16)
        d = remote(st.at[me], st.at[q], ss.at[o], sr.at[o], (lax.div(q, 8), lax.rem(q, 8)))
        d.wait_send()
        d.wait_recv()
    zx.wait_send()
    remote(x_ref, xa.at[oth, :], zs.at[0], zr.at[0], dev_z).wait_recv()

    gain = gain_ref[...]
    stat_cols = []
    for k in range(2):
        s = st[8 * k]
        for j in range(1, 8):
            s = s + st[8 * k + j]
        c0, c1 = unpack_cols(s)
        mean = c0 / d_model
        inv = lax.rsqrt(c1 / d_model - mean * mean + LN_EPS)
        rs = slice(k * rows, (k + 1) * rows)
        xhat = (xa[rs, :].astype(jnp.float32) - mean) * inv
        xh[rs, :] = xhat
        h_ref[rs, :] = (gain * xhat).astype(jnp.bfloat16)
        stat_cols.append((mean, inv))
    mean_own = jnp.where(ty == 0, stat_cols[0][0], stat_cols[1][0])
    inv_own = jnp.where(ty == 0, stat_cols[0][1], stat_cols[1][1])
    cols_ref[...] = jnp.where(lane == 0, mean_own, jnp.where(lane == 1, inv_own, 0.0))

    m_acc[...] = jnp.zeros_like(m_acc)
    dh_acc[...] = jnp.zeros_like(dh_acc)
    zdy.wait_send()
    remote(dy_ref, dya_ref.at[oth, :], zs.at[1], zr.at[1], dev_z).wait_recv()

    ca = slice(0, half)
    cb = slice(half, FC)

    def seg(base, size, mult):
        return pl.ds(mo(base, mult), size)

    own_c = seg(c * q1, q1, q1)
    oth_c = seg((1 - c) * q1, q1, q1)
    a_keep = seg(c * q1 + xc * q2, q2, q2)
    a_send = seg(c * q1 + (1 - xc) * q2, q2, q2)
    b_keep = seg(c * q1 + yc * q2, q2, q2)
    b_send = seg(c * q1 + (1 - yc) * q2, q2, q2)
    a_fin = seg(c * q1 + xc * q2 + yc * q3, q3, q3)
    a_fin_n = seg(c * q1 + xc * q2 + (1 - yc) * q3, q3, q3)
    b_fin = seg(c * q1 + yc * q2 + xc * q3, q3, q3)
    b_fin_n = seg(c * q1 + yc * q2 + (1 - xc) * q3, q3, q3)
    r_keep = (seg(yc * q3, q3, q3), seg(xc * q3, q3, q3))
    r_send = (seg((1 - yc) * q3, q3, q3), seg((1 - xc) * q3, q3, q3))
    keep1, send1 = (a_keep, b_keep), (a_send, b_send)
    fin, fin_n = (a_fin, b_fin), (a_fin_n, b_fin_n)
    colw = (ca, cb)
    dev1, dev2 = (dev_x, dev_y), (dev_y, dev_x)

    def gcols(j, r):
        return pl.ds(mo(j * FC + r * half, half), half)

    def d_copy(j):
        return remote(part.at[lax.rem(j, P_SLOTS), :, oth_c, :], dsum.at[lax.rem(j, D_SLOTS)], ds.at[j], dr.at[j], dev_c)

    def p1_copy(j, r):
        return remote(part.at[lax.rem(j, P_SLOTS), :, send1[r], colw[r]], r1.at[j, r], p1s.at[r, j], p1r.at[r, j], dev1[r])

    def p2_copy(j, r):
        return remote(r1.at[j, r, :, r_send[r], :], r2.at[j, r], p2s.at[r, j], p2r.at[r, j], dev2[r])

    def g1_copy(j, r):
        ref = gat.at[:, fin[r], gcols(j, r)]
        return remote(ref, ref, g1s.at[r, j], g1r.at[r, j], dev2[r])

    def g1_in(j, r):
        ref = gat.at[:, fin_n[r], gcols(j, r)]
        return remote(ref, ref, g1s.at[r, j], g1r.at[r, j], dev2[r])

    def g2_copy(j, r):
        ref = gat.at[:, keep1[r], gcols(j, r)]
        return remote(ref, ref, g2s.at[r, j], g2r.at[r, j], dev1[r])

    def g2_in(j, r):
        ref = gat.at[:, send1[r], gcols(j, r)]
        return remote(ref, ref, g2s.at[r, j], g2r.at[r, j], dev1[r])

    def gd_copy(j, side):
        ref = gat.at[:, side, pl.ds(mo(j * FC, FC), FC)]
        return remote(ref, ref, gds.at[j], gdr.at[j], dev_c)

    def out_copy(j, k):
        cs = pl.ds(mo(j * FC, FC), FC)
        dst = (a_hbm, du_hbm, dv_hbm)[k]
        return pltpu.make_async_copy(gat.at[k, :, cs], dst.at[:, cs], osem.at[k, j])

    def step(i, carry):
        @pl.when(jnp.logical_and(i >= P_SLOTS, i < n_steps + P_SLOTS))
        def _():
            j = i - P_SLOTS
            d_copy(j).wait_send()
            for r in range(2):
                p1_copy(j, r).wait_send()

        @pl.when(i < n_steps)
        def _():
            for k in range(3):
                wcopy(k, i).wait()
            cs = pl.ds(mo(i * FC, FC), FC)
            slot = lax.rem(i, P_SLOTS)
            h = h_ref[...]
            part[slot, 0] = jnp.dot(h, wg[:, cs], preferred_element_type=jnp.float32)
            part[slot, 1] = jnp.dot(h, wu[:, cs], preferred_element_type=jnp.float32)
            part[slot, 2] = contract_cols(dya_ref[...], wd[cs, :])
            d_copy(i).start()

        @pl.when(jnp.logical_and(i >= 1, i < n_steps + 1))
        def _():
            j = i - 1
            d_copy(j).wait_recv()
            slot = lax.rem(j, P_SLOTS)
            dslot = lax.rem(j, D_SLOTS)
            for k in range(3):
                part[slot, k, own_c, :] = part[slot, k, own_c, :] + dsum[dslot, k]
            for r in range(2):
                p1_copy(j, r).start()

        @pl.when(jnp.logical_and(i >= 2, i < n_steps + 2))
        def _():
            j = i - 2
            slot = lax.rem(j, P_SLOTS)
            for r in range(2):
                p1_copy(j, r).wait_recv()
                for k in range(3):
                    r1[j, r, k] = r1[j, r, k] + part[slot, k, keep1[r], colw[r]]
                p2_copy(j, r).start()

        @pl.when(jnp.logical_and(i >= 3, i < n_steps + 3))
        def _():
            j = i - 3
            for r in range(2):
                p2_copy(j, r).wait_recv()
                u = r1[j, r, 0, r_keep[r], :] + r2[j, r, 0]
                v = r1[j, r, 1, r_keep[r], :] + r2[j, r, 1]
                da = r1[j, r, 2, r_keep[r], :] + r2[j, r, 2]
                sig = jax.nn.sigmoid(u)
                swish = u * sig
                cs = gcols(j, r)
                gat[0, fin[r], cs] = (swish * v).astype(jnp.bfloat16)
                gat[1, fin[r], cs] = (da * v * sig * (1.0 + u * (1.0 - sig))).astype(jnp.bfloat16)
                gat[2, fin[r], cs] = (da * swish).astype(jnp.bfloat16)
                g1_copy(j, r).start()

        @pl.when(jnp.logical_and(i >= 4, i < n_steps + 4))
        def _():
            j = i - 4
            for r in range(2):
                g1_in(j, r).wait_recv()
                g2_copy(j, r).start()

        @pl.when(jnp.logical_and(i >= 5, i < n_steps + 5))
        def _():
            j = i - 5
            for r in range(2):
                g2_in(j, r).wait_recv()
            gd_copy(j, own_c).start()

        @pl.when(i >= 6)
        def _():
            j = i - 6
            gd_copy(j, oth_c).wait_recv()
            for k in range(3):
                out_copy(j, k).start()
            cs = pl.ds(mo(j * FC, FC), FC)
            m_acc[...] += jnp.dot(gat[0, :, cs], wd[cs, :], preferred_element_type=jnp.float32)
            dh_acc[...] += contract_cols(gat[1, :, cs], wg[:, cs]) + contract_cols(gat[2, :, cs], wu[:, cs])
            for r in range(2):
                p2_copy(j, r).wait_send()
                g1_copy(j, r).wait_send()
                g2_copy(j, r).wait_send()
            gd_copy(j, own_c).wait_send()
        return carry

    lax.fori_loop(0, n_steps + 6, step, 0)

    for k in range(2):
        rs = slice(k * rows, (k + 1) * rows)
        e = dh_acc[rs, :] * gain
        sb[k] = pack_cols(jnp.sum(e, axis=1, keepdims=True), jnp.sum(e * xh[rs, :], axis=1, keepdims=True))
    rb[me] = sb[ty]
    for o in range(1, 16):
        q = lax.rem(me + o, 16)
        remote(sb.at[lax.div(q, 8)], rb.at[me], bs.at[o], br.at[o], (lax.div(q, 8), lax.rem(q, 8))).start()
    dg_ref[...] = jnp.sum(dh_acc[...] * xh[...], axis=0, keepdims=True)
    m_own_ref[...] = m_acc[own, :]
    m_oth_ref[...] = m_acc[oth, :]
    dh_own_ref[...] = dh_acc[own, :]
    dh_oth_ref[...] = dh_acc[oth, :]
    for o in range(1, 16):
        q = lax.rem(me + 16 - o, 16)
        d = remote(sb.at[0], rb.at[q], bs.at[o], br.at[o], (lax.div(q, 8), lax.rem(q, 8)))
        d.wait_send()
        d.wait_recv()
    s = rb[0]
    for j in range(1, 16):
        s = s + rb[j]
    c0, c1 = unpack_cols(s)
    cols_ref[...] = jnp.where(lane == 2, c0 / d_model, jnp.where(lane == 3, c1 / d_model, cols_ref[...]))

    def drain(j, carry):
        for k in range(3):
            out_copy(j, k).wait()
        return carry

    lax.fori_loop(0, n_steps, drain, 0)


def solution(mesh):
    tx_size = mesh.shape["tx"]
    ty_size = mesh.shape["ty"]

    def local_step(x_blk, dy_blk, gain_blk, w_gate_blk, w_up_blk, w_down_blk):
        rows, dl = x_blk.shape
        fl = w_gate_blk.shape[1]
        tok = rows * ty_size
        d_model = dl * tx_size
        n = fl // FC
        half = FC // 2
        f32, bf16 = jnp.float32, jnp.bfloat16
        vm = pl.BlockSpec(memory_space=pltpu.VMEM)
        anyspec = pl.BlockSpec(memory_space=pl.ANY)
        sem = pltpu.SemaphoreType.DMA
        S = jax.ShapeDtypeStruct
        outs = pl.pallas_call(
            functools.partial(branch_kernel, d_model, n),
            out_shape=[S((tok, fl), bf16)] * 3 + [S((tok, dl), bf16)] * 2 + [S((rows, dl), f32)] * 4
            + [S((1, dl), f32), S((rows, 128), f32)],
            in_specs=[vm] * 3 + [anyspec] * 3,
            out_specs=[anyspec] * 3 + [vm] * 8,
            scratch_shapes=[
                pltpu.VMEM((dl, fl), bf16), pltpu.VMEM((dl, fl), bf16), pltpu.VMEM((fl, dl), bf16),
                pltpu.VMEM((tok, dl), bf16), pltpu.VMEM((tok, dl), f32),
                pltpu.VMEM((P_SLOTS, 3, tok, FC), f32),
                pltpu.VMEM((D_SLOTS, 3, tok // 2, FC), f32),
                pltpu.VMEM((n, 2, 3, tok // 4, half), f32),
                pltpu.VMEM((n, 2, 3, tok // 8, half), f32),
                pltpu.VMEM((3, tok, fl), bf16),
                pltpu.VMEM((tok, dl), f32), pltpu.VMEM((tok, dl), f32),
                pltpu.VMEM((16, 8, 128), f32), pltpu.VMEM((2, 8, 128), f32), pltpu.VMEM((16, 8, 128), f32),
                sem((3, n)), sem((2,)), sem((2,)), sem((16,)), sem((16,)), sem((16,)), sem((16,)),
                sem((n,)), sem((n,)), sem((2, n)), sem((2, n)), sem((2, n)), sem((2, n)),
                sem((2, n)), sem((2, n)), sem((2, n)), sem((2, n)), sem((n,)), sem((n,)), sem((3, n)),
            ],
            compiler_params=pltpu.CompilerParams(collective_id=0, has_side_effects=True, vmem_limit_bytes=62 * 1024 * 1024),
            cost_estimate=pl.CostEstimate(flops=12 * tok * dl * fl, bytes_accessed=6 * dl * fl + 6 * tok * fl, transcendentals=0),
        )(x_blk, dy_blk, gain_blk[None, :], w_gate_blk, w_up_blk, w_down_blk)
        (a_all, du_all, dv_all, h_all, dy_all, m_own, m_oth, dh_own, dh_oth, dg, cols) = outs

        swap = [(0, 1), (1, 0)]
        m_in = lax.ppermute(m_oth, "ty", swap)
        dh_in = lax.ppermute(dh_oth, "ty", swap)
        dg_in = lax.ppermute(dg, "ty", swap)
        dw_gate_blk = contract_rows(h_all, du_all)
        dw_up_blk = contract_rows(h_all, dv_all)
        dw_down_blk = contract_rows(a_all, dy_all)

        x_float = x_blk.astype(f32)
        y_blk = (x_float + (m_own + m_in)).astype(bf16)
        mean_x, inv_std, mean_e, mean_ex = cols[:, 0:1], cols[:, 1:2], cols[:, 2:3], cols[:, 3:4]
        x_hat = (x_float - mean_x) * inv_std
        e = (dh_own + dh_in) * gain_blk
        dx_ln = inv_std * (e - mean_e - x_hat * mean_ex)
        dx_blk = (dy_blk.astype(f32) + dx_ln).astype(bf16)
        d_gain_blk = (dg + dg_in)[0]
        return (y_blk, dx_blk, dw_gate_blk, dw_up_blk, dw_down_blk, d_gain_blk)

    return jax.shard_map(
        local_step, mesh=mesh,
        in_specs=(P("ty", "tx"), P("ty", "tx"), P("tx"), P("tx", "ty"), P("tx", "ty"), P("ty", "tx")),
        out_specs=(P("ty", "tx"), P("ty", "tx"), P("tx", "ty"), P("tx", "ty"), P("ty", "tx"), P("tx")),
        check_vma=False)
```

```python
import functools

import jax
import jax.numpy as jnp
from jax import lax
from jax.experimental import pallas as pl
from jax.experimental.pallas import tpu as pltpu
from jax.sharding import PartitionSpec as P

LN_EPS = 1e-6
MESH = pl.DeviceIdType.MESH
FC = 512
OWN_FIRST = 2
P_SLOTS = 4
D_SLOTS = 4
RING = 8


def contract_rows(left_op, right_op):
    return lax.dot_general(left_op, right_op, (((0,), (0,)), ((), ())), preferred_element_type=jnp.float32)


def contract_cols(left_op, right_op):
    return lax.dot_general(left_op, right_op, (((1,), (1,)), ((), ())), preferred_element_type=jnp.float32)


def mo(value, multiple):
    return pl.multiple_of(value, multiple)


def branch_kernel(d_model, n_f,
                  x_ref, dy_ref, gain_ref, wg_hbm, wu_hbm, wd_hbm,
                  a_hbm, du_hbm, dv_hbm, h_ref, dya_ref, y_ref, dx_ref, dg_ref,
                  wg, wu, wd, xh, part, dsum, r1, r2, gat, acc, zin, st, rb, dgs, dgr,
                  wsem, zs, zr, ss, sr, bs, br, ds, dr, p1s, p1r, p2s, p2r, g1s, g1r, g2s, g2r, gds, gdr, osem):
    half = FC // 2
    rows = x_ref.shape[0]
    q1, q2, q3 = rows // 2, rows // 4, rows // 8
    n_units = 2 * n_f
    last_oth = OWN_FIRST + n_f - 1

    ty = lax.axis_index("ty")
    t = lax.axis_index("tx")
    c = lax.rem(t, 2)
    xc = lax.rem(lax.div(t, 2), 2)
    yc = lax.div(t, 4)
    dev_c = (ty, t + 1 - 2 * c)
    dev_x = (ty, t + 2 - 4 * xc)
    dev_y = (ty, t + 4 - 8 * yc)
    dev_z = (1 - ty, t)

    def remote(src, dst, ssem, rsem, dev):
        return pltpu.make_async_remote_copy(src_ref=src, dst_ref=dst, send_sem=ssem, recv_sem=rsem,
                                            device_id=dev, device_id_type=MESH)

    def f_of(j):
        return lax.rem(j + (n_f - OWN_FIRST), n_f)

    def oth_of(j):
        return lax.rem(lax.div(j + (n_f - OWN_FIRST), n_f), 2)

    def base_of(j):
        k = oth_of(j)
        return (ty + k - 2 * ty * k) * rows

    def fcols(j):
        return pl.ds(mo(f_of(j) * FC, FC), FC)

    def trows(j):
        return pl.ds(mo(base_of(j), rows), rows)

    def wcopy(k, i):
        cs = fcols(i)
        if k == 0:
            return pltpu.make_async_copy(wg_hbm.at[:, cs], wg.at[:, cs], wsem.at[0, i])
        if k == 1:
            return pltpu.make_async_copy(wu_hbm.at[:, cs], wu.at[:, cs], wsem.at[1, i])
        return pltpu.make_async_copy(wd_hbm.at[cs, :], wd.at[cs, :], wsem.at[2, i])

    def start_w(i, carry):
        for k in range(3):
            wcopy(k, i).start()
        return carry

    lax.fori_loop(0, n_f, start_w, 0)

    barrier = pltpu.get_barrier_semaphore()
    for o in range(1, 8):
        pl.semaphore_signal(barrier, inc=1, device_id=(ty, lax.rem(t + o, 8)), device_id_type=MESH)
    pl.semaphore_signal(barrier, inc=1, device_id=dev_z, device_id_type=MESH)

    own = pl.ds(mo(ty * rows, rows), rows)
    oth = pl.ds(mo((1 - ty) * rows, rows), rows)
    lane = lax.broadcasted_iota(jnp.int32, (rows, 128), 1)

    def pack_cols(c0, c1):
        both = jnp.where(lane == 0, c0, jnp.where(lane == 1, c1, 0.0))
        return both.T[0:8, :]

    def unpack_cols(packed):
        full = jnp.concatenate([packed, jnp.zeros((rows - 8, 128), jnp.float32)], axis=0).T
        return full[:, 0:1], full[:, 1:2]

    def send_stats(buf, ssem, rsem):
        for o in range(1, 8):
            remote(buf.at[t], buf.at[t], ssem.at[o], rsem.at[o], (ty, lax.rem(t + o, 8))).start()

    def total_stats(buf, ssem, rsem):
        for o in range(1, 8):
            q = lax.rem(t + 8 - o, 8)
            d = remote(buf.at[t], buf.at[q], ssem.at[o], rsem.at[o], (ty, q))
            d.wait_send()
            d.wait_recv()
        s = buf[0]
        for j in range(1, 8):
            s = s + buf[j]
        return unpack_cols(s)

    x_own = x_ref[...].astype(jnp.float32)
    st[t] = pack_cols(jnp.sum(x_own, axis=1, keepdims=True), jnp.sum(x_own * x_own, axis=1, keepdims=True))
    pl.semaphore_wait(barrier, 8)
    send_stats(st, ss, sr)
    zdy = remote(dy_ref, dya_ref.at[own, :], zs.at[0], zr.at[0], dev_z)
    zdy.start()
    dya_ref[own, :] = dy_ref[...]
    acc[...] = jnp.zeros_like(acc)

    gain = gain_ref[...]
    c0, c1 = total_stats(st, ss, sr)
    mean_x = c0 / d_model
    inv_std = lax.rsqrt(c1 / d_model - mean_x * mean_x + LN_EPS)
    xhat = (x_ref[...].astype(jnp.float32) - mean_x) * inv_std
    xh[...] = xhat
    h_ref[own, :] = (gain * xhat).astype(jnp.bfloat16)

    def h_copy(block):
        return remote(h_ref.at[own, :], h_ref.at[block, :], zs.at[1], zr.at[1], dev_z)

    h_copy(own).start()

    def seg(base, size):
        return pl.ds(mo(base, size), size)

    own_c = seg(c * q1, q1)
    oth_c = seg((1 - c) * q1, q1)
    keep1 = (seg(c * q1 + xc * q2, q2), seg(c * q1 + yc * q2, q2))
    send1 = (seg(c * q1 + (1 - xc) * q2, q2), seg(c * q1 + (1 - yc) * q2, q2))
    r_keep = (seg(yc * q3, q3), seg(xc * q3, q3))
    r_send = (seg((1 - yc) * q3, q3), seg((1 - xc) * q3, q3))
    colw = (slice(0, half), slice(half, FC))
    dev1, dev2 = (dev_x, dev_y), (dev_y, dev_x)
    g_c = (c * q1, (1 - c) * q1)
    g_keep1 = (c * q1 + xc * q2, c * q1 + yc * q2)
    g_send1 = (c * q1 + (1 - xc) * q2, c * q1 + (1 - yc) * q2)
    g_fin = (g_keep1[0] + yc * q3, g_keep1[1] + xc * q3)
    g_fin_n = (g_keep1[0] + (1 - yc) * q3, g_keep1[1] + (1 - xc) * q3)

    def gcols(j, r):
        return pl.ds(mo(f_of(j) * FC + r * half, half), half)

    def grows(j, off, size):
        return pl.ds(mo(base_of(j) + off, size), size)

    def ring(j):
        return lax.rem(j, RING)

    def d_copy(j):
        return remote(part.at[lax.rem(j, P_SLOTS), :, oth_c, :], dsum.at[lax.rem(j, D_SLOTS)],
                      ds.at[ring(j)], dr.at[ring(j)], dev_c)

    def p1_copy(j, r):
        return remote(part.at[lax.rem(j, P_SLOTS), :, send1[r], colw[r]], r1.at[j, r],
                      p1s.at[r, ring(j)], p1r.at[r, ring(j)], dev1[r])

    def p2_copy(j, r):
        return remote(r1.at[j, r, :, r_send[r], :], r2.at[j, r], p2s.at[r, ring(j)], p2r.at[r, ring(j)], dev2[r])

    def g1_copy(j, r, off):
        ref = gat.at[:, grows(j, off[r], q3), gcols(j, r)]
        return remote(ref, ref, g1s.at[r, ring(j)], g1r.at[r, ring(j)], dev2[r])

    def g2_copy(j, r, off):
        ref = gat.at[:, grows(j, off[r], q2), gcols(j, r)]
        return remote(ref, ref, g2s.at[r, ring(j)], g2r.at[r, ring(j)], dev1[r])

    def gd_copy(j, off):
        ref = gat.at[:, grows(j, off, q1), fcols(j)]
        return remote(ref, ref, gds.at[ring(j)], gdr.at[ring(j)], dev_c)

    def out_copy(j, k):
        dst = (a_hbm, du_hbm, dv_hbm)[k]
        return pltpu.make_async_copy(gat.at[k, trows(j), fcols(j)], dst.at[trows(j), fcols(j)], osem.at[k, ring(j)])

    z_sum = remote(acc.at[1], zin, zs.at[2], zr.at[2], dev_z)

    def step(i, carry):
        @pl.when(jnp.logical_and(i >= P_SLOTS, i < n_units + P_SLOTS))
        def _():
            j = i - P_SLOTS
            d_copy(j).wait_send()
            for r in range(2):
                p1_copy(j, r).wait_send()

        @pl.when(i < n_f)
        def _():
            for k in range(3):
                wcopy(k, i).wait()

        @pl.when(i == OWN_FIRST)
        def _():
            remote(dy_ref, dya_ref.at[oth, :], zs.at[0], zr.at[0], dev_z).wait_recv()
            h_copy(oth).wait_recv()

        @pl.when(i < n_units)
        def _():
            cs = fcols(i)
            slot = lax.rem(i, P_SLOTS)
            h = h_ref[trows(i), :]
            part[slot, 0] = jnp.dot(h, wg[:, cs], preferred_element_type=jnp.float32)
            part[slot, 1] = jnp.dot(h, wu[:, cs], preferred_element_type=jnp.float32)
            part[slot, 2] = contract_cols(dya_ref[trows(i), :], wd[cs, :])
            d_copy(i).start()

        @pl.when(jnp.logical_and(i >= 1, i < n_units + 1))
        def _():
            j = i - 1
            d_copy(j).wait_recv()
            slot = lax.rem(j, P_SLOTS)
            dslot = lax.rem(j, D_SLOTS)
            for k in range(3):
                part[slot, k, own_c, :] = part[slot, k, own_c, :] + dsum[dslot, k]
            for r in range(2):
                p1_copy(j, r).start()

        @pl.when(jnp.logical_and(i >= 2, i < n_units + 2))
        def _():
            j = i - 2
            slot = lax.rem(j, P_SLOTS)
            for r in range(2):
                p1_copy(j, r).wait_recv()
                for k in range(3):
                    r1[j, r, k] = r1[j, r, k] + part[slot, k, keep1[r], colw[r]]
                p2_copy(j, r).start()

        @pl.when(jnp.logical_and(i >= 3, i < n_units + 3))
        def _():
            j = i - 3
            for r in range(2):
                p2_copy(j, r).wait_recv()
                u = r1[j, r, 0, r_keep[r], :] + r2[j, r, 0]
                v = r1[j, r, 1, r_keep[r], :] + r2[j, r, 1]
                da = r1[j, r, 2, r_keep[r], :] + r2[j, r, 2]
                sig = jax.nn.sigmoid(u)
                swish = u * sig
                cs = gcols(j, r)
                rs = grows(j, g_fin[r], q3)
                gat[0, rs, cs] = (swish * v).astype(jnp.bfloat16)
                gat[1, rs, cs] = (da * v * sig * (1.0 + u * (1.0 - sig))).astype(jnp.bfloat16)
                gat[2, rs, cs] = (da * swish).astype(jnp.bfloat16)
                g1_copy(j, r, g_fin).start()

        @pl.when(jnp.logical_and(i >= 4, i < n_units + 4))
        def _():
            j = i - 4
            for r in range(2):
                g1_copy(j, r, g_fin_n).wait_recv()
                g2_copy(j, r, g_keep1).start()

        @pl.when(jnp.logical_and(i >= 5, i < n_units + 5))
        def _():
            j = i - 5
            for r in range(2):
                g2_copy(j, r, g_send1).wait_recv()
            gd_copy(j, g_c[0]).start()

        @pl.when(i >= 6)
        def _():
            j = i - 6
            gd_copy(j, g_c[1]).wait_recv()

            @pl.when(j >= RING)
            def _():
                for k in range(3):
                    out_copy(j - RING, k).wait()

            for k in range(3):
                out_copy(j, k).start()
            cs = fcols(j)
            rs = trows(j)
            side = oth_of(j)
            acc[side, 0] += jnp.dot(gat[0, rs, cs], wd[cs, :], preferred_element_type=jnp.float32)
            acc[side, 1] += contract_cols(gat[1, rs, cs], wg[:, cs]) + contract_cols(gat[2, rs, cs], wu[:, cs])
            for r in range(2):
                p2_copy(j, r).wait_send()
                g1_copy(j, r, g_fin).wait_send()
                g2_copy(j, r, g_keep1).wait_send()
            gd_copy(j, g_c[0]).wait_send()

            @pl.when(j == last_oth)
            def _():
                z_sum.start()
        return carry

    lax.fori_loop(0, n_units + 6, step, 0)

    z_sum.wait()
    d_hnorm = acc[0, 1] + zin[1]
    e = d_hnorm * gain
    rb[t] = pack_cols(jnp.sum(e, axis=1, keepdims=True), jnp.sum(e * xh[...], axis=1, keepdims=True))
    send_stats(rb, bs, br)
    dgs[...] = jnp.broadcast_to(jnp.sum(d_hnorm * xh[...], axis=0, keepdims=True), dgs.shape)
    z_dg = remote(dgs, dgr, zs.at[3], zr.at[3], dev_z)
    z_dg.start()
    zdy.wait_send()
    h_copy(own).wait_send()
    y_ref[...] = (x_ref[...].astype(jnp.float32) + (acc[0, 0] + zin[0])).astype(jnp.bfloat16)
    c0, c1 = total_stats(rb, bs, br)
    dx_ln = inv_std * (e - c0 / d_model - xh[...] * (c1 / d_model))
    dx_ref[...] = (dy_ref[...].astype(jnp.float32) + dx_ln).astype(jnp.bfloat16)
    z_dg.wait()
    dg_ref[...] = dgs[0:1, :] + dgr[0:1, :]

    def drain(j, carry):
        for k in range(3):
            out_copy(j, k).wait()
        return carry

    lax.fori_loop(n_units - RING, n_units, drain, 0)


def weight_grad_kernel(a_ref, du_ref, dv_ref, h_ref, dy_ref, y_in, dx_in, dg_in,
                       dwg_ref, dwu_ref, dwd_ref, y_ref, dx_ref, dg_ref, h_t):
    @pl.when(pl.program_id(0) == 0)
    def _():
        h_t[...] = h_ref[...].T
        y_ref[...] = y_in[...]
        dx_ref[...] = dx_in[...]
        dg_ref[...] = dg_in[...]

    dwg_ref[...] = jnp.dot(h_t[...], du_ref[...], preferred_element_type=jnp.float32)
    dwu_ref[...] = jnp.dot(h_t[...], dv_ref[...], preferred_element_type=jnp.float32)
    dwd_ref[...] = contract_rows(a_ref[...], dy_ref[...])


def solution(mesh):
    tx_size = mesh.shape["tx"]
    ty_size = mesh.shape["ty"]

    def local_step(x_blk, dy_blk, gain_blk, w_gate_blk, w_up_blk, w_down_blk):
        rows, dl = x_blk.shape
        fl = w_gate_blk.shape[1]
        tok = rows * ty_size
        d_model = dl * tx_size
        n = fl // FC
        half = FC // 2
        f32, bf16 = jnp.float32, jnp.bfloat16
        vm = pl.BlockSpec(memory_space=pltpu.VMEM)
        anyspec = pl.BlockSpec(memory_space=pl.ANY)
        sem = pltpu.SemaphoreType.DMA
        S = jax.ShapeDtypeStruct
        outs = pl.pallas_call(
            functools.partial(branch_kernel, d_model, n),
            out_shape=[S((tok, fl), bf16)] * 3 + [S((tok, dl), bf16)] * 2 + [S((rows, dl), bf16)] * 2 + [S((1, dl), f32)],
            in_specs=[vm] * 3 + [anyspec] * 3,
            out_specs=[anyspec] * 3 + [vm] * 5,
            scratch_shapes=[
                pltpu.VMEM((dl, fl), bf16), pltpu.VMEM((dl, fl), bf16), pltpu.VMEM((fl, dl), bf16),
                pltpu.VMEM((rows, dl), f32),
                pltpu.VMEM((P_SLOTS, 3, rows, FC), f32),
                pltpu.VMEM((D_SLOTS, 3, rows // 2, FC), f32),
                pltpu.VMEM((2 * n, 2, 3, rows // 4, half), f32),
                pltpu.VMEM((2 * n, 2, 3, rows // 8, half), f32),
                pltpu.VMEM((3, tok, fl), bf16),
                pltpu.VMEM((2, 2, rows, dl), f32), pltpu.VMEM((2, rows, dl), f32),
                pltpu.VMEM((8, 8, 128), f32), pltpu.VMEM((8, 8, 128), f32),
                pltpu.VMEM((8, dl), f32), pltpu.VMEM((8, dl), f32),
                sem((3, n)), sem((4,)), sem((4,)), sem((8,)), sem((8,)), sem((8,)), sem((8,)),
                sem((RING,)), sem((RING,)), sem((2, RING)), sem((2, RING)), sem((2, RING)), sem((2, RING)),
                sem((2, RING)), sem((2, RING)), sem((2, RING)), sem((2, RING)), sem((RING,)), sem((RING,)), sem((3, RING)),
            ],
            compiler_params=pltpu.CompilerParams(collective_id=0, has_side_effects=True, vmem_limit_bytes=62 * 1024 * 1024),
            cost_estimate=pl.CostEstimate(flops=12 * tok * dl * fl, bytes_accessed=6 * dl * fl + 6 * tok * fl, transcendentals=0),
        )(x_blk, dy_blk, gain_blk[None, :], w_gate_blk, w_up_blk, w_down_blk)

        kf = 512
        whole = lambda shape: pl.BlockSpec(shape, lambda i: (0, 0))
        cols = pl.BlockSpec((tok, kf), lambda i: (0, i))
        dwg, dwu, dwd, y_blk, dx_blk, dg = pl.pallas_call(
            weight_grad_kernel,
            grid=(fl // kf,),
            out_shape=[S((dl, fl), f32)] * 2 + [S((fl, dl), f32)] + [S((rows, dl), bf16)] * 2 + [S((1, dl), f32)],
            in_specs=[cols] * 3 + [whole((tok, dl))] * 2 + [whole((rows, dl))] * 2 + [whole((1, dl))],
            out_specs=[pl.BlockSpec((dl, kf), lambda i: (0, i))] * 2 + [pl.BlockSpec((kf, dl), lambda i: (i, 0))]
            + [whole((rows, dl))] * 2 + [whole((1, dl))],
            scratch_shapes=[pltpu.VMEM((dl, tok), bf16)],
            compiler_params=pltpu.CompilerParams(dimension_semantics=("arbitrary",), vmem_limit_bytes=48 * 1024 * 1024),
            cost_estimate=pl.CostEstimate(flops=6 * tok * dl * fl, bytes_accessed=12 * dl * fl + 6 * tok * fl, transcendentals=0),
        )(*outs)
        return (y_blk, dx_blk, dwg, dwu, dwd, dg[0])

    return jax.shard_map(
        local_step, mesh=mesh,
        in_specs=(P("ty", "tx"), P("ty", "tx"), P("tx"), P("tx", "ty"), P("tx", "ty"), P("ty", "tx")),
        out_specs=(P("ty", "tx"), P("ty", "tx"), P("tx", "ty"), P("tx", "ty"), P("ty", "tx"), P("tx")),
        check_vma=False)
```

```python
import functools

import jax
import jax.numpy as jnp
from jax import lax
from jax.experimental import pallas as pl
from jax.experimental.pallas import tpu as pltpu
from jax.sharding import PartitionSpec as P

LN_EPS = 1e-6
MESH = pl.DeviceIdType.MESH
FC = 512
OWN_FIRST = 8
LEAD = 6
P_SLOTS = 4
L_SLOTS = LEAD + P_SLOTS
RING = 16
STAGES = (1, 3, 5, 7, 9, 10)
WB = 512
W_SLOTS = 3
VMEM_LIMIT = 62 * 1024 * 1024


def contract_rows(left_op, right_op):
    return lax.dot_general(left_op, right_op, (((0,), (0,)), ((), ())), preferred_element_type=jnp.float32)


def contract_cols(left_op, right_op):
    return lax.dot_general(left_op, right_op, (((1,), (1,)), ((), ())), preferred_element_type=jnp.float32)


def mo(value, multiple):
    return pl.multiple_of(value, multiple)


def branch_kernel(d_model, n_f,
                  x_hbm, dy_hbm, gain_hbm, wg_hbm, wu_hbm, wd_hbm,
                  a_hbm, du_hbm, dv_hbm, h_hbm, dya_hbm, y_hbm, dx_hbm, dg_hbm,
                  x_ref, gain_ref, h_ref, dya_ref, y_ref, dx_ref, dg_ref,
                  wg, wu, wd, xh, part, part_d, dsum, dsum_d, r1, r2, gat, acc, zin, st, rb, dgs, dgr,
                  wsem, isem, zs, zr, ss, sr, bs, br, ds, dr, dds, ddr, p1s, p1r, pds, pdr, p2s, p2r,
                  g1s, g1r, g2s, g2r, gds, gdr, osem, fsem):
    half = FC // 2
    rows = x_ref.shape[0]
    q1, q2, q3 = rows // 2, rows // 4, rows // 8
    n_units = 2 * n_f
    last_oth = OWN_FIRST + n_f - 1

    ty = lax.axis_index("ty")
    t = lax.axis_index("tx")
    c = lax.rem(t, 2)
    xc = lax.rem(lax.div(t, 2), 2)
    yc = lax.div(t, 4)
    dev_c = (ty, t + 1 - 2 * c)
    dev_x = (ty, t + 2 - 4 * xc)
    dev_y = (ty, t + 4 - 8 * yc)
    dev_z = (1 - ty, t)
    own = pl.ds(mo(ty * rows, rows), rows)
    oth = pl.ds(mo((1 - ty) * rows, rows), rows)

    def remote(src, dst, ssem, rsem, dev):
        return pltpu.make_async_remote_copy(src_ref=src, dst_ref=dst, send_sem=ssem, recv_sem=rsem,
                                            device_id=dev, device_id_type=MESH)

    def f_of(j):
        return lax.rem(j + (n_f - OWN_FIRST), n_f)

    def oth_of(j):
        return lax.rem(lax.div(j + (n_f - OWN_FIRST), n_f), 2)

    def base_of(j):
        k = oth_of(j)
        return (ty + k - 2 * ty * k) * rows

    def fcols(j):
        return pl.ds(mo(f_of(j) * FC, FC), FC)

    def trows(j):
        return pl.ds(mo(base_of(j), rows), rows)

    def wcopy(k, i):
        cs = fcols(i)
        if k == 0:
            return pltpu.make_async_copy(wg_hbm.at[:, cs], wg.at[:, cs], wsem.at[0, i])
        if k == 1:
            return pltpu.make_async_copy(wu_hbm.at[:, cs], wu.at[:, cs], wsem.at[1, i])
        return pltpu.make_async_copy(wd_hbm.at[cs, :], wd.at[cs, :], wsem.at[2, i])

    in_dy = pltpu.make_async_copy(dy_hbm, dya_ref.at[own, :], isem.at[0])
    in_x = pltpu.make_async_copy(x_hbm, x_ref, isem.at[1])
    in_gain = pltpu.make_async_copy(gain_hbm, gain_ref, isem.at[2])
    in_x.start()
    in_dy.start()
    in_gain.start()
    for i in range(LEAD):
        wcopy(2, i).start()

    barrier = pltpu.get_barrier_semaphore()
    for o in range(1, 8):
        pl.semaphore_signal(barrier, inc=1, device_id=(ty, lax.rem(t + o, 8)), device_id_type=MESH)
    pl.semaphore_signal(barrier, inc=1, device_id=dev_z, device_id_type=MESH)

    def start_w(i, carry):
        wcopy(0, i).start()
        wcopy(1, i).start()

        @pl.when(i + LEAD < n_f)
        def _():
            wcopy(2, i + LEAD).start()
        return carry

    lax.fori_loop(0, n_f, start_w, 0)

    lane = lax.broadcasted_iota(jnp.int32, (rows, 128), 1)

    def pack_cols(c0, c1):
        both = jnp.where(lane == 0, c0, jnp.where(lane == 1, c1, 0.0))
        return both.T[0:8, :]

    def unpack_cols(packed):
        full = jnp.concatenate([packed, jnp.zeros((rows - 8, 128), jnp.float32)], axis=0).T
        return full[:, 0:1], full[:, 1:2]

    def send_stats(buf, ssem, rsem):
        for o in range(1, 8):
            remote(buf.at[t], buf.at[t], ssem.at[o], rsem.at[o], (ty, lax.rem(t + o, 8))).start()

    def total_stats(buf, ssem, rsem):
        for o in range(1, 8):
            q = lax.rem(t + 8 - o, 8)
            d = remote(buf.at[t], buf.at[q], ssem.at[o], rsem.at[o], (ty, q))
            d.wait_send()
            d.wait_recv()
        s = buf[0]
        for j in range(1, 8):
            s = s + buf[j]
        return unpack_cols(s)

    def seg(base, size):
        return pl.ds(mo(base, size), size)

    own_c = seg(c * q1, q1)
    oth_c = seg((1 - c) * q1, q1)
    keep1 = (seg(c * q1 + xc * q2, q2), seg(c * q1 + yc * q2, q2))
    send1 = (seg(c * q1 + (1 - xc) * q2, q2), seg(c * q1 + (1 - yc) * q2, q2))
    r_keep = (seg(yc * q3, q3), seg(xc * q3, q3))
    r_send = (seg((1 - yc) * q3, q3), seg((1 - xc) * q3, q3))
    colw = (slice(0, half), slice(half, FC))
    dev1, dev2 = (dev_x, dev_y), (dev_y, dev_x)
    g_c = (c * q1, (1 - c) * q1)
    g_keep1 = (c * q1 + xc * q2, c * q1 + yc * q2)
    g_send1 = (c * q1 + (1 - xc) * q2, c * q1 + (1 - yc) * q2)
    g_fin = (g_keep1[0] + yc * q3, g_keep1[1] + xc * q3)
    g_fin_n = (g_keep1[0] + (1 - yc) * q3, g_keep1[1] + (1 - xc) * q3)

    def gcols(j, r):
        return pl.ds(mo(f_of(j) * FC + r * half, half), half)

    def grows(j, off, size):
        return pl.ds(mo(base_of(j) + off, size), size)

    def ring(j):
        return lax.rem(j, RING)

    def d_copy(j):
        slot = lax.rem(j, P_SLOTS)
        return remote(part.at[slot, :, oth_c, :], dsum.at[slot], ds.at[ring(j)], dr.at[ring(j)], dev_c)

    def dd_copy(j):
        slot = lax.rem(j, L_SLOTS)
        return remote(part_d.at[slot, oth_c, :], dsum_d.at[slot], dds.at[ring(j)], ddr.at[ring(j)], dev_c)

    def p1_copy(j, r):
        return remote(part.at[lax.rem(j, P_SLOTS), :, send1[r], colw[r]], r1.at[j, r, 0:2],
                      p1s.at[r, ring(j)], p1r.at[r, ring(j)], dev1[r])

    def pd_copy(j, r):
        return remote(part_d.at[lax.rem(j, L_SLOTS), send1[r], colw[r]], r1.at[j, r, 2],
                      pds.at[r, ring(j)], pdr.at[r, ring(j)], dev1[r])

    def p2_copy(j, r):
        return remote(r1.at[j, r, :, r_send[r], :], r2.at[j, r], p2s.at[r, ring(j)], p2r.at[r, ring(j)], dev2[r])

    def g1_copy(j, r, off):
        ref = gat.at[:, grows(j, off[r], q3), gcols(j, r)]
        return remote(ref, ref, g1s.at[r, ring(j)], g1r.at[r, ring(j)], dev2[r])

    def g2_copy(j, r, off):
        ref = gat.at[:, grows(j, off[r], q2), gcols(j, r)]
        return remote(ref, ref, g2s.at[r, ring(j)], g2r.at[r, ring(j)], dev1[r])

    def gd_copy(j, off):
        ref = gat.at[:, grows(j, off, q1), fcols(j)]
        return remote(ref, ref, gds.at[ring(j)], gdr.at[ring(j)], dev_c)

    def out_copy(j, k):
        dst = (a_hbm, du_hbm, dv_hbm)[k]
        return pltpu.make_async_copy(gat.at[k, trows(j), fcols(j)], dst.at[trows(j), fcols(j)], osem.at[k, ring(j)])

    def da_product(j):
        part_d[lax.rem(j, L_SLOTS)] = contract_cols(dya_ref[trows(j), :], wd[fcols(j), :])
        dd_copy(j).start()

    def da_pair_sum(j):
        dd_copy(j).wait_recv()
        slot = lax.rem(j, L_SLOTS)
        part_d[slot, own_c, :] = part_d[slot, own_c, :] + dsum_d[slot]
        for r in range(2):
            pd_copy(j, r).start()

    in_x.wait()
    x_own = x_ref[...].astype(jnp.float32)
    st[t] = pack_cols(jnp.sum(x_own, axis=1, keepdims=True), jnp.sum(x_own * x_own, axis=1, keepdims=True))
    in_dy.wait()
    in_gain.wait()
    pl.semaphore_wait(barrier, 8)
    send_stats(st, ss, sr)
    zdy = remote(dya_ref.at[own, :], dya_ref.at[own, :], zs.at[0], zr.at[0], dev_z)
    zdy.start()
    for i in range(LEAD):
        wcopy(2, i).wait()
        da_product(i)
    for i in range(LEAD):
        da_pair_sum(i)
    acc[...] = jnp.zeros_like(acc)

    gain = gain_ref[...]
    c0, c1 = total_stats(st, ss, sr)
    mean_x = c0 / d_model
    inv_std = lax.rsqrt(c1 / d_model - mean_x * mean_x + LN_EPS)
    xhat = (x_ref[...].astype(jnp.float32) - mean_x) * inv_std
    xh[...] = xhat
    h_ref[own, :] = (gain * xhat).astype(jnp.bfloat16)

    def h_copy(block):
        return remote(h_ref.at[own, :], h_ref.at[block, :], zs.at[1], zr.at[1], dev_z)

    h_copy(own).start()

    z_sum = remote(acc.at[1], zin, zs.at[2], zr.at[2], dev_z)
    h_out = pltpu.make_async_copy(h_ref, h_hbm, fsem.at[0])
    dya_out = pltpu.make_async_copy(dya_ref, dya_hbm, fsem.at[1])

    def step(i, carry):
        @pl.when(jnp.logical_and(i >= P_SLOTS, i < n_units + P_SLOTS))
        def _():
            j = i - P_SLOTS
            d_copy(j).wait_send()
            dd_copy(j).wait_send()
            for r in range(2):
                p1_copy(j, r).wait_send()
                pd_copy(j, r).wait_send()

        @pl.when(i < n_f)
        def _():
            wcopy(0, i).wait()
            wcopy(1, i).wait()

        @pl.when(i + LEAD < n_f)
        def _():
            wcopy(2, i + LEAD).wait()

        @pl.when(i == OWN_FIRST - LEAD)
        def _():
            remote(dya_ref.at[own, :], dya_ref.at[oth, :], zs.at[0], zr.at[0], dev_z).wait_recv()
            dya_out.start()

        @pl.when(i == OWN_FIRST)
        def _():
            h_copy(oth).wait_recv()
            h_out.start()

        @pl.when(i < n_units)
        def _():
            cs = fcols(i)
            slot = lax.rem(i, P_SLOTS)
            h = h_ref[trows(i), :]
            part[slot, 0] = jnp.dot(h, wg[:, cs], preferred_element_type=jnp.float32)
            part[slot, 1] = jnp.dot(h, wu[:, cs], preferred_element_type=jnp.float32)
            d_copy(i).start()

        @pl.when(i + LEAD < n_units)
        def _():
            da_product(i + LEAD)

        @pl.when(jnp.logical_and(i >= STAGES[0], i < n_units + STAGES[0]))
        def _():
            j = i - STAGES[0]
            d_copy(j).wait_recv()
            slot = lax.rem(j, P_SLOTS)
            for k in range(2):
                part[slot, k, own_c, :] = part[slot, k, own_c, :] + dsum[slot, k]
            for r in range(2):
                p1_copy(j, r).start()

            @pl.when(j + LEAD < n_units)
            def _():
                da_pair_sum(j + LEAD)

        @pl.when(jnp.logical_and(i >= STAGES[1], i < n_units + STAGES[1]))
        def _():
            j = i - STAGES[1]
            slot = lax.rem(j, P_SLOTS)
            for r in range(2):
                pd_copy(j, r).wait_recv()
                p1_copy(j, r).wait_recv()
                for k in range(2):
                    r1[j, r, k] = r1[j, r, k] + part[slot, k, keep1[r], colw[r]]
                r1[j, r, 2] = r1[j, r, 2] + part_d[lax.rem(j, L_SLOTS), keep1[r], colw[r]]
                p2_copy(j, r).start()

        @pl.when(jnp.logical_and(i >= STAGES[2], i < n_units + STAGES[2]))
        def _():
            j = i - STAGES[2]
            for r in range(2):
                p2_copy(j, r).wait_recv()
                u = r1[j, r, 0, r_keep[r], :] + r2[j, r, 0]
                v = r1[j, r, 1, r_keep[r], :] + r2[j, r, 1]
                da = r1[j, r, 2, r_keep[r], :] + r2[j, r, 2]
                sig = jax.nn.sigmoid(u)
                swish = u * sig
                cs = gcols(j, r)
                rs = grows(j, g_fin[r], q3)
                gat[0, rs, cs] = (swish * v).astype(jnp.bfloat16)
                gat[1, rs, cs] = (da * v * sig * (1.0 + u * (1.0 - sig))).astype(jnp.bfloat16)
                gat[2, rs, cs] = (da * swish).astype(jnp.bfloat16)
                g1_copy(j, r, g_fin).start()

        @pl.when(jnp.logical_and(i >= STAGES[3], i < n_units + STAGES[3]))
        def _():
            j = i - STAGES[3]
            for r in range(2):
                g1_copy(j, r, g_fin_n).wait_recv()
                g2_copy(j, r, g_keep1).start()

        @pl.when(jnp.logical_and(i >= STAGES[4], i < n_units + STAGES[4]))
        def _():
            j = i - STAGES[4]
            for r in range(2):
                g2_copy(j, r, g_send1).wait_recv()
            gd_copy(j, g_c[0]).start()

        @pl.when(i >= STAGES[5])
        def _():
            j = i - STAGES[5]
            gd_copy(j, g_c[1]).wait_recv()

            @pl.when(j >= RING)
            def _():
                for k in range(3):
                    out_copy(j - RING, k).wait()

            for k in range(3):
                out_copy(j, k).start()
            cs = fcols(j)
            rs = trows(j)
            side = oth_of(j)
            acc[side, 0] += jnp.dot(gat[0, rs, cs], wd[cs, :], preferred_element_type=jnp.float32)
            acc[side, 1] += contract_cols(gat[1, rs, cs], wg[:, cs]) + contract_cols(gat[2, rs, cs], wu[:, cs])
            for r in range(2):
                p2_copy(j, r).wait_send()
                g1_copy(j, r, g_fin).wait_send()
                g2_copy(j, r, g_keep1).wait_send()
            gd_copy(j, g_c[0]).wait_send()

            @pl.when(j == last_oth)
            def _():
                z_sum.start()
        return carry

    lax.fori_loop(0, n_units + STAGES[5], step, 0)

    z_sum.wait()
    d_hnorm = acc[0, 1] + zin[1]
    e = d_hnorm * gain
    rb[t] = pack_cols(jnp.sum(e, axis=1, keepdims=True), jnp.sum(e * xh[...], axis=1, keepdims=True))
    send_stats(rb, bs, br)
    dgs[...] = jnp.broadcast_to(jnp.sum(d_hnorm * xh[...], axis=0, keepdims=True), dgs.shape)
    z_dg = remote(dgs, dgr, zs.at[3], zr.at[3], dev_z)
    z_dg.start()
    y_ref[...] = (x_ref[...].astype(jnp.float32) + (acc[0, 0] + zin[0])).astype(jnp.bfloat16)
    y_out = pltpu.make_async_copy(y_ref, y_hbm, fsem.at[2])
    y_out.start()
    zdy.wait_send()
    h_copy(own).wait_send()
    h_out.wait()
    dya_out.wait()

    def drain(j, carry):
        for k in range(3):
            out_copy(j, k).wait()
        return carry

    lax.fori_loop(n_units - RING, n_units, drain, 0)
    c0, c1 = total_stats(rb, bs, br)
    dx_ln = inv_std * (e - c0 / d_model - xh[...] * (c1 / d_model))
    dx_ref[...] = (dya_ref[own, :].astype(jnp.float32) + dx_ln).astype(jnp.bfloat16)
    dx_out = pltpu.make_async_copy(dx_ref, dx_hbm, fsem.at[3])
    dx_out.start()
    z_dg.wait()
    dg_ref[...] = dgs[0:1, :] + dgr[0:1, :]
    dg_out = pltpu.make_async_copy(dg_ref, dg_hbm, fsem.at[4])
    dg_out.start()
    y_out.wait()
    dx_out.wait()
    dg_out.wait()


def weight_grad_kernel(a_hbm, du_hbm, dv_hbm, h_hbm, dy_hbm, y_in, dx_in, dg_in,
                       dwg_hbm, dwu_hbm, dwd_hbm, y_hbm, dx_hbm, dg_hbm,
                       h_ref, dy_ref, h_t, y_ref, dx_ref, dg_ref, ins, buf, isem, bsem, ssem):
    n_blocks = a_hbm.shape[1] // WB

    def in_copy(b, k):
        slot = lax.rem(b, W_SLOTS)
        src = (a_hbm, du_hbm, dv_hbm)[k].at[:, pl.ds(mo(b * WB, WB), WB)]
        return pltpu.make_async_copy(src, ins.at[slot, k], isem.at[slot, k])

    def out_copy(b, k):
        cs = pl.ds(mo(b * WB, WB), WB)
        dst = (dwg_hbm.at[:, cs], dwu_hbm.at[:, cs], dwd_hbm.at[cs, :])[k]
        slot = lax.rem(b, W_SLOTS)
        return pltpu.make_async_copy(buf.at[slot, k], dst, bsem.at[slot, k])

    h_in = pltpu.make_async_copy(h_hbm, h_ref, ssem.at[0])
    dy_in = pltpu.make_async_copy(dy_hbm, dy_ref, ssem.at[1])
    small_in = [pltpu.make_async_copy(src, dst, ssem.at[2 + k])
                for k, (src, dst) in enumerate(((y_in, y_ref), (dx_in, dx_ref), (dg_in, dg_ref)))]
    small_out = [pltpu.make_async_copy(src, dst, ssem.at[5 + k])
                 for k, (src, dst) in enumerate(((y_ref, y_hbm), (dx_ref, dx_hbm), (dg_ref, dg_hbm)))]
    h_in.start()
    for k in (1, 2, 0):
        in_copy(0, k).start()
    dy_in.start()
    for b in range(1, W_SLOTS):
        for k in range(3):
            in_copy(b, k).start()
    for d in small_in:
        d.start()
    h_in.wait()
    h_t[...] = h_ref[...].T
    dy_in.wait()

    def block(b, carry):
        slot = lax.rem(b, W_SLOTS)
        for k in range(3):
            src = (1, 2, 0)[k]

            @pl.when(b >= W_SLOTS)
            def _():
                out_copy(b - W_SLOTS, k).wait()

            in_copy(b, src).wait()
            if k < 2:
                buf[slot, k] = jnp.dot(h_t[...], ins[slot, src], preferred_element_type=jnp.float32)
            else:
                buf[slot, k] = contract_rows(ins[slot, src], dy_ref[...])
            out_copy(b, k).start()

            @pl.when(b + W_SLOTS < n_blocks)
            def _():
                in_copy(b + W_SLOTS, src).start()
        return carry

    lax.fori_loop(0, n_blocks, block, 0)
    for d in small_in:
        d.wait()
    for d in small_out:
        d.start()

    def drain(b, carry):
        for k in range(3):
            out_copy(b, k).wait()
        return carry

    lax.fori_loop(n_blocks - W_SLOTS, n_blocks, drain, 0)
    for d in small_out:
        d.wait()


def solution(mesh):
    tx_size = mesh.shape["tx"]
    ty_size = mesh.shape["ty"]

    def local_step(x_blk, dy_blk, gain_blk, w_gate_blk, w_up_blk, w_down_blk):
        rows, dl = x_blk.shape
        fl = w_gate_blk.shape[1]
        tok = rows * ty_size
        d_model = dl * tx_size
        n = fl // FC
        half = FC // 2
        f32, bf16 = jnp.float32, jnp.bfloat16
        anyspec = pl.BlockSpec(memory_space=pl.ANY)
        sem = pltpu.SemaphoreType.DMA
        S = jax.ShapeDtypeStruct
        V = pltpu.VMEM
        small = [((rows, dl), bf16), ((rows, dl), bf16), ((1, dl), f32)]
        outs = pl.pallas_call(
            functools.partial(branch_kernel, d_model, n),
            out_shape=[S((tok, fl), bf16)] * 3 + [S((tok, dl), bf16)] * 2 + [S(*s) for s in small],
            in_specs=[anyspec] * 6,
            out_specs=[anyspec] * 8,
            scratch_shapes=[
                V((rows, dl), bf16), V((1, dl), f32), V((tok, dl), bf16), V((tok, dl), bf16), *[V(*s) for s in small],
                V((dl, fl), bf16), V((dl, fl), bf16), V((fl, dl), bf16),
                V((rows, dl), f32),
                V((P_SLOTS, 2, rows, FC), f32), V((L_SLOTS, rows, FC), f32),
                V((P_SLOTS, 2, rows // 2, FC), f32), V((L_SLOTS, rows // 2, FC), f32),
                V((2 * n, 2, 3, rows // 4, half), f32), V((2 * n, 2, 3, rows // 8, half), f32),
                V((3, tok, fl), bf16),
                V((2, 2, rows, dl), f32), V((2, rows, dl), f32),
                V((8, 8, 128), f32), V((8, 8, 128), f32), V((8, dl), f32), V((8, dl), f32),
                sem((3, n)), sem((3,)), sem((4,)), sem((4,)), sem((8,)), sem((8,)), sem((8,)), sem((8,)),
                sem((RING,)), sem((RING,)), sem((RING,)), sem((RING,)),
                *[sem((2, RING)) for _ in range(10)],
                sem((RING,)), sem((RING,)), sem((3, RING)), sem((5,)),
            ],
            compiler_params=pltpu.CompilerParams(collective_id=0, has_side_effects=True, vmem_limit_bytes=VMEM_LIMIT),
            cost_estimate=pl.CostEstimate(flops=12 * tok * dl * fl, bytes_accessed=6 * dl * fl + 6 * tok * fl, transcendentals=0),
        )(x_blk, dy_blk, gain_blk[None, :], w_gate_blk, w_up_blk, w_down_blk)

        dwg, dwu, dwd, y_blk, dx_blk, dg = pl.pallas_call(
            weight_grad_kernel,
            out_shape=[S((dl, fl), f32)] * 2 + [S((fl, dl), f32)] + [S(*s) for s in small],
            in_specs=[anyspec] * 8,
            out_specs=[anyspec] * 6,
            scratch_shapes=[
                V((tok, dl), bf16), V((tok, dl), bf16), V((dl, tok), bf16), *[V(*s) for s in small],
                V((W_SLOTS, 3, tok, WB), bf16), V((W_SLOTS, 3, dl, WB), f32),
                sem((W_SLOTS, 3)), sem((W_SLOTS, 3)), sem((8,)),
            ],
            compiler_params=pltpu.CompilerParams(vmem_limit_bytes=VMEM_LIMIT),
            cost_estimate=pl.CostEstimate(flops=6 * tok * dl * fl, bytes_accessed=12 * dl * fl + 6 * tok * fl, transcendentals=0),
        )(*outs)
        return (y_blk, dx_blk, dwg, dwu, dwd, dg[0])

    return jax.shard_map(
        local_step, mesh=mesh,
        in_specs=(P("ty", "tx"), P("ty", "tx"), P("tx"), P("tx", "ty"), P("tx", "ty"), P("ty", "tx")),
        out_specs=(P("ty", "tx"), P("ty", "tx"), P("tx", "ty"), P("tx", "ty"), P("ty", "tx"), P("tx")),
        check_vma=False)
```

```python
import functools

import jax
import jax.numpy as jnp
from jax import lax
from jax.experimental import pallas as pl
from jax.experimental.pallas import tpu as pltpu
from jax.sharding import PartitionSpec as P

LN_EPS = 1e-6
MESH = pl.DeviceIdType.MESH
FC = 512
OWN_FIRST = 8
LEAD = 6
P_SLOTS = 4
L_SLOTS = LEAD + P_SLOTS
RING = 16
STAGES = (1, 3, 5, 7, 9, 10)
WB = 512
W_SLOTS = 3
VMEM_LIMIT = 44 * 1024 * 1024


def contract_rows(left_op, right_op):
    return lax.dot_general(left_op, right_op, (((0,), (0,)), ((), ())), preferred_element_type=jnp.float32)


def contract_cols(left_op, right_op):
    return lax.dot_general(left_op, right_op, (((1,), (1,)), ((), ())), preferred_element_type=jnp.float32)


def mo(value, multiple):
    return pl.multiple_of(value, multiple)


def branch_kernel(d_model, n_f,
                  x_hbm, dy_hbm, gain_hbm, wg_hbm, wu_hbm, wd_hbm,
                  gat, h_t, dya_ref, y_ref, dx_ref, dg_ref,
                  x_ref, gain_ref, h_ref,
                  wg, wu, wd, xh, part, part_d, dsum, dsum_d, r1, r2, acc, zin, st, rb, dgs, dgr,
                  wsem, isem, zs, zr, ss, sr, bs, br, ds, dr, dds, ddr, p1s, p1r, pds, pdr, p2s, p2r,
                  g1s, g1r, g2s, g2r, gds, gdr):
    half = FC // 2
    rows = x_ref.shape[0]
    q1, q2, q3 = rows // 2, rows // 4, rows // 8
    n_units = 2 * n_f
    last_oth = OWN_FIRST + n_f - 1

    ty = lax.axis_index("ty")
    t = lax.axis_index("tx")
    c = lax.rem(t, 2)
    xc = lax.rem(lax.div(t, 2), 2)
    yc = lax.div(t, 4)
    dev_c = (ty, t + 1 - 2 * c)
    dev_x = (ty, t + 2 - 4 * xc)
    dev_y = (ty, t + 4 - 8 * yc)
    dev_z = (1 - ty, t)
    own = pl.ds(mo(ty * rows, rows), rows)
    oth = pl.ds(mo((1 - ty) * rows, rows), rows)

    def remote(src, dst, ssem, rsem, dev):
        return pltpu.make_async_remote_copy(src_ref=src, dst_ref=dst, send_sem=ssem, recv_sem=rsem,
                                            device_id=dev, device_id_type=MESH)

    def f_of(j):
        return lax.rem(j + (n_f - OWN_FIRST), n_f)

    def oth_of(j):
        return lax.rem(lax.div(j + (n_f - OWN_FIRST), n_f), 2)

    def base_of(j):
        k = oth_of(j)
        return (ty + k - 2 * ty * k) * rows

    def fcols(j):
        return pl.ds(mo(f_of(j) * FC, FC), FC)

    def trows(j):
        return pl.ds(mo(base_of(j), rows), rows)

    def wcopy(k, i):
        cs = fcols(i)
        if k == 0:
            return pltpu.make_async_copy(wg_hbm.at[:, cs], wg.at[:, cs], wsem.at[0, i])
        if k == 1:
            return pltpu.make_async_copy(wu_hbm.at[:, cs], wu.at[:, cs], wsem.at[1, i])
        return pltpu.make_async_copy(wd_hbm.at[cs, :], wd.at[cs, :], wsem.at[2, i])

    in_dy = pltpu.make_async_copy(dy_hbm, dya_ref.at[own, :], isem.at[0])
    in_x = pltpu.make_async_copy(x_hbm, x_ref, isem.at[1])
    in_gain = pltpu.make_async_copy(gain_hbm, gain_ref, isem.at[2])
    in_x.start()
    in_dy.start()
    in_gain.start()
    for i in range(LEAD):
        wcopy(2, i).start()

    barrier = pltpu.get_barrier_semaphore()
    for o in range(1, 8):
        pl.semaphore_signal(barrier, inc=1, device_id=(ty, lax.rem(t + o, 8)), device_id_type=MESH)
    pl.semaphore_signal(barrier, inc=1, device_id=dev_z, device_id_type=MESH)

    def start_w(i, carry):
        wcopy(0, i).start()
        wcopy(1, i).start()

        @pl.when(i + LEAD < n_f)
        def _():
            wcopy(2, i + LEAD).start()
        return carry

    lax.fori_loop(0, n_f, start_w, 0)

    lane = lax.broadcasted_iota(jnp.int32, (rows, 128), 1)

    def pack_cols(c0, c1):
        both = jnp.where(lane == 0, c0, jnp.where(lane == 1, c1, 0.0))
        return both.T[0:8, :]

    def unpack_cols(packed):
        full = jnp.concatenate([packed, jnp.zeros((rows - 8, 128), jnp.float32)], axis=0).T
        return full[:, 0:1], full[:, 1:2]

    def send_stats(buf, ssem, rsem):
        for o in range(1, 8):
            remote(buf.at[t], buf.at[t], ssem.at[o], rsem.at[o], (ty, lax.rem(t + o, 8))).start()

    def total_stats(buf, ssem, rsem):
        for o in range(1, 8):
            q = lax.rem(t + 8 - o, 8)
            d = remote(buf.at[t], buf.at[q], ssem.at[o], rsem.at[o], (ty, q))
            d.wait_send()
            d.wait_recv()
        s = buf[0]
        for j in range(1, 8):
            s = s + buf[j]
        return unpack_cols(s)

    def seg(base, size):
        return pl.ds(mo(base, size), size)

    own_c = seg(c * q1, q1)
    oth_c = seg((1 - c) * q1, q1)
    keep1 = (seg(c * q1 + xc * q2, q2), seg(c * q1 + yc * q2, q2))
    send1 = (seg(c * q1 + (1 - xc) * q2, q2), seg(c * q1 + (1 - yc) * q2, q2))
    r_keep = (seg(yc * q3, q3), seg(xc * q3, q3))
    r_send = (seg((1 - yc) * q3, q3), seg((1 - xc) * q3, q3))
    colw = (slice(0, half), slice(half, FC))
    dev1, dev2 = (dev_x, dev_y), (dev_y, dev_x)
    g_c = (c * q1, (1 - c) * q1)
    g_keep1 = (c * q1 + xc * q2, c * q1 + yc * q2)
    g_send1 = (c * q1 + (1 - xc) * q2, c * q1 + (1 - yc) * q2)
    g_fin = (g_keep1[0] + yc * q3, g_keep1[1] + xc * q3)
    g_fin_n = (g_keep1[0] + (1 - yc) * q3, g_keep1[1] + (1 - xc) * q3)

    def gcols(j, r):
        return pl.ds(mo(f_of(j) * FC + r * half, half), half)

    def grows(j, off, size):
        return pl.ds(mo(base_of(j) + off, size), size)

    def ring(j):
        return lax.rem(j, RING)

    def d_copy(j):
        slot = lax.rem(j, P_SLOTS)
        return remote(part.at[slot, :, oth_c, :], dsum.at[slot], ds.at[ring(j)], dr.at[ring(j)], dev_c)

    def dd_copy(j):
        slot = lax.rem(j, L_SLOTS)
        return remote(part_d.at[slot, oth_c, :], dsum_d.at[slot], dds.at[ring(j)], ddr.at[ring(j)], dev_c)

    def p1_copy(j, r):
        return remote(part.at[lax.rem(j, P_SLOTS), :, send1[r], colw[r]], r1.at[j, r, 0:2],
                      p1s.at[r, ring(j)], p1r.at[r, ring(j)], dev1[r])

    def pd_copy(j, r):
        return remote(part_d.at[lax.rem(j, L_SLOTS), send1[r], colw[r]], r1.at[j, r, 2],
                      pds.at[r, ring(j)], pdr.at[r, ring(j)], dev1[r])

    def p2_copy(j, r):
        return remote(r1.at[j, r, :, r_send[r], :], r2.at[j, r], p2s.at[r, ring(j)], p2r.at[r, ring(j)], dev2[r])

    def g1_copy(j, r, off):
        ref = gat.at[:, grows(j, off[r], q3), gcols(j, r)]
        return remote(ref, ref, g1s.at[r, ring(j)], g1r.at[r, ring(j)], dev2[r])

    def g2_copy(j, r, off):
        ref = gat.at[:, grows(j, off[r], q2), gcols(j, r)]
        return remote(ref, ref, g2s.at[r, ring(j)], g2r.at[r, ring(j)], dev1[r])

    def gd_copy(j, off):
        ref = gat.at[:, grows(j, off, q1), fcols(j)]
        return remote(ref, ref, gds.at[ring(j)], gdr.at[ring(j)], dev_c)

    def da_product(j):
        part_d[lax.rem(j, L_SLOTS)] = contract_cols(dya_ref[trows(j), :], wd[fcols(j), :])
        dd_copy(j).start()

    def da_pair_sum(j):
        dd_copy(j).wait_recv()
        slot = lax.rem(j, L_SLOTS)
        part_d[slot, own_c, :] = part_d[slot, own_c, :] + dsum_d[slot]
        for r in range(2):
            pd_copy(j, r).start()

    in_x.wait()
    x_own = x_ref[...].astype(jnp.float32)
    st[t] = pack_cols(jnp.sum(x_own, axis=1, keepdims=True), jnp.sum(x_own * x_own, axis=1, keepdims=True))
    in_dy.wait()
    in_gain.wait()
    pl.semaphore_wait(barrier, 8)
    send_stats(st, ss, sr)
    zdy = remote(dya_ref.at[own, :], dya_ref.at[own, :], zs.at[0], zr.at[0], dev_z)
    zdy.start()
    for i in range(LEAD):
        wcopy(2, i).wait()
        da_product(i)
    for i in range(LEAD):
        da_pair_sum(i)
    acc[...] = jnp.zeros_like(acc)

    gain = gain_ref[...]
    c0, c1 = total_stats(st, ss, sr)
    mean_x = c0 / d_model
    inv_std = lax.rsqrt(c1 / d_model - mean_x * mean_x + LN_EPS)
    xhat = (x_ref[...].astype(jnp.float32) - mean_x) * inv_std
    xh[...] = xhat
    h_ref[own, :] = (gain * xhat).astype(jnp.bfloat16)

    def h_copy(block):
        return remote(h_ref.at[own, :], h_ref.at[block, :], zs.at[1], zr.at[1], dev_z)

    h_copy(own).start()

    z_sum = remote(acc.at[1], zin, zs.at[2], zr.at[2], dev_z)

    def step(i, carry):
        @pl.when(jnp.logical_and(i >= P_SLOTS, i < n_units + P_SLOTS))
        def _():
            j = i - P_SLOTS
            d_copy(j).wait_send()
            dd_copy(j).wait_send()
            for r in range(2):
                p1_copy(j, r).wait_send()
                pd_copy(j, r).wait_send()

        @pl.when(i < n_f)
        def _():
            wcopy(0, i).wait()
            wcopy(1, i).wait()

        @pl.when(i + LEAD < n_f)
        def _():
            wcopy(2, i + LEAD).wait()

        @pl.when(i == OWN_FIRST - LEAD)
        def _():
            remote(dya_ref.at[own, :], dya_ref.at[oth, :], zs.at[0], zr.at[0], dev_z).wait_recv()

        @pl.when(i == OWN_FIRST)
        def _():
            h_copy(oth).wait_recv()
            h_t[...] = h_ref[...].T

        @pl.when(i < n_units)
        def _():
            cs = fcols(i)
            slot = lax.rem(i, P_SLOTS)
            h = h_ref[trows(i), :]
            part[slot, 0] = jnp.dot(h, wg[:, cs], preferred_element_type=jnp.float32)
            part[slot, 1] = jnp.dot(h, wu[:, cs], preferred_element_type=jnp.float32)
            d_copy(i).start()

        @pl.when(i + LEAD < n_units)
        def _():
            da_product(i + LEAD)

        @pl.when(jnp.logical_and(i >= STAGES[0], i < n_units + STAGES[0]))
        def _():
            j = i - STAGES[0]
            d_copy(j).wait_recv()
            slot = lax.rem(j, P_SLOTS)
            for k in range(2):
                part[slot, k, own_c, :] = part[slot, k, own_c, :] + dsum[slot, k]
            for r in range(2):
                p1_copy(j, r).start()

            @pl.when(j + LEAD < n_units)
            def _():
                da_pair_sum(j + LEAD)

        @pl.when(jnp.logical_and(i >= STAGES[1], i < n_units + STAGES[1]))
        def _():
            j = i - STAGES[1]
            slot = lax.rem(j, P_SLOTS)
            for r in range(2):
                pd_copy(j, r).wait_recv()
                p1_copy(j, r).wait_recv()
                for k in range(2):
                    r1[j, r, k] = r1[j, r, k] + part[slot, k, keep1[r], colw[r]]
                r1[j, r, 2] = r1[j, r, 2] + part_d[lax.rem(j, L_SLOTS), keep1[r], colw[r]]
                p2_copy(j, r).start()

        @pl.when(jnp.logical_and(i >= STAGES[2], i < n_units + STAGES[2]))
        def _():
            j = i - STAGES[2]
            for r in range(2):
                p2_copy(j, r).wait_recv()
                u = r1[j, r, 0, r_keep[r], :] + r2[j, r, 0]
                v = r1[j, r, 1, r_keep[r], :] + r2[j, r, 1]
                da = r1[j, r, 2, r_keep[r], :] + r2[j, r, 2]
                sig = jax.nn.sigmoid(u)
                swish = u * sig
                cs = gcols(j, r)
                rs = grows(j, g_fin[r], q3)
                gat[0, rs, cs] = (swish * v).astype(jnp.bfloat16)
                gat[1, rs, cs] = (da * v * sig * (1.0 + u * (1.0 - sig))).astype(jnp.bfloat16)
                gat[2, rs, cs] = (da * swish).astype(jnp.bfloat16)
                g1_copy(j, r, g_fin).start()

        @pl.when(jnp.logical_and(i >= STAGES[3], i < n_units + STAGES[3]))
        def _():
            j = i - STAGES[3]
            for r in range(2):
                g1_copy(j, r, g_fin_n).wait_recv()
                g2_copy(j, r, g_keep1).start()

        @pl.when(jnp.logical_and(i >= STAGES[4], i < n_units + STAGES[4]))
        def _():
            j = i - STAGES[4]
            for r in range(2):
                g2_copy(j, r, g_send1).wait_recv()
            gd_copy(j, g_c[0]).start()

        @pl.when(i >= STAGES[5])
        def _():
            j = i - STAGES[5]
            gd_copy(j, g_c[1]).wait_recv()

            cs = fcols(j)
            rs = trows(j)
            side = oth_of(j)
            acc[side, 0] += jnp.dot(gat[0, rs, cs], wd[cs, :], preferred_element_type=jnp.float32)
            acc[side, 1] += contract_cols(gat[1, rs, cs], wg[:, cs]) + contract_cols(gat[2, rs, cs], wu[:, cs])
            for r in range(2):
                p2_copy(j, r).wait_send()
                g1_copy(j, r, g_fin).wait_send()
                g2_copy(j, r, g_keep1).wait_send()
            gd_copy(j, g_c[0]).wait_send()

            @pl.when(j == last_oth)
            def _():
                z_sum.start()
        return carry

    lax.fori_loop(0, n_units + STAGES[5], step, 0)

    z_sum.wait()
    d_hnorm = acc[0, 1] + zin[1]
    e = d_hnorm * gain
    rb[t] = pack_cols(jnp.sum(e, axis=1, keepdims=True), jnp.sum(e * xh[...], axis=1, keepdims=True))
    send_stats(rb, bs, br)
    dgs[...] = jnp.broadcast_to(jnp.sum(d_hnorm * xh[...], axis=0, keepdims=True), dgs.shape)
    z_dg = remote(dgs, dgr, zs.at[3], zr.at[3], dev_z)
    z_dg.start()
    y_ref[...] = (x_ref[...].astype(jnp.float32) + (acc[0, 0] + zin[0])).astype(jnp.bfloat16)
    zdy.wait_send()
    h_copy(own).wait_send()
    c0, c1 = total_stats(rb, bs, br)
    dx_ln = inv_std * (e - c0 / d_model - xh[...] * (c1 / d_model))
    dx_ref[...] = (dya_ref[own, :].astype(jnp.float32) + dx_ln).astype(jnp.bfloat16)
    z_dg.wait()
    dg_ref[...] = dgs[0:1, :] + dgr[0:1, :]


def weight_grad_kernel(gat, h_t, dy_ref, y_in, dx_in, dg_in,
                       dwg_hbm, dwu_hbm, dwd_hbm, y_hbm, dx_hbm, dg_hbm, buf, bsem, ssem):
    n_blocks = gat.shape[2] // WB

    def out_copy(b, k):
        cs = pl.ds(mo(b * WB, WB), WB)
        dst = (dwg_hbm.at[:, cs], dwu_hbm.at[:, cs], dwd_hbm.at[cs, :])[k]
        slot = lax.rem(b, W_SLOTS)
        return pltpu.make_async_copy(buf.at[slot, k], dst, bsem.at[slot, k])

    def block(b, carry):
        cs = pl.ds(mo(b * WB, WB), WB)
        slot = lax.rem(b, W_SLOTS)
        for k in range(3):
            @pl.when(b >= W_SLOTS)
            def _():
                out_copy(b - W_SLOTS, k).wait()

            if k < 2:
                buf[slot, k] = jnp.dot(h_t[...], gat[k + 1, :, cs], preferred_element_type=jnp.float32)
            else:
                buf[slot, k] = contract_rows(gat[0, :, cs], dy_ref[...])
            out_copy(b, k).start()
        return carry

    lax.fori_loop(0, n_blocks, block, 0)
    small = [pltpu.make_async_copy(src, dst, ssem.at[k])
             for k, (src, dst) in enumerate(((y_in, y_hbm), (dx_in, dx_hbm), (dg_in, dg_hbm)))]
    for d in small:
        d.start()

    def drain(b, carry):
        for k in range(3):
            out_copy(b, k).wait()
        return carry

    lax.fori_loop(n_blocks - W_SLOTS, n_blocks, drain, 0)
    for d in small:
        d.wait()


def solution(mesh):
    tx_size = mesh.shape["tx"]
    ty_size = mesh.shape["ty"]

    def local_step(x_blk, dy_blk, gain_blk, w_gate_blk, w_up_blk, w_down_blk):
        rows, dl = x_blk.shape
        fl = w_gate_blk.shape[1]
        tok = rows * ty_size
        d_model = dl * tx_size
        n = fl // FC
        half = FC // 2
        f32, bf16 = jnp.float32, jnp.bfloat16
        anyspec = pl.BlockSpec(memory_space=pl.ANY)
        sem = pltpu.SemaphoreType.DMA
        vm = pl.BlockSpec(memory_space=pltpu.VMEM)
        S = jax.ShapeDtypeStruct
        V = pltpu.VMEM
        small = [((rows, dl), bf16), ((rows, dl), bf16), ((1, dl), f32)]
        outs = pl.pallas_call(
            functools.partial(branch_kernel, d_model, n),
            out_shape=[V((3, tok, fl), bf16), V((dl, tok), bf16), V((tok, dl), bf16)] + [V(*s) for s in small],
            in_specs=[anyspec] * 6,
            out_specs=[vm] * 6,
            scratch_shapes=[
                V((rows, dl), bf16), V((1, dl), f32), V((tok, dl), bf16),
                V((dl, fl), bf16), V((dl, fl), bf16), V((fl, dl), bf16),
                V((rows, dl), f32),
                V((P_SLOTS, 2, rows, FC), f32), V((L_SLOTS, rows, FC), f32),
                V((P_SLOTS, 2, rows // 2, FC), f32), V((L_SLOTS, rows // 2, FC), f32),
                V((2 * n, 2, 3, rows // 4, half), f32), V((2 * n, 2, 3, rows // 8, half), f32),
                V((2, 2, rows, dl), f32), V((2, rows, dl), f32),
                V((8, 8, 128), f32), V((8, 8, 128), f32), V((8, dl), f32), V((8, dl), f32),
                sem((3, n)), sem((3,)), sem((4,)), sem((4,)), sem((8,)), sem((8,)), sem((8,)), sem((8,)),
                sem((RING,)), sem((RING,)), sem((RING,)), sem((RING,)),
                *[sem((2, RING)) for _ in range(10)],
                sem((RING,)), sem((RING,)),
            ],
            compiler_params=pltpu.CompilerParams(collective_id=0, has_side_effects=True, vmem_limit_bytes=VMEM_LIMIT),
            cost_estimate=pl.CostEstimate(flops=12 * tok * dl * fl, bytes_accessed=6 * dl * fl + 6 * tok * fl, transcendentals=0),
        )(x_blk, dy_blk, gain_blk[None, :], w_gate_blk, w_up_blk, w_down_blk)

        dwg, dwu, dwd, y_blk, dx_blk, dg = pl.pallas_call(
            weight_grad_kernel,
            out_shape=[S((dl, fl), f32)] * 2 + [S((fl, dl), f32)] + [S(*s) for s in small],
            in_specs=[vm] * 6,
            out_specs=[anyspec] * 6,
            scratch_shapes=[
                V((W_SLOTS, 3, dl, WB), f32), sem((W_SLOTS, 3)), sem((3,)),
            ],
            compiler_params=pltpu.CompilerParams(vmem_limit_bytes=VMEM_LIMIT),
            cost_estimate=pl.CostEstimate(flops=6 * tok * dl * fl, bytes_accessed=12 * dl * fl + 6 * tok * fl, transcendentals=0),
        )(*[pltpu.with_memory_space_constraint(o, pltpu.VMEM) for o in outs])
        return (y_blk, dx_blk, dwg, dwu, dwd, dg[0])

    return jax.shard_map(
        local_step, mesh=mesh,
        in_specs=(P("ty", "tx"), P("ty", "tx"), P("tx"), P("tx", "ty"), P("tx", "ty"), P("ty", "tx")),
        out_specs=(P("ty", "tx"), P("ty", "tx"), P("tx", "ty"), P("tx", "ty"), P("ty", "tx"), P("tx")),
        check_vma=False)
```

```python
import functools

import jax
import jax.numpy as jnp
from jax import lax
from jax.experimental import pallas as pl
from jax.experimental.pallas import tpu as pltpu
from jax.sharding import PartitionSpec as P

LN_EPS = 1e-6
MESH = pl.DeviceIdType.MESH
FC = 512
OWN_FIRST = 8
LEAD = 8
P_SLOTS = 4
L_SLOTS = LEAD + P_SLOTS
HELD = 8
RING = 16
STAGES = (1, 3, 5, 7, 9, 10)
WB = 512
W_SLOTS = 3
VMEM_LIMIT = 48 * 1024 * 1024


def contract_rows(left_op, right_op):
    return lax.dot_general(left_op, right_op, (((0,), (0,)), ((), ())), preferred_element_type=jnp.float32)


def contract_cols(left_op, right_op):
    return lax.dot_general(left_op, right_op, (((1,), (1,)), ((), ())), preferred_element_type=jnp.float32)


def mo(value, multiple):
    return pl.multiple_of(value, multiple)


def branch_kernel(d_model, n_f,
                  x_hbm, dy_hbm, gain_hbm, wg_hbm, wu_hbm, wd_hbm,
                  gat, h_t, dya_ref, y_ref, dx_ref, dg_ref,
                  x_ref, gain_ref, h_ref,
                  wg, wu, wd, xh, part, part_d, dsum, dsum_d, r1, r2, acc, zin, st, rb, dgs, dgr,
                  wsem, isem, zs, zr, ss, sr, bs, br, ds, dr, dds, ddr, p1s, p1r, pds, pdr, p2s, p2r,
                  g1s, g1r, g2s, g2r, gds, gdr, a1s, a1r, a2s, a2r, ads, adr):
    half = FC // 2
    rows = x_ref.shape[0]
    q1, q2, q3 = rows // 2, rows // 4, rows // 8
    n_units = 2 * n_f
    last_oth = OWN_FIRST + n_f - 1
    held = n_units - HELD

    ty = lax.axis_index("ty")
    t = lax.axis_index("tx")
    c = lax.rem(t, 2)
    xc = lax.rem(lax.div(t, 2), 2)
    yc = lax.div(t, 4)
    dev_c = (ty, t + 1 - 2 * c)
    dev_x = (ty, t + 2 - 4 * xc)
    dev_y = (ty, t + 4 - 8 * yc)
    dev_z = (1 - ty, t)
    own = pl.ds(mo(ty * rows, rows), rows)
    oth = pl.ds(mo((1 - ty) * rows, rows), rows)

    def remote(src, dst, ssem, rsem, dev):
        return pltpu.make_async_remote_copy(src_ref=src, dst_ref=dst, send_sem=ssem, recv_sem=rsem,
                                            device_id=dev, device_id_type=MESH)

    def f_of(j):
        return lax.rem(j + (n_f - OWN_FIRST), n_f)

    def oth_of(j):
        return lax.rem(lax.div(j + (n_f - OWN_FIRST), n_f), 2)

    def base_of(j):
        k = oth_of(j)
        return (ty + k - 2 * ty * k) * rows

    def fcols(j):
        return pl.ds(mo(f_of(j) * FC, FC), FC)

    def trows(j):
        return pl.ds(mo(base_of(j), rows), rows)

    def wcopy(k, i):
        cs = fcols(i)
        if k == 0:
            return pltpu.make_async_copy(wg_hbm.at[:, cs], wg.at[:, cs], wsem.at[0, i])
        if k == 1:
            return pltpu.make_async_copy(wu_hbm.at[:, cs], wu.at[:, cs], wsem.at[1, i])
        return pltpu.make_async_copy(wd_hbm.at[cs, :], wd.at[cs, :], wsem.at[2, i])

    in_dy = pltpu.make_async_copy(dy_hbm, dya_ref.at[own, :], isem.at[0])
    in_x = pltpu.make_async_copy(x_hbm, x_ref, isem.at[1])
    in_gain = pltpu.make_async_copy(gain_hbm, gain_ref, isem.at[2])
    in_x.start()
    in_dy.start()
    in_gain.start()
    for i in range(LEAD):
        wcopy(2, i).start()

    barrier = pltpu.get_barrier_semaphore()
    for o in range(1, 8):
        pl.semaphore_signal(barrier, inc=1, device_id=(ty, lax.rem(t + o, 8)), device_id_type=MESH)
    pl.semaphore_signal(barrier, inc=1, device_id=dev_z, device_id_type=MESH)

    def start_w(i, carry):
        wcopy(0, i).start()
        wcopy(1, i).start()

        @pl.when(i + LEAD < n_f)
        def _():
            wcopy(2, i + LEAD).start()
        return carry

    lax.fori_loop(0, n_f, start_w, 0)

    lane = lax.broadcasted_iota(jnp.int32, (rows, 128), 1)

    def pack_cols(c0, c1):
        both = jnp.where(lane == 0, c0, jnp.where(lane == 1, c1, 0.0))
        return both.T[0:8, :]

    def unpack_cols(packed):
        full = jnp.concatenate([packed, jnp.zeros((rows - 8, 128), jnp.float32)], axis=0).T
        return full[:, 0:1], full[:, 1:2]

    def send_stats(buf, ssem, rsem):
        for o in range(1, 8):
            remote(buf.at[t], buf.at[t], ssem.at[o], rsem.at[o], (ty, lax.rem(t + o, 8))).start()

    def total_stats(buf, ssem, rsem):
        for o in range(1, 8):
            q = lax.rem(t + 8 - o, 8)
            d = remote(buf.at[t], buf.at[q], ssem.at[o], rsem.at[o], (ty, q))
            d.wait_send()
            d.wait_recv()
        s = buf[0]
        for j in range(1, 8):
            s = s + buf[j]
        return unpack_cols(s)

    def seg(base, size):
        return pl.ds(mo(base, size), size)

    own_c = seg(c * q1, q1)
    oth_c = seg((1 - c) * q1, q1)
    keep1 = (seg(c * q1 + xc * q2, q2), seg(c * q1 + yc * q2, q2))
    send1 = (seg(c * q1 + (1 - xc) * q2, q2), seg(c * q1 + (1 - yc) * q2, q2))
    r_keep = (seg(yc * q3, q3), seg(xc * q3, q3))
    r_send = (seg((1 - yc) * q3, q3), seg((1 - xc) * q3, q3))
    colw = (slice(0, half), slice(half, FC))
    dev1, dev2 = (dev_x, dev_y), (dev_y, dev_x)
    g_c = (c * q1, (1 - c) * q1)
    g_keep1 = (c * q1 + xc * q2, c * q1 + yc * q2)
    g_send1 = (c * q1 + (1 - xc) * q2, c * q1 + (1 - yc) * q2)
    g_fin = (g_keep1[0] + yc * q3, g_keep1[1] + xc * q3)
    g_fin_n = (g_keep1[0] + (1 - yc) * q3, g_keep1[1] + (1 - xc) * q3)

    def gcols(j, r):
        return pl.ds(mo(f_of(j) * FC + r * half, half), half)

    def grows(j, off, size):
        return pl.ds(mo(base_of(j) + off, size), size)

    def ring(j):
        return lax.rem(j, RING)

    def d_copy(j):
        slot = lax.rem(j, P_SLOTS)
        return remote(part.at[slot, :, oth_c, :], dsum.at[slot], ds.at[ring(j)], dr.at[ring(j)], dev_c)

    def dd_copy(j):
        slot = lax.rem(j, L_SLOTS)
        return remote(part_d.at[slot, oth_c, :], dsum_d.at[slot], dds.at[ring(j)], ddr.at[ring(j)], dev_c)

    def p1_copy(j, r):
        return remote(part.at[lax.rem(j, P_SLOTS), :, send1[r], colw[r]], r1.at[j, r, 0:2],
                      p1s.at[r, ring(j)], p1r.at[r, ring(j)], dev1[r])

    def pd_copy(j, r):
        return remote(part_d.at[lax.rem(j, L_SLOTS), send1[r], colw[r]], r1.at[j, r, 2],
                      pds.at[r, ring(j)], pdr.at[r, ring(j)], dev1[r])

    def p2_copy(j, r):
        return remote(r1.at[j, r, :, r_send[r], :], r2.at[j, r], p2s.at[r, ring(j)], p2r.at[r, ring(j)], dev2[r])

    def g1_copy(j, r, off, lo):
        ref = gat.at[lo:3, grows(j, off[r], q3), gcols(j, r)]
        return remote(ref, ref, g1s.at[r, ring(j)], g1r.at[r, ring(j)], dev2[r])

    def g2_copy(j, r, off, lo):
        ref = gat.at[lo:3, grows(j, off[r], q2), gcols(j, r)]
        return remote(ref, ref, g2s.at[r, ring(j)], g2r.at[r, ring(j)], dev1[r])

    def gd_copy(j, off, lo):
        ref = gat.at[lo:3, grows(j, off, q1), fcols(j)]
        return remote(ref, ref, gds.at[ring(j)], gdr.at[ring(j)], dev_c)

    def a1_copy(k, r, off):
        ref = gat.at[0, grows(held + k, off[r], q3), gcols(held + k, r)]
        return remote(ref, ref, a1s.at[r, k], a1r.at[r, k], dev2[r])

    def a2_copy(k, r, off):
        ref = gat.at[0, grows(held + k, off[r], q2), gcols(held + k, r)]
        return remote(ref, ref, a2s.at[r, k], a2r.at[r, k], dev1[r])

    def ad_copy(k, off):
        ref = gat.at[0, grows(held + k, off, q1), fcols(held + k)]
        return remote(ref, ref, ads.at[k], adr.at[k], dev_c)

    def by_arrays(j, body):
        @pl.when(j < held)
        def _():
            body(0)

        @pl.when(j >= held)
        def _():
            body(1)

    def each_held(body):
        def one(k, carry):
            body(k)
            return carry

        lax.fori_loop(0, HELD, one, 0)

    def da_dot(j):
        part_d[lax.rem(j, L_SLOTS)] = contract_cols(dya_ref[trows(j), :], wd[fcols(j), :])

    def da_product(j):
        da_dot(j)
        dd_copy(j).start()

    def da_pair_sum(j):
        dd_copy(j).wait_recv()
        slot = lax.rem(j, L_SLOTS)
        part_d[slot, own_c, :] = part_d[slot, own_c, :] + dsum_d[slot]
        for r in range(2):
            pd_copy(j, r).start()

    in_dy.wait()
    wcopy(2, 0).wait()
    da_dot(0)
    pl.semaphore_wait(barrier, 8)
    dd_copy(0).start()
    in_x.wait()
    x_own = x_ref[...].astype(jnp.float32)
    st[t] = pack_cols(jnp.sum(x_own, axis=1, keepdims=True), jnp.sum(x_own * x_own, axis=1, keepdims=True))
    send_stats(st, ss, sr)
    zdy = remote(dya_ref.at[own, :], dya_ref.at[own, :], zs.at[0], zr.at[0], dev_z)
    zdy.start()
    for i in range(1, 3):
        wcopy(2, i).wait()
        da_product(i)
    for i in range(LEAD):
        da_pair_sum(i)
        if i + 3 < LEAD:
            wcopy(2, i + 3).wait()
            da_product(i + 3)
    in_gain.wait()
    acc[...] = jnp.zeros_like(acc)

    gain = gain_ref[...]
    c0, c1 = total_stats(st, ss, sr)
    mean_x = c0 / d_model
    inv_std = lax.rsqrt(c1 / d_model - mean_x * mean_x + LN_EPS)
    xhat = (x_ref[...].astype(jnp.float32) - mean_x) * inv_std
    xh[...] = xhat
    h_ref[own, :] = (gain * xhat).astype(jnp.bfloat16)

    def h_copy(block):
        return remote(h_ref.at[own, :], h_ref.at[block, :], zs.at[1], zr.at[1], dev_z)

    h_copy(own).start()

    z_sum = remote(acc.at[1], zin, zs.at[2], zr.at[2], dev_z)

    def step(i, carry):
        @pl.when(jnp.logical_and(i >= P_SLOTS, i < n_units + P_SLOTS))
        def _():
            j = i - P_SLOTS
            d_copy(j).wait_send()
            dd_copy(j).wait_send()
            for r in range(2):
                p1_copy(j, r).wait_send()
                pd_copy(j, r).wait_send()

        @pl.when(i < n_f)
        def _():
            wcopy(0, i).wait()
            wcopy(1, i).wait()

        @pl.when(i + LEAD < n_f)
        def _():
            wcopy(2, i + LEAD).wait()

        @pl.when(i == OWN_FIRST - LEAD)
        def _():
            remote(dya_ref.at[own, :], dya_ref.at[oth, :], zs.at[0], zr.at[0], dev_z).wait_recv()

        @pl.when(i == OWN_FIRST)
        def _():
            h_copy(oth).wait_recv()
            h_t[...] = h_ref[...].T

        @pl.when(i < n_units)
        def _():
            cs = fcols(i)
            slot = lax.rem(i, P_SLOTS)
            h = h_ref[trows(i), :]
            part[slot, 0] = jnp.dot(h, wg[:, cs], preferred_element_type=jnp.float32)
            part[slot, 1] = jnp.dot(h, wu[:, cs], preferred_element_type=jnp.float32)
            d_copy(i).start()

        @pl.when(i + LEAD < n_units)
        def _():
            da_product(i + LEAD)

        @pl.when(jnp.logical_and(i >= STAGES[0], i < n_units + STAGES[0]))
        def _():
            j = i - STAGES[0]
            d_copy(j).wait_recv()
            slot = lax.rem(j, P_SLOTS)
            for k in range(2):
                part[slot, k, own_c, :] = part[slot, k, own_c, :] + dsum[slot, k]
            for r in range(2):
                p1_copy(j, r).start()

            @pl.when(j + LEAD < n_units)
            def _():
                da_pair_sum(j + LEAD)

        @pl.when(jnp.logical_and(i >= STAGES[1], i < n_units + STAGES[1]))
        def _():
            j = i - STAGES[1]
            slot = lax.rem(j, P_SLOTS)
            for r in range(2):
                pd_copy(j, r).wait_recv()
                p1_copy(j, r).wait_recv()
                for k in range(2):
                    r1[j, r, k] = r1[j, r, k] + part[slot, k, keep1[r], colw[r]]
                r1[j, r, 2] = r1[j, r, 2] + part_d[lax.rem(j, L_SLOTS), keep1[r], colw[r]]
                p2_copy(j, r).start()

        @pl.when(jnp.logical_and(i >= STAGES[2], i < n_units + STAGES[2]))
        def _():
            j = i - STAGES[2]
            for r in range(2):
                p2_copy(j, r).wait_recv()
                u = r1[j, r, 0, r_keep[r], :] + r2[j, r, 0]
                v = r1[j, r, 1, r_keep[r], :] + r2[j, r, 1]
                da = r1[j, r, 2, r_keep[r], :] + r2[j, r, 2]
                sig = jax.nn.sigmoid(u)
                swish = u * sig
                cs = gcols(j, r)
                rs = grows(j, g_fin[r], q3)
                gat[0, rs, cs] = (swish * v).astype(jnp.bfloat16)
                gat[1, rs, cs] = (da * v * sig * (1.0 + u * (1.0 - sig))).astype(jnp.bfloat16)
                gat[2, rs, cs] = (da * swish).astype(jnp.bfloat16)
            by_arrays(j, lambda lo: [g1_copy(j, r, g_fin, lo).start() for r in range(2)])

        @pl.when(jnp.logical_and(i >= STAGES[3], i < n_units + STAGES[3]))
        def _():
            j = i - STAGES[3]

            def forward(lo):
                for r in range(2):
                    g1_copy(j, r, g_fin_n, lo).wait_recv()
                    g2_copy(j, r, g_keep1, lo).start()

            by_arrays(j, forward)

        @pl.when(jnp.logical_and(i >= STAGES[4], i < n_units + STAGES[4]))
        def _():
            j = i - STAGES[4]

            def to_core(lo):
                for r in range(2):
                    g2_copy(j, r, g_send1, lo).wait_recv()
                gd_copy(j, g_c[0], lo).start()

            by_arrays(j, to_core)

        @pl.when(i >= STAGES[5])
        def _():
            j = i - STAGES[5]
            by_arrays(j, lambda lo: gd_copy(j, g_c[1], lo).wait_recv())
            cs = fcols(j)
            rs = trows(j)
            side = oth_of(j)

            @pl.when(j < held)
            def _():
                acc[side, 0] += jnp.dot(gat[0, rs, cs], wd[cs, :], preferred_element_type=jnp.float32)

            acc[side, 1] += contract_cols(gat[1, rs, cs], wg[:, cs]) + contract_cols(gat[2, rs, cs], wu[:, cs])

            def sent(lo):
                for r in range(2):
                    p2_copy(j, r).wait_send()
                    g1_copy(j, r, g_fin, lo).wait_send()
                    g2_copy(j, r, g_keep1, lo).wait_send()
                gd_copy(j, g_c[0], lo).wait_send()

            by_arrays(j, sent)

            @pl.when(j == last_oth)
            def _():
                z_sum.start()

        @pl.when(i == n_units - 1 + STAGES[2])
        def _():
            each_held(lambda k: [a1_copy(k, r, g_fin).start() for r in range(2)])

        @pl.when(i == n_units - 1 + STAGES[3])
        def _():
            def forward(k):
                for r in range(2):
                    a1_copy(k, r, g_fin_n).wait_recv()
                    a2_copy(k, r, g_keep1).start()

            each_held(forward)
        return carry

    lax.fori_loop(0, n_units + STAGES[5], step, 0)

    z_sum.wait()
    d_hnorm = acc[0, 1] + zin[1]
    e = d_hnorm * gain
    rb[t] = pack_cols(jnp.sum(e, axis=1, keepdims=True), jnp.sum(e * xh[...], axis=1, keepdims=True))
    send_stats(rb, bs, br)
    dgs[...] = jnp.broadcast_to(jnp.sum(d_hnorm * xh[...], axis=0, keepdims=True), dgs.shape)
    z_dg = remote(dgs, dgr, zs.at[3], zr.at[3], dev_z)
    z_dg.start()

    def to_core(k):
        for r in range(2):
            a2_copy(k, r, g_send1).wait_recv()
        ad_copy(k, g_c[0]).start()

    each_held(to_core)

    def m_product(k):
        ad_copy(k, g_c[1]).wait_recv()
        cs = fcols(held + k)
        acc[0, 0] += jnp.dot(gat[0, own, cs], wd[cs, :], preferred_element_type=jnp.float32)
        for r in range(2):
            a1_copy(k, r, g_fin).wait_send()
            a2_copy(k, r, g_keep1).wait_send()
        ad_copy(k, g_c[0]).wait_send()

    each_held(m_product)
    y_ref[...] = (x_ref[...].astype(jnp.float32) + (acc[0, 0] + zin[0])).astype(jnp.bfloat16)
    zdy.wait_send()
    h_copy(own).wait_send()
    c0, c1 = total_stats(rb, bs, br)
    dx_ln = inv_std * (e - c0 / d_model - xh[...] * (c1 / d_model))
    dx_ref[...] = (dya_ref[own, :].astype(jnp.float32) + dx_ln).astype(jnp.bfloat16)
    z_dg.wait()
    dg_ref[...] = dgs[0:1, :] + dgr[0:1, :]


def weight_grad_kernel(gat, h_t, dy_ref, y_in, dx_in, dg_in,
                       dwg_hbm, dwu_hbm, dwd_hbm, y_hbm, dx_hbm, dg_hbm, buf, bsem, ssem):
    n_blocks = gat.shape[2] // WB

    def out_copy(b, k):
        cs = pl.ds(mo(b * WB, WB), WB)
        dst = (dwg_hbm.at[:, cs], dwu_hbm.at[:, cs], dwd_hbm.at[cs, :])[k]
        slot = lax.rem(b, W_SLOTS)
        return pltpu.make_async_copy(buf.at[slot, k], dst, bsem.at[slot, k])

    def block(b, carry):
        cs = pl.ds(mo(b * WB, WB), WB)
        slot = lax.rem(b, W_SLOTS)
        for k in range(3):
            @pl.when(b >= W_SLOTS)
            def _():
                out_copy(b - W_SLOTS, k).wait()

            if k < 2:
                buf[slot, k] = jnp.dot(h_t[...], gat[k + 1, :, cs], preferred_element_type=jnp.float32)
            else:
                buf[slot, k] = contract_rows(gat[0, :, cs], dy_ref[...])
            out_copy(b, k).start()
        return carry

    lax.fori_loop(0, n_blocks, block, 0)
    small = [pltpu.make_async_copy(src, dst, ssem.at[k])
             for k, (src, dst) in enumerate(((y_in, y_hbm), (dx_in, dx_hbm), (dg_in, dg_hbm)))]
    for d in small:
        d.start()

    def drain(b, carry):
        for k in range(3):
            out_copy(b, k).wait()
        return carry

    lax.fori_loop(n_blocks - W_SLOTS, n_blocks, drain, 0)
    for d in small:
        d.wait()


def solution(mesh):
    tx_size = mesh.shape["tx"]
    ty_size = mesh.shape["ty"]

    def local_step(x_blk, dy_blk, gain_blk, w_gate_blk, w_up_blk, w_down_blk):
        rows, dl = x_blk.shape
        fl = w_gate_blk.shape[1]
        tok = rows * ty_size
        d_model = dl * tx_size
        n = fl // FC
        half = FC // 2
        f32, bf16 = jnp.float32, jnp.bfloat16
        anyspec = pl.BlockSpec(memory_space=pl.ANY)
        sem = pltpu.SemaphoreType.DMA
        vm = pl.BlockSpec(memory_space=pltpu.VMEM)
        S = jax.ShapeDtypeStruct
        V = pltpu.VMEM
        small = [((rows, dl), bf16), ((rows, dl), bf16), ((1, dl), f32)]
        outs = pl.pallas_call(
            functools.partial(branch_kernel, d_model, n),
            out_shape=[V((3, tok, fl), bf16), V((dl, tok), bf16), V((tok, dl), bf16)] + [V(*s) for s in small],
            in_specs=[anyspec] * 6,
            out_specs=[vm] * 6,
            scratch_shapes=[
                V((rows, dl), bf16), V((1, dl), f32), V((tok, dl), bf16),
                V((dl, fl), bf16), V((dl, fl), bf16), V((fl, dl), bf16),
                V((rows, dl), f32),
                V((P_SLOTS, 2, rows, FC), f32), V((L_SLOTS, rows, FC), f32),
                V((P_SLOTS, 2, rows // 2, FC), f32), V((L_SLOTS, rows // 2, FC), f32),
                V((2 * n, 2, 3, rows // 4, half), f32), V((2 * n, 2, 3, rows // 8, half), f32),
                V((2, 2, rows, dl), f32), V((2, rows, dl), f32),
                V((8, 8, 128), f32), V((8, 8, 128), f32), V((8, dl), f32), V((8, dl), f32),
                sem((3, n)), sem((3,)), sem((4,)), sem((4,)), sem((8,)), sem((8,)), sem((8,)), sem((8,)),
                sem((RING,)), sem((RING,)), sem((RING,)), sem((RING,)),
                *[sem((2, RING)) for _ in range(10)],
                sem((RING,)), sem((RING,)),
                *[sem((2, HELD)) for _ in range(4)], sem((HELD,)), sem((HELD,)),
            ],
            compiler_params=pltpu.CompilerParams(collective_id=0, has_side_effects=True, vmem_limit_bytes=VMEM_LIMIT),
            cost_estimate=pl.CostEstimate(flops=12 * tok * dl * fl, bytes_accessed=6 * dl * fl + 6 * tok * fl, transcendentals=0),
        )(x_blk, dy_blk, gain_blk[None, :], w_gate_blk, w_up_blk, w_down_blk)

        dwg, dwu, dwd, y_blk, dx_blk, dg = pl.pallas_call(
            weight_grad_kernel,
            out_shape=[S((dl, fl), f32)] * 2 + [S((fl, dl), f32)] + [S(*s) for s in small],
            in_specs=[vm] * 6,
            out_specs=[anyspec] * 6,
            scratch_shapes=[
                V((W_SLOTS, 3, dl, WB), f32), sem((W_SLOTS, 3)), sem((3,)),
            ],
            compiler_params=pltpu.CompilerParams(vmem_limit_bytes=VMEM_LIMIT),
            cost_estimate=pl.CostEstimate(flops=6 * tok * dl * fl, bytes_accessed=12 * dl * fl + 6 * tok * fl, transcendentals=0),
        )(*[pltpu.with_memory_space_constraint(o, pltpu.VMEM) for o in outs])
        return (y_blk, dx_blk, dwg, dwu, dwd, dg[0])

    return jax.shard_map(
        local_step, mesh=mesh,
        in_specs=(P("ty", "tx"), P("ty", "tx"), P("tx"), P("tx", "ty"), P("tx", "ty"), P("ty", "tx")),
        out_specs=(P("ty", "tx"), P("ty", "tx"), P("tx", "ty"), P("tx", "ty"), P("ty", "tx"), P("tx")),
        check_vma=False)
```

```python
import functools

import jax
import jax.numpy as jnp
from jax import lax
from jax.experimental import pallas as pl
from jax.experimental.pallas import tpu as pltpu
from jax.sharding import PartitionSpec as P

LN_EPS = 1e-6
MESH = pl.DeviceIdType.MESH
FC = 256
OWN_FIRST = 16
LEAD = 14
P_SLOTS = 6
L_SLOTS = LEAD + P_SLOTS
HELD = 16
RING = 24
STAGES = (1, 4, 7, 10, 13, 14)
WB = 512
W_SLOTS = 3
VMEM_LIMIT = 48 * 1024 * 1024


def contract_rows(left_op, right_op):
    return lax.dot_general(left_op, right_op, (((0,), (0,)), ((), ())), preferred_element_type=jnp.float32)


def contract_cols(left_op, right_op):
    return lax.dot_general(left_op, right_op, (((1,), (1,)), ((), ())), preferred_element_type=jnp.float32)


def mo(value, multiple):
    return pl.multiple_of(value, multiple)


def branch_kernel(d_model, n_f,
                  x_hbm, dy_hbm, gain_hbm, wg_hbm, wu_hbm, wd_hbm,
                  gat, h_t, dya_ref, y_ref, dx_ref, dg_ref,
                  x_ref, gain_ref, h_ref,
                  wg, wu, wd, xh, part, part_d, dsum, dsum_d, r1, r2, acc, zin, st, rb, dgs, dgr,
                  wsem, isem, zs, zr, ss, sr, bs, br, ds, dr, dds, ddr, p1s, p1r, pds, pdr, p2s, p2r,
                  g1s, g1r, g2s, g2r, gds, gdr, a1s, a1r, a2s, a2r, ads, adr):
    half = FC // 2
    rows = x_ref.shape[0]
    q1, q2, q3 = rows // 2, rows // 4, rows // 8
    n_units = 2 * n_f
    last_oth = OWN_FIRST + n_f - 1
    held = n_units - HELD

    ty = lax.axis_index("ty")
    t = lax.axis_index("tx")
    c = lax.rem(t, 2)
    xc = lax.rem(lax.div(t, 2), 2)
    yc = lax.div(t, 4)
    dev_c = (ty, t + 1 - 2 * c)
    dev_x = (ty, t + 2 - 4 * xc)
    dev_y = (ty, t + 4 - 8 * yc)
    dev_z = (1 - ty, t)
    own = pl.ds(mo(ty * rows, rows), rows)
    oth = pl.ds(mo((1 - ty) * rows, rows), rows)

    def remote(src, dst, ssem, rsem, dev):
        return pltpu.make_async_remote_copy(src_ref=src, dst_ref=dst, send_sem=ssem, recv_sem=rsem,
                                            device_id=dev, device_id_type=MESH)

    def f_of(j):
        return lax.rem(j + (n_f - OWN_FIRST), n_f)

    def oth_of(j):
        return lax.rem(lax.div(j + (n_f - OWN_FIRST), n_f), 2)

    def base_of(j):
        k = oth_of(j)
        return (ty + k - 2 * ty * k) * rows

    def fcols(j):
        return pl.ds(mo(f_of(j) * FC, FC), FC)

    def trows(j):
        return pl.ds(mo(base_of(j), rows), rows)

    def wcopy(k, i):
        cs = fcols(i)
        if k == 0:
            return pltpu.make_async_copy(wg_hbm.at[:, cs], wg.at[:, cs], wsem.at[0, i])
        if k == 1:
            return pltpu.make_async_copy(wu_hbm.at[:, cs], wu.at[:, cs], wsem.at[1, i])
        return pltpu.make_async_copy(wd_hbm.at[cs, :], wd.at[cs, :], wsem.at[2, i])

    in_dy = pltpu.make_async_copy(dy_hbm, dya_ref.at[own, :], isem.at[0])
    in_x = pltpu.make_async_copy(x_hbm, x_ref, isem.at[1])
    in_gain = pltpu.make_async_copy(gain_hbm, gain_ref, isem.at[2])
    in_x.start()
    in_dy.start()
    in_gain.start()
    for i in range(LEAD):
        wcopy(2, i).start()

    barrier = pltpu.get_barrier_semaphore()
    for o in range(1, 8):
        pl.semaphore_signal(barrier, inc=1, device_id=(ty, lax.rem(t + o, 8)), device_id_type=MESH)
    pl.semaphore_signal(barrier, inc=1, device_id=dev_z, device_id_type=MESH)

    def start_w(i, carry):
        wcopy(0, i).start()
        wcopy(1, i).start()

        @pl.when(i + LEAD < n_f)
        def _():
            wcopy(2, i + LEAD).start()
        return carry

    lax.fori_loop(0, n_f, start_w, 0)

    lane = lax.broadcasted_iota(jnp.int32, (rows, 128), 1)

    def pack_cols(c0, c1):
        both = jnp.where(lane == 0, c0, jnp.where(lane == 1, c1, 0.0))
        return both.T[0:8, :]

    def unpack_cols(packed):
        full = jnp.concatenate([packed, jnp.zeros((rows - 8, 128), jnp.float32)], axis=0).T
        return full[:, 0:1], full[:, 1:2]

    def send_stats(buf, ssem, rsem):
        for o in range(1, 8):
            remote(buf.at[t], buf.at[t], ssem.at[o], rsem.at[o], (ty, lax.rem(t + o, 8))).start()

    def total_stats(buf, ssem, rsem):
        for o in range(1, 8):
            q = lax.rem(t + 8 - o, 8)
            d = remote(buf.at[t], buf.at[q], ssem.at[o], rsem.at[o], (ty, q))
            d.wait_send()
            d.wait_recv()
        s = buf[0]
        for j in range(1, 8):
            s = s + buf[j]
        return unpack_cols(s)

    def seg(base, size):
        return pl.ds(mo(base, size), size)

    own_c = seg(c * q1, q1)
    oth_c = seg((1 - c) * q1, q1)
    keep1 = (seg(c * q1 + xc * q2, q2), seg(c * q1 + yc * q2, q2))
    send1 = (seg(c * q1 + (1 - xc) * q2, q2), seg(c * q1 + (1 - yc) * q2, q2))
    r_keep = (seg(yc * q3, q3), seg(xc * q3, q3))
    r_send = (seg((1 - yc) * q3, q3), seg((1 - xc) * q3, q3))
    colw = (slice(0, half), slice(half, FC))
    dev1, dev2 = (dev_x, dev_y), (dev_y, dev_x)
    g_c = (c * q1, (1 - c) * q1)
    g_keep1 = (c * q1 + xc * q2, c * q1 + yc * q2)
    g_send1 = (c * q1 + (1 - xc) * q2, c * q1 + (1 - yc) * q2)
    g_fin = (g_keep1[0] + yc * q3, g_keep1[1] + xc * q3)
    g_fin_n = (g_keep1[0] + (1 - yc) * q3, g_keep1[1] + (1 - xc) * q3)

    def gcols(j, r):
        return pl.ds(mo(f_of(j) * FC + r * half, half), half)

    def grows(j, off, size):
        return pl.ds(mo(base_of(j) + off, size), size)

    def ring(j):
        return lax.rem(j, RING)

    def d_copy(j):
        slot = lax.rem(j, P_SLOTS)
        return remote(part.at[slot, :, oth_c, :], dsum.at[slot], ds.at[ring(j)], dr.at[ring(j)], dev_c)

    def dd_copy(j):
        slot = lax.rem(j, L_SLOTS)
        return remote(part_d.at[slot, oth_c, :], dsum_d.at[slot], dds.at[ring(j)], ddr.at[ring(j)], dev_c)

    def p1_copy(j, r):
        return remote(part.at[lax.rem(j, P_SLOTS), :, send1[r], colw[r]], r1.at[j, r, 0:2],
                      p1s.at[r, ring(j)], p1r.at[r, ring(j)], dev1[r])

    def pd_copy(j, r):
        return remote(part_d.at[lax.rem(j, L_SLOTS), send1[r], colw[r]], r1.at[j, r, 2],
                      pds.at[r, ring(j)], pdr.at[r, ring(j)], dev1[r])

    def p2_copy(j, r):
        return remote(r1.at[j, r, :, r_send[r], :], r2.at[j, r], p2s.at[r, ring(j)], p2r.at[r, ring(j)], dev2[r])

    def g1_copy(j, r, off, lo):
        ref = gat.at[lo:3, grows(j, off[r], q3), gcols(j, r)]
        return remote(ref, ref, g1s.at[r, ring(j)], g1r.at[r, ring(j)], dev2[r])

    def g2_copy(j, r, off, lo):
        ref = gat.at[lo:3, grows(j, off[r], q2), gcols(j, r)]
        return remote(ref, ref, g2s.at[r, ring(j)], g2r.at[r, ring(j)], dev1[r])

    def gd_copy(j, off, lo):
        ref = gat.at[lo:3, grows(j, off, q1), fcols(j)]
        return remote(ref, ref, gds.at[ring(j)], gdr.at[ring(j)], dev_c)

    def a1_copy(k, r, off):
        ref = gat.at[0, grows(held + k, off[r], q3), gcols(held + k, r)]
        return remote(ref, ref, a1s.at[r, k], a1r.at[r, k], dev2[r])

    def a2_copy(k, r, off):
        ref = gat.at[0, grows(held + k, off[r], q2), gcols(held + k, r)]
        return remote(ref, ref, a2s.at[r, k], a2r.at[r, k], dev1[r])

    def ad_copy(k, off):
        ref = gat.at[0, grows(held + k, off, q1), fcols(held + k)]
        return remote(ref, ref, ads.at[k], adr.at[k], dev_c)

    def by_arrays(j, body):
        @pl.when(j < held)
        def _():
            body(0)

        @pl.when(j >= held)
        def _():
            body(1)

    def each_held(body):
        def one(k, carry):
            body(k)
            return carry

        lax.fori_loop(0, HELD, one, 0)

    def da_dot(j):
        part_d[lax.rem(j, L_SLOTS)] = contract_cols(dya_ref[trows(j), :], wd[fcols(j), :])

    def da_product(j):
        da_dot(j)
        dd_copy(j).start()

    def da_pair_sum(j):
        dd_copy(j).wait_recv()
        slot = lax.rem(j, L_SLOTS)
        part_d[slot, own_c, :] = part_d[slot, own_c, :] + dsum_d[slot]
        for r in range(2):
            pd_copy(j, r).start()

    in_dy.wait()
    wcopy(2, 0).wait()
    da_dot(0)
    pl.semaphore_wait(barrier, 8)
    dd_copy(0).start()
    in_x.wait()
    x_own = x_ref[...].astype(jnp.float32)
    st[t] = pack_cols(jnp.sum(x_own, axis=1, keepdims=True), jnp.sum(x_own * x_own, axis=1, keepdims=True))
    send_stats(st, ss, sr)
    zdy = remote(dya_ref.at[own, :], dya_ref.at[own, :], zs.at[0], zr.at[0], dev_z)
    zdy.start()
    for i in range(1, 3):
        wcopy(2, i).wait()
        da_product(i)
    for i in range(LEAD):
        da_pair_sum(i)
        if i + 3 < LEAD:
            wcopy(2, i + 3).wait()
            da_product(i + 3)
    in_gain.wait()
    acc[...] = jnp.zeros_like(acc)

    gain = gain_ref[...]
    c0, c1 = total_stats(st, ss, sr)
    mean_x = c0 / d_model
    inv_std = lax.rsqrt(c1 / d_model - mean_x * mean_x + LN_EPS)
    xhat = (x_ref[...].astype(jnp.float32) - mean_x) * inv_std
    xh[...] = xhat
    h_ref[own, :] = (gain * xhat).astype(jnp.bfloat16)

    def h_copy(block):
        return remote(h_ref.at[own, :], h_ref.at[block, :], zs.at[1], zr.at[1], dev_z)

    h_copy(own).start()

    z_sum = remote(acc.at[1], zin, zs.at[2], zr.at[2], dev_z)

    def step(i, carry):
        @pl.when(jnp.logical_and(i >= P_SLOTS, i < n_units + P_SLOTS))
        def _():
            j = i - P_SLOTS
            d_copy(j).wait_send()
            dd_copy(j).wait_send()
            for r in range(2):
                p1_copy(j, r).wait_send()
                pd_copy(j, r).wait_send()

        @pl.when(i < n_f)
        def _():
            wcopy(0, i).wait()
            wcopy(1, i).wait()

        @pl.when(i + LEAD < n_f)
        def _():
            wcopy(2, i + LEAD).wait()

        @pl.when(i == OWN_FIRST - LEAD)
        def _():
            remote(dya_ref.at[own, :], dya_ref.at[oth, :], zs.at[0], zr.at[0], dev_z).wait_recv()

        @pl.when(i == OWN_FIRST)
        def _():
            h_copy(oth).wait_recv()
            h_t[...] = h_ref[...].T

        @pl.when(i < n_units)
        def _():
            cs = fcols(i)
            slot = lax.rem(i, P_SLOTS)
            h = h_ref[trows(i), :]
            part[slot, 0] = jnp.dot(h, wg[:, cs], preferred_element_type=jnp.float32)
            part[slot, 1] = jnp.dot(h, wu[:, cs], preferred_element_type=jnp.float32)
            d_copy(i).start()

        @pl.when(i + LEAD < n_units)
        def _():
            da_product(i + LEAD)

        @pl.when(jnp.logical_and(i >= STAGES[0], i < n_units + STAGES[0]))
        def _():
            j = i - STAGES[0]
            d_copy(j).wait_recv()
            slot = lax.rem(j, P_SLOTS)
            for k in range(2):
                part[slot, k, own_c, :] = part[slot, k, own_c, :] + dsum[slot, k]
            for r in range(2):
                p1_copy(j, r).start()

            @pl.when(j + LEAD < n_units)
            def _():
                da_pair_sum(j + LEAD)

        @pl.when(jnp.logical_and(i >= STAGES[1], i < n_units + STAGES[1]))
        def _():
            j = i - STAGES[1]
            slot = lax.rem(j, P_SLOTS)
            for r in range(2):
                pd_copy(j, r).wait_recv()
                p1_copy(j, r).wait_recv()
                for k in range(2):
                    r1[j, r, k] = r1[j, r, k] + part[slot, k, keep1[r], colw[r]]
                r1[j, r, 2] = r1[j, r, 2] + part_d[lax.rem(j, L_SLOTS), keep1[r], colw[r]]
                p2_copy(j, r).start()

        @pl.when(jnp.logical_and(i >= STAGES[2], i < n_units + STAGES[2]))
        def _():
            j = i - STAGES[2]
            for r in range(2):
                p2_copy(j, r).wait_recv()
                u = r1[j, r, 0, r_keep[r], :] + r2[j, r, 0]
                v = r1[j, r, 1, r_keep[r], :] + r2[j, r, 1]
                da = r1[j, r, 2, r_keep[r], :] + r2[j, r, 2]
                sig = jax.nn.sigmoid(u)
                swish = u * sig
                cs = gcols(j, r)
                rs = grows(j, g_fin[r], q3)
                gat[0, rs, cs] = (swish * v).astype(jnp.bfloat16)
                gat[1, rs, cs] = (da * v * sig * (1.0 + u * (1.0 - sig))).astype(jnp.bfloat16)
                gat[2, rs, cs] = (da * swish).astype(jnp.bfloat16)
            by_arrays(j, lambda lo: [g1_copy(j, r, g_fin, lo).start() for r in range(2)])

        @pl.when(jnp.logical_and(i >= STAGES[3], i < n_units + STAGES[3]))
        def _():
            j = i - STAGES[3]

            def forward(lo):
                for r in range(2):
                    g1_copy(j, r, g_fin_n, lo).wait_recv()
                    g2_copy(j, r, g_keep1, lo).start()

            by_arrays(j, forward)

        @pl.when(jnp.logical_and(i >= STAGES[4], i < n_units + STAGES[4]))
        def _():
            j = i - STAGES[4]

            def to_core(lo):
                for r in range(2):
                    g2_copy(j, r, g_send1, lo).wait_recv()
                gd_copy(j, g_c[0], lo).start()

            by_arrays(j, to_core)

        @pl.when(i >= STAGES[5])
        def _():
            j = i - STAGES[5]
            by_arrays(j, lambda lo: gd_copy(j, g_c[1], lo).wait_recv())
            cs = fcols(j)
            rs = trows(j)
            side = oth_of(j)

            @pl.when(j < held)
            def _():
                acc[side, 0] += jnp.dot(gat[0, rs, cs], wd[cs, :], preferred_element_type=jnp.float32)

            acc[side, 1] += contract_cols(gat[1, rs, cs], wg[:, cs]) + contract_cols(gat[2, rs, cs], wu[:, cs])

            def sent(lo):
                for r in range(2):
                    p2_copy(j, r).wait_send()
                    g1_copy(j, r, g_fin, lo).wait_send()
                    g2_copy(j, r, g_keep1, lo).wait_send()
                gd_copy(j, g_c[0], lo).wait_send()

            by_arrays(j, sent)

            @pl.when(j == last_oth)
            def _():
                z_sum.start()

        @pl.when(i == n_units - 1 + STAGES[2])
        def _():
            each_held(lambda k: [a1_copy(k, r, g_fin).start() for r in range(2)])

        @pl.when(i == n_units - 1 + STAGES[3])
        def _():
            def forward(k):
                for r in range(2):
                    a1_copy(k, r, g_fin_n).wait_recv()
                    a2_copy(k, r, g_keep1).start()

            each_held(forward)
        return carry

    lax.fori_loop(0, n_units + STAGES[5], step, 0)

    z_sum.wait()
    d_hnorm = acc[0, 1] + zin[1]
    e = d_hnorm * gain
    rb[t] = pack_cols(jnp.sum(e, axis=1, keepdims=True), jnp.sum(e * xh[...], axis=1, keepdims=True))
    send_stats(rb, bs, br)
    dgs[...] = jnp.broadcast_to(jnp.sum(d_hnorm * xh[...], axis=0, keepdims=True), dgs.shape)
    z_dg = remote(dgs, dgr, zs.at[3], zr.at[3], dev_z)
    z_dg.start()

    def to_core(k):
        for r in range(2):
            a2_copy(k, r, g_send1).wait_recv()
        ad_copy(k, g_c[0]).start()

    each_held(to_core)

    def m_product(k):
        ad_copy(k, g_c[1]).wait_recv()
        cs = fcols(held + k)
        acc[0, 0] += jnp.dot(gat[0, own, cs], wd[cs, :], preferred_element_type=jnp.float32)
        for r in range(2):
            a1_copy(k, r, g_fin).wait_send()
            a2_copy(k, r, g_keep1).wait_send()
        ad_copy(k, g_c[0]).wait_send()

    each_held(m_product)
    y_ref[...] = (x_ref[...].astype(jnp.float32) + (acc[0, 0] + zin[0])).astype(jnp.bfloat16)
    zdy.wait_send()
    h_copy(own).wait_send()
    c0, c1 = total_stats(rb, bs, br)
    dx_ln = inv_std * (e - c0 / d_model - xh[...] * (c1 / d_model))
    dx_ref[...] = (dya_ref[own, :].astype(jnp.float32) + dx_ln).astype(jnp.bfloat16)
    z_dg.wait()
    dg_ref[...] = dgs[0:1, :] + dgr[0:1, :]


def weight_grad_kernel(gat, h_t, dy_ref, y_in, dx_in, dg_in,
                       dwg_hbm, dwu_hbm, dwd_hbm, y_hbm, dx_hbm, dg_hbm, buf, bsem, ssem):
    n_blocks = gat.shape[2] // WB

    def out_copy(b, k):
        cs = pl.ds(mo(b * WB, WB), WB)
        dst = (dwg_hbm.at[:, cs], dwu_hbm.at[:, cs], dwd_hbm.at[cs, :])[k]
        slot = lax.rem(b, W_SLOTS)
        return pltpu.make_async_copy(buf.at[slot, k], dst, bsem.at[slot, k])

    def block(b, carry):
        cs = pl.ds(mo(b * WB, WB), WB)
        slot = lax.rem(b, W_SLOTS)
        for k in range(3):
            @pl.when(b >= W_SLOTS)
            def _():
                out_copy(b - W_SLOTS, k).wait()

            if k < 2:
                buf[slot, k] = jnp.dot(h_t[...], gat[k + 1, :, cs], preferred_element_type=jnp.float32)
            else:
                buf[slot, k] = contract_rows(gat[0, :, cs], dy_ref[...])
            out_copy(b, k).start()
        return carry

    lax.fori_loop(0, n_blocks, block, 0)
    small = [pltpu.make_async_copy(src, dst, ssem.at[k])
             for k, (src, dst) in enumerate(((y_in, y_hbm), (dx_in, dx_hbm), (dg_in, dg_hbm)))]
    for d in small:
        d.start()

    def drain(b, carry):
        for k in range(3):
            out_copy(b, k).wait()
        return carry

    lax.fori_loop(n_blocks - W_SLOTS, n_blocks, drain, 0)
    for d in small:
        d.wait()


def solution(mesh):
    tx_size = mesh.shape["tx"]
    ty_size = mesh.shape["ty"]

    def local_step(x_blk, dy_blk, gain_blk, w_gate_blk, w_up_blk, w_down_blk):
        rows, dl = x_blk.shape
        fl = w_gate_blk.shape[1]
        tok = rows * ty_size
        d_model = dl * tx_size
        n = fl // FC
        half = FC // 2
        f32, bf16 = jnp.float32, jnp.bfloat16
        anyspec = pl.BlockSpec(memory_space=pl.ANY)
        sem = pltpu.SemaphoreType.DMA
        vm = pl.BlockSpec(memory_space=pltpu.VMEM)
        S = jax.ShapeDtypeStruct
        V = pltpu.VMEM
        small = [((rows, dl), bf16), ((rows, dl), bf16), ((1, dl), f32)]
        outs = pl.pallas_call(
            functools.partial(branch_kernel, d_model, n),
            out_shape=[V((3, tok, fl), bf16), V((dl, tok), bf16), V((tok, dl), bf16)] + [V(*s) for s in small],
            in_specs=[anyspec] * 6,
            out_specs=[vm] * 6,
            scratch_shapes=[
                V((rows, dl), bf16), V((1, dl), f32), V((tok, dl), bf16),
                V((dl, fl), bf16), V((dl, fl), bf16), V((fl, dl), bf16),
                V((rows, dl), f32),
                V((P_SLOTS, 2, rows, FC), f32), V((L_SLOTS, rows, FC), f32),
                V((P_SLOTS, 2, rows // 2, FC), f32), V((L_SLOTS, rows // 2, FC), f32),
                V((2 * n, 2, 3, rows // 4, half), f32), V((2 * n, 2, 3, rows // 8, half), f32),
                V((2, 2, rows, dl), f32), V((2, rows, dl), f32),
                V((8, 8, 128), f32), V((8, 8, 128), f32), V((8, dl), f32), V((8, dl), f32),
                sem((3, n)), sem((3,)), sem((4,)), sem((4,)), sem((8,)), sem((8,)), sem((8,)), sem((8,)),
                sem((RING,)), sem((RING,)), sem((RING,)), sem((RING,)),
                *[sem((2, RING)) for _ in range(10)],
                sem((RING,)), sem((RING,)),
                *[sem((2, HELD)) for _ in range(4)], sem((HELD,)), sem((HELD,)),
            ],
            compiler_params=pltpu.CompilerParams(collective_id=0, has_side_effects=True, vmem_limit_bytes=VMEM_LIMIT),
            cost_estimate=pl.CostEstimate(flops=12 * tok * dl * fl, bytes_accessed=6 * dl * fl + 6 * tok * fl, transcendentals=0),
        )(x_blk, dy_blk, gain_blk[None, :], w_gate_blk, w_up_blk, w_down_blk)

        dwg, dwu, dwd, y_blk, dx_blk, dg = pl.pallas_call(
            weight_grad_kernel,
            out_shape=[S((dl, fl), f32)] * 2 + [S((fl, dl), f32)] + [S(*s) for s in small],
            in_specs=[vm] * 6,
            out_specs=[anyspec] * 6,
            scratch_shapes=[
                V((W_SLOTS, 3, dl, WB), f32), sem((W_SLOTS, 3)), sem((3,)),
            ],
            compiler_params=pltpu.CompilerParams(vmem_limit_bytes=VMEM_LIMIT),
            cost_estimate=pl.CostEstimate(flops=6 * tok * dl * fl, bytes_accessed=12 * dl * fl + 6 * tok * fl, transcendentals=0),
        )(*[pltpu.with_memory_space_constraint(o, pltpu.VMEM) for o in outs])
        return (y_blk, dx_blk, dwg, dwu, dwd, dg[0])

    return jax.shard_map(
        local_step, mesh=mesh,
        in_specs=(P("ty", "tx"), P("ty", "tx"), P("tx"), P("tx", "ty"), P("tx", "ty"), P("ty", "tx")),
        out_specs=(P("ty", "tx"), P("ty", "tx"), P("tx", "ty"), P("tx", "ty"), P("ty", "tx"), P("tx")),
        check_vma=False)
```

```python
import functools

import jax
import jax.numpy as jnp
from jax import lax
from jax.experimental import pallas as pl
from jax.experimental.pallas import tpu as pltpu
from jax.sharding import PartitionSpec as P

LN_EPS = 1e-6
MESH = pl.DeviceIdType.MESH
FC = 512
OWN_FIRST = 8
LEAD = 8
P_SLOTS = 4
L_SLOTS = LEAD + P_SLOTS
HELD = 8
RING = 16
STAGES = (1, 3, 5, 7, 9, 10)
W_SLOTS = 3
VMEM_LIMIT = 48 * 1024 * 1024


def contract_rows(left_op, right_op):
    return lax.dot_general(left_op, right_op, (((0,), (0,)), ((), ())), preferred_element_type=jnp.float32)


def contract_cols(left_op, right_op):
    return lax.dot_general(left_op, right_op, (((1,), (1,)), ((), ())), preferred_element_type=jnp.float32)


def mo(value, multiple):
    return pl.multiple_of(value, multiple)


def branch_kernel(d_model, n_f,
                  x_hbm, dy_hbm, gain_hbm, wg_hbm, wu_hbm, wd_hbm,
                  gat, h_t, dya_ref, y_ref, dx_ref, dg_ref,
                  x_ref, gain_ref, h_ref,
                  wg, wu, wd, xh, part, part_d, dsum, dsum_d, r1, r2, acc, zin, st, rb, dgs, dgr,
                  wsem, isem, zs, zr, ss, sr, bs, br, ds, dr, dds, ddr, p1s, p1r, pds, pdr, p2s, p2r,
                  g1s, g1r, g2s, g2r, gds, gdr, a1s, a1r, a2s, a2r, ads, adr):
    half = FC // 2
    rows = x_ref.shape[0]
    q1, q2, q3 = rows // 2, rows // 4, rows // 8
    n_units = 2 * n_f
    last_oth = OWN_FIRST + n_f - 1
    held = n_units - HELD

    ty = lax.axis_index("ty")
    t = lax.axis_index("tx")
    c = lax.rem(t, 2)
    xc = lax.rem(lax.div(t, 2), 2)
    yc = lax.div(t, 4)
    dev_c = (ty, t + 1 - 2 * c)
    dev_x = (ty, t + 2 - 4 * xc)
    dev_y = (ty, t + 4 - 8 * yc)
    dev_z = (1 - ty, t)
    own = pl.ds(mo(ty * rows, rows), rows)
    oth = pl.ds(mo((1 - ty) * rows, rows), rows)

    def remote(src, dst, ssem, rsem, dev):
        return pltpu.make_async_remote_copy(src_ref=src, dst_ref=dst, send_sem=ssem, recv_sem=rsem,
                                            device_id=dev, device_id_type=MESH)

    def f_of(j):
        return lax.rem(j + (n_f - OWN_FIRST), n_f)

    def oth_of(j):
        return lax.rem(lax.div(j + (n_f - OWN_FIRST), n_f), 2)

    def base_of(j):
        k = oth_of(j)
        return (ty + k - 2 * ty * k) * rows

    def fcols(j):
        return pl.ds(mo(f_of(j) * FC, FC), FC)

    def rcols(j, r):
        return pl.ds(mo(f_of(j) * FC + r * half, half), half)

    def trows(j):
        return pl.ds(mo(base_of(j), rows), rows)

    def wcopy(k, i):
        cs = fcols(i)
        if k == 0:
            return pltpu.make_async_copy(wg_hbm.at[:, cs], wg.at[:, cs], wsem.at[0, i])
        if k == 1:
            return pltpu.make_async_copy(wu_hbm.at[:, cs], wu.at[:, cs], wsem.at[1, i])
        return pltpu.make_async_copy(wd_hbm.at[cs, :], wd.at[cs, :], wsem.at[2, i])

    in_dy = pltpu.make_async_copy(dy_hbm, dya_ref.at[own, :], isem.at[0])
    in_x = pltpu.make_async_copy(x_hbm, x_ref, isem.at[1])
    in_gain = pltpu.make_async_copy(gain_hbm, gain_ref, isem.at[2])
    in_x.start()
    in_dy.start()
    in_gain.start()
    for i in range(LEAD):
        wcopy(2, i).start()

    barrier = pltpu.get_barrier_semaphore()
    for o in range(1, 8):
        pl.semaphore_signal(barrier, inc=1, device_id=(ty, lax.rem(t + o, 8)), device_id_type=MESH)
    pl.semaphore_signal(barrier, inc=1, device_id=dev_z, device_id_type=MESH)

    def start_w(i, carry):
        wcopy(0, i).start()
        wcopy(1, i).start()

        @pl.when(i + LEAD < n_f)
        def _():
            wcopy(2, i + LEAD).start()
        return carry

    lax.fori_loop(0, n_f, start_w, 0)

    lane = lax.broadcasted_iota(jnp.int32, (rows, 128), 1)

    def pack_cols(c0, c1):
        both = jnp.where(lane == 0, c0, jnp.where(lane == 1, c1, 0.0))
        return both.T[0:8, :]

    def unpack_cols(packed):
        full = jnp.concatenate([packed, jnp.zeros((rows - 8, 128), jnp.float32)], axis=0).T
        return full[:, 0:1], full[:, 1:2]

    def send_stats(buf, ssem, rsem):
        for o in range(1, 8):
            remote(buf.at[t], buf.at[t], ssem.at[o], rsem.at[o], (ty, lax.rem(t + o, 8))).start()

    def total_stats(buf, ssem, rsem):
        for o in range(1, 8):
            q = lax.rem(t + 8 - o, 8)
            d = remote(buf.at[t], buf.at[q], ssem.at[o], rsem.at[o], (ty, q))
            d.wait_send()
            d.wait_recv()
        s = buf[0]
        for j in range(1, 8):
            s = s + buf[j]
        return unpack_cols(s)

    def seg(base, size):
        return pl.ds(mo(base, size), size)

    own_c = seg(c * q1, q1)
    oth_c = seg((1 - c) * q1, q1)
    keep1 = (seg(c * q1 + xc * q2, q2), seg(c * q1 + yc * q2, q2))
    send1 = (seg(c * q1 + (1 - xc) * q2, q2), seg(c * q1 + (1 - yc) * q2, q2))
    r_keep = (seg(yc * q3, q3), seg(xc * q3, q3))
    r_send = (seg((1 - yc) * q3, q3), seg((1 - xc) * q3, q3))
    lanes = [slice(k * half, (k + 1) * half) for k in range(3)]
    dev1, dev2 = (dev_x, dev_y), (dev_y, dev_x)
    g_c = (c * q1, (1 - c) * q1)
    g_keep1 = (c * q1 + xc * q2, c * q1 + yc * q2)
    g_send1 = (c * q1 + (1 - xc) * q2, c * q1 + (1 - yc) * q2)
    g_fin = (g_keep1[0] + yc * q3, g_keep1[1] + xc * q3)
    g_fin_n = (g_keep1[0] + (1 - yc) * q3, g_keep1[1] + (1 - xc) * q3)

    def grows(j, off, size):
        return pl.ds(mo(base_of(j) + off, size), size)

    def ring(j):
        return lax.rem(j, RING)

    def d_copy(j):
        slot = lax.rem(j, P_SLOTS)
        return remote(part.at[slot, :, :, oth_c, :], dsum.at[slot], ds.at[ring(j)], dr.at[ring(j)], dev_c)

    def dd_copy(j):
        slot = lax.rem(j, L_SLOTS)
        return remote(part_d.at[slot, :, oth_c, :], dsum_d.at[slot], dds.at[ring(j)], ddr.at[ring(j)], dev_c)

    def p1_copy(j, r):
        return remote(part.at[lax.rem(j, P_SLOTS), r, :, send1[r], :], r1.at[j, r, 0:2],
                      p1s.at[r, ring(j)], p1r.at[r, ring(j)], dev1[r])

    def pd_copy(j, r):
        return remote(part_d.at[lax.rem(j, L_SLOTS), r, send1[r], :], r1.at[j, r, 2],
                      pds.at[r, ring(j)], pdr.at[r, ring(j)], dev1[r])

    def p2_copy(j, r):
        return remote(r1.at[j, r, :, r_send[r], :], r2.at[j, r], p2s.at[r, ring(j)], p2r.at[r, ring(j)], dev2[r])

    def g1_copy(j, r, off, lo):
        ref = gat.at[f_of(j), r, grows(j, off[r], q3), lo * half:]
        return remote(ref, ref, g1s.at[r, ring(j)], g1r.at[r, ring(j)], dev2[r])

    def g2_copy(j, r, off, lo):
        ref = gat.at[f_of(j), r, grows(j, off[r], q2), lo * half:]
        return remote(ref, ref, g2s.at[r, ring(j)], g2r.at[r, ring(j)], dev1[r])

    def gd_copy(j, off, lo):
        ref = gat.at[f_of(j), :, grows(j, off, q1), lo * half:]
        return remote(ref, ref, gds.at[ring(j)], gdr.at[ring(j)], dev_c)

    def a1_copy(k, r, off):
        ref = gat.at[f_of(held + k), r, grows(held + k, off[r], q3), lanes[0]]
        return remote(ref, ref, a1s.at[r, k], a1r.at[r, k], dev2[r])

    def a2_copy(k, r, off):
        ref = gat.at[f_of(held + k), r, grows(held + k, off[r], q2), lanes[0]]
        return remote(ref, ref, a2s.at[r, k], a2r.at[r, k], dev1[r])

    def ad_copy(k, off):
        ref = gat.at[f_of(held + k), :, grows(held + k, off, q1), lanes[0]]
        return remote(ref, ref, ads.at[k], adr.at[k], dev_c)

    def by_arrays(j, body):
        @pl.when(j < held)
        def _():
            body(0)

        @pl.when(j >= held)
        def _():
            body(1)

    def each_held(body):
        def one(k, carry):
            body(k)
            return carry

        lax.fori_loop(0, HELD, one, 0)

    def da_dot(j):
        for r in range(2):
            part_d[lax.rem(j, L_SLOTS), r] = contract_cols(dya_ref[trows(j), :], wd[rcols(j, r), :])

    def da_product(j):
        da_dot(j)
        dd_copy(j).start()

    def da_pair_sum(j):
        dd_copy(j).wait_recv()
        slot = lax.rem(j, L_SLOTS)
        for r in range(2):
            part_d[slot, r, own_c, :] = part_d[slot, r, own_c, :] + dsum_d[slot, r]
            pd_copy(j, r).start()

    in_dy.wait()
    wcopy(2, 0).wait()
    da_dot(0)
    pl.semaphore_wait(barrier, 8)
    dd_copy(0).start()
    in_x.wait()
    x_own = x_ref[...].astype(jnp.float32)
    st[t] = pack_cols(jnp.sum(x_own, axis=1, keepdims=True), jnp.sum(x_own * x_own, axis=1, keepdims=True))
    send_stats(st, ss, sr)
    zdy = remote(dya_ref.at[own, :], dya_ref.at[own, :], zs.at[0], zr.at[0], dev_z)
    zdy.start()
    for i in range(1, 3):
        wcopy(2, i).wait()
        da_product(i)
    for i in range(LEAD):
        da_pair_sum(i)
        if i + 3 < LEAD:
            wcopy(2, i + 3).wait()
            da_product(i + 3)
    in_gain.wait()
    acc[...] = jnp.zeros_like(acc)

    gain = gain_ref[...]
    c0, c1 = total_stats(st, ss, sr)
    mean_x = c0 / d_model
    inv_std = lax.rsqrt(c1 / d_model - mean_x * mean_x + LN_EPS)
    xhat = (x_ref[...].astype(jnp.float32) - mean_x) * inv_std
    xh[...] = xhat
    h_ref[own, :] = (gain * xhat).astype(jnp.bfloat16)

    def h_copy(block):
        return remote(h_ref.at[own, :], h_ref.at[block, :], zs.at[1], zr.at[1], dev_z)

    h_copy(own).start()

    def m_part(f, rs, j):
        return sum(jnp.dot(gat[f, r, rs, lanes[0]], wd[rcols(j, r), :], preferred_element_type=jnp.float32) for r in range(2))

    z_sum = remote(acc.at[1], zin, zs.at[2], zr.at[2], dev_z)

    def step(i, carry):
        @pl.when(jnp.logical_and(i >= P_SLOTS, i < n_units + P_SLOTS))
        def _():
            j = i - P_SLOTS
            d_copy(j).wait_send()
            dd_copy(j).wait_send()
            for r in range(2):
                p1_copy(j, r).wait_send()
                pd_copy(j, r).wait_send()

        @pl.when(i < n_f)
        def _():
            wcopy(0, i).wait()
            wcopy(1, i).wait()

        @pl.when(i + LEAD < n_f)
        def _():
            wcopy(2, i + LEAD).wait()

        @pl.when(i == OWN_FIRST - LEAD)
        def _():
            remote(dya_ref.at[own, :], dya_ref.at[oth, :], zs.at[0], zr.at[0], dev_z).wait_recv()

        @pl.when(i == OWN_FIRST)
        def _():
            h_copy(oth).wait_recv()
            h_t[...] = h_ref[...].T

        @pl.when(i < n_units)
        def _():
            slot = lax.rem(i, P_SLOTS)
            h = h_ref[trows(i), :]
            for r in range(2):
                part[slot, r, 0] = jnp.dot(h, wg[:, rcols(i, r)], preferred_element_type=jnp.float32)
                part[slot, r, 1] = jnp.dot(h, wu[:, rcols(i, r)], preferred_element_type=jnp.float32)
            d_copy(i).start()

        @pl.when(i + LEAD < n_units)
        def _():
            da_product(i + LEAD)

        @pl.when(jnp.logical_and(i >= STAGES[0], i < n_units + STAGES[0]))
        def _():
            j = i - STAGES[0]
            d_copy(j).wait_recv()
            slot = lax.rem(j, P_SLOTS)
            for r in range(2):
                for k in range(2):
                    part[slot, r, k, own_c, :] = part[slot, r, k, own_c, :] + dsum[slot, r, k]
                p1_copy(j, r).start()

            @pl.when(j + LEAD < n_units)
            def _():
                da_pair_sum(j + LEAD)

        @pl.when(jnp.logical_and(i >= STAGES[1], i < n_units + STAGES[1]))
        def _():
            j = i - STAGES[1]
            slot = lax.rem(j, P_SLOTS)
            for r in range(2):
                pd_copy(j, r).wait_recv()
                p1_copy(j, r).wait_recv()
                for k in range(2):
                    r1[j, r, k] = r1[j, r, k] + part[slot, r, k, keep1[r], :]
                r1[j, r, 2] = r1[j, r, 2] + part_d[lax.rem(j, L_SLOTS), r, keep1[r], :]
                p2_copy(j, r).start()

        @pl.when(jnp.logical_and(i >= STAGES[2], i < n_units + STAGES[2]))
        def _():
            j = i - STAGES[2]
            for r in range(2):
                p2_copy(j, r).wait_recv()
                u = r1[j, r, 0, r_keep[r], :] + r2[j, r, 0]
                v = r1[j, r, 1, r_keep[r], :] + r2[j, r, 1]
                da = r1[j, r, 2, r_keep[r], :] + r2[j, r, 2]
                sig = jax.nn.sigmoid(u)
                swish = u * sig
                f = f_of(j)
                rs = grows(j, g_fin[r], q3)
                gat[f, r, rs, lanes[0]] = (swish * v).astype(jnp.bfloat16)
                gat[f, r, rs, lanes[1]] = (da * v * sig * (1.0 + u * (1.0 - sig))).astype(jnp.bfloat16)
                gat[f, r, rs, lanes[2]] = (da * swish).astype(jnp.bfloat16)
            by_arrays(j, lambda lo: [g1_copy(j, r, g_fin, lo).start() for r in range(2)])

        @pl.when(jnp.logical_and(i >= STAGES[3], i < n_units + STAGES[3]))
        def _():
            j = i - STAGES[3]

            def forward(lo):
                for r in range(2):
                    g1_copy(j, r, g_fin_n, lo).wait_recv()
                    g2_copy(j, r, g_keep1, lo).start()

            by_arrays(j, forward)

        @pl.when(jnp.logical_and(i >= STAGES[4], i < n_units + STAGES[4]))
        def _():
            j = i - STAGES[4]

            def to_core(lo):
                for r in range(2):
                    g2_copy(j, r, g_send1, lo).wait_recv()
                gd_copy(j, g_c[0], lo).start()

            by_arrays(j, to_core)

        @pl.when(i >= STAGES[5])
        def _():
            j = i - STAGES[5]
            by_arrays(j, lambda lo: gd_copy(j, g_c[1], lo).wait_recv())
            f = f_of(j)
            rs = trows(j)
            side = oth_of(j)

            @pl.when(j < held)
            def _():
                acc[side, 0] += m_part(f, rs, j)

            acc[side, 1] += sum(contract_cols(gat[f, r, rs, lanes[1]], wg[:, rcols(j, r)])
                                + contract_cols(gat[f, r, rs, lanes[2]], wu[:, rcols(j, r)]) for r in range(2))

            def sent(lo):
                for r in range(2):
                    p2_copy(j, r).wait_send()
                    g1_copy(j, r, g_fin, lo).wait_send()
                    g2_copy(j, r, g_keep1, lo).wait_send()
                gd_copy(j, g_c[0], lo).wait_send()

            by_arrays(j, sent)

            @pl.when(j == last_oth)
            def _():
                z_sum.start()

        @pl.when(i == n_units - 1 + STAGES[2])
        def _():
            each_held(lambda k: [a1_copy(k, r, g_fin).start() for r in range(2)])

        @pl.when(i == n_units - 1 + STAGES[3])
        def _():
            def forward(k):
                for r in range(2):
                    a1_copy(k, r, g_fin_n).wait_recv()
                    a2_copy(k, r, g_keep1).start()

            each_held(forward)
        return carry

    lax.fori_loop(0, n_units + STAGES[5], step, 0)

    z_sum.wait()
    d_hnorm = acc[0, 1] + zin[1]
    e = d_hnorm * gain
    rb[t] = pack_cols(jnp.sum(e, axis=1, keepdims=True), jnp.sum(e * xh[...], axis=1, keepdims=True))
    send_stats(rb, bs, br)
    dgs[...] = jnp.broadcast_to(jnp.sum(d_hnorm * xh[...], axis=0, keepdims=True), dgs.shape)
    z_dg = remote(dgs, dgr, zs.at[3], zr.at[3], dev_z)
    z_dg.start()

    def to_core(k):
        for r in range(2):
            a2_copy(k, r, g_send1).wait_recv()
        ad_copy(k, g_c[0]).start()

    each_held(to_core)

    def m_product(k):
        ad_copy(k, g_c[1]).wait_recv()
        acc[0, 0] += m_part(f_of(held + k), own, held + k)
        for r in range(2):
            a1_copy(k, r, g_fin).wait_send()
            a2_copy(k, r, g_keep1).wait_send()
        ad_copy(k, g_c[0]).wait_send()

    each_held(m_product)
    y_ref[...] = (x_ref[...].astype(jnp.float32) + (acc[0, 0] + zin[0])).astype(jnp.bfloat16)
    zdy.wait_send()
    h_copy(own).wait_send()
    c0, c1 = total_stats(rb, bs, br)
    dx_ln = inv_std * (e - c0 / d_model - xh[...] * (c1 / d_model))
    dx_ref[...] = (dya_ref[own, :].astype(jnp.float32) + dx_ln).astype(jnp.bfloat16)
    z_dg.wait()
    dg_ref[...] = dgs[0:1, :] + dgr[0:1, :]


def weight_grad_kernel(gat, h_t, dy_ref, y_in, dx_in, dg_in,
                       dwg_hbm, dwu_hbm, dwd_hbm, y_hbm, dx_hbm, dg_hbm, buf, bsem, ssem):
    n_blocks, _, _, width = gat.shape
    half = width // 3
    WB = 2 * half

    def out_copy(b, k):
        cs = pl.ds(mo(b * WB, WB), WB)
        dst = (dwg_hbm.at[:, cs], dwu_hbm.at[:, cs], dwd_hbm.at[cs, :])[k]
        slot = lax.rem(b, W_SLOTS)
        return pltpu.make_async_copy(buf.at[slot, k], dst, bsem.at[slot, k])

    def block(b, carry):
        slot = lax.rem(b, W_SLOTS)
        for k in range(3):
            @pl.when(b >= W_SLOTS)
            def _():
                out_copy(b - W_SLOTS, k).wait()

            for r in range(2):
                rs = slice(r * half, (r + 1) * half)
                src = gat[b, r, :, (k + 1) % 3 * half:((k + 1) % 3 + 1) * half]
                if k < 2:
                    buf[slot, k, :, rs] = jnp.dot(h_t[...], src, preferred_element_type=jnp.float32)
                else:
                    buf[slot, k, rs, :] = contract_rows(src, dy_ref[...])
            out_copy(b, k).start()
        return carry

    lax.fori_loop(0, n_blocks, block, 0)
    small = [pltpu.make_async_copy(src, dst, ssem.at[k])
             for k, (src, dst) in enumerate(((y_in, y_hbm), (dx_in, dx_hbm), (dg_in, dg_hbm)))]
    for d in small:
        d.start()

    def drain(b, carry):
        for k in range(3):
            out_copy(b, k).wait()
        return carry

    lax.fori_loop(n_blocks - W_SLOTS, n_blocks, drain, 0)
    for d in small:
        d.wait()


def solution(mesh):
    tx_size = mesh.shape["tx"]
    ty_size = mesh.shape["ty"]

    def local_step(x_blk, dy_blk, gain_blk, w_gate_blk, w_up_blk, w_down_blk):
        rows, dl = x_blk.shape
        fl = w_gate_blk.shape[1]
        tok = rows * ty_size
        d_model = dl * tx_size
        n = fl // FC
        half = FC // 2
        f32, bf16 = jnp.float32, jnp.bfloat16
        anyspec = pl.BlockSpec(memory_space=pl.ANY)
        sem = pltpu.SemaphoreType.DMA
        vm = pl.BlockSpec(memory_space=pltpu.VMEM)
        S = jax.ShapeDtypeStruct
        V = pltpu.VMEM
        small = [((rows, dl), bf16), ((rows, dl), bf16), ((1, dl), f32)]
        outs = pl.pallas_call(
            functools.partial(branch_kernel, d_model, n),
            out_shape=[V((n, 2, tok, 3 * half), bf16), V((dl, tok), bf16), V((tok, dl), bf16)] + [V(*s) for s in small],
            in_specs=[anyspec] * 6,
            out_specs=[vm] * 6,
            scratch_shapes=[
                V((rows, dl), bf16), V((1, dl), f32), V((tok, dl), bf16),
                V((dl, fl), bf16), V((dl, fl), bf16), V((fl, dl), bf16),
                V((rows, dl), f32),
                V((P_SLOTS, 2, 2, rows, half), f32), V((L_SLOTS, 2, rows, half), f32),
                V((P_SLOTS, 2, 2, rows // 2, half), f32), V((L_SLOTS, 2, rows // 2, half), f32),
                V((2 * n, 2, 3, rows // 4, half), f32), V((2 * n, 2, 3, rows // 8, half), f32),
                V((2, 2, rows, dl), f32), V((2, rows, dl), f32),
                V((8, 8, 128), f32), V((8, 8, 128), f32), V((8, dl), f32), V((8, dl), f32),
                sem((3, n)), sem((3,)), sem((4,)), sem((4,)), sem((8,)), sem((8,)), sem((8,)), sem((8,)),
                sem((RING,)), sem((RING,)), sem((RING,)), sem((RING,)),
                *[sem((2, RING)) for _ in range(10)],
                sem((RING,)), sem((RING,)),
                *[sem((2, HELD)) for _ in range(4)], sem((HELD,)), sem((HELD,)),
            ],
            compiler_params=pltpu.CompilerParams(collective_id=0, has_side_effects=True, vmem_limit_bytes=VMEM_LIMIT),
            cost_estimate=pl.CostEstimate(flops=12 * tok * dl * fl, bytes_accessed=6 * dl * fl + 6 * tok * fl, transcendentals=0),
        )(x_blk, dy_blk, gain_blk[None, :], w_gate_blk, w_up_blk, w_down_blk)

        dwg, dwu, dwd, y_blk, dx_blk, dg = pl.pallas_call(
            weight_grad_kernel,
            out_shape=[S((dl, fl), f32)] * 2 + [S((fl, dl), f32)] + [S(*s) for s in small],
            in_specs=[vm] * 6,
            out_specs=[anyspec] * 6,
            scratch_shapes=[
                V((W_SLOTS, 3, dl, FC), f32), sem((W_SLOTS, 3)), sem((3,)),
            ],
            compiler_params=pltpu.CompilerParams(vmem_limit_bytes=VMEM_LIMIT),
            cost_estimate=pl.CostEstimate(flops=6 * tok * dl * fl, bytes_accessed=12 * dl * fl + 6 * tok * fl, transcendentals=0),
        )(*[pltpu.with_memory_space_constraint(o, pltpu.VMEM) for o in outs])
        return (y_blk, dx_blk, dwg, dwu, dwd, dg[0])

    return jax.shard_map(
        local_step, mesh=mesh,
        in_specs=(P("ty", "tx"), P("ty", "tx"), P("tx"), P("tx", "ty"), P("tx", "ty"), P("ty", "tx")),
        out_specs=(P("ty", "tx"), P("ty", "tx"), P("tx", "ty"), P("tx", "ty"), P("ty", "tx"), P("tx")),
        check_vma=False)
```

```python
import functools

import jax
import jax.numpy as jnp
from jax import lax
from jax.experimental import pallas as pl
from jax.experimental.pallas import tpu as pltpu
from jax.sharding import PartitionSpec as P

LN_EPS = 1e-6
MESH = pl.DeviceIdType.MESH
FC = 1024
OWN_FIRST = 4
LEAD = 4
P_SLOTS = 3
D_SLOTS = 4
L_SLOTS = LEAD + P_SLOTS
HELD = 4
RING = 16
STAGES = (1, 2, 4, 6, 8, 9)
W_SLOTS = 3
VMEM_LIMIT = 49 * 1024 * 1024


def contract_rows(left_op, right_op):
    return lax.dot_general(left_op, right_op, (((0,), (0,)), ((), ())), preferred_element_type=jnp.float32)


def contract_cols(left_op, right_op):
    return lax.dot_general(left_op, right_op, (((1,), (1,)), ((), ())), preferred_element_type=jnp.float32)


def mo(value, multiple):
    return pl.multiple_of(value, multiple)


def branch_kernel(d_model, n_f,
                  x_hbm, dy_hbm, gain_hbm, wg_hbm, wu_hbm, wd_hbm,
                  gat, h_t, dya_ref, y_ref, dx_ref, dg_ref,
                  x_ref, gain_ref, h_ref,
                  wg, wu, wd, xh, part, part_d, dsum, dsum_d, r1, r2, acc, zin, st, rb, dgs, dgr,
                  wsem, isem, zs, zr, ss, sr, bs, br, ds, dr, dds, ddr, p1s, p1r, pds, pdr, p2s, p2r,
                  g1s, g1r, g2s, g2r, gds, gdr, a1s, a1r, a2s, a2r, ads, adr):
    half = FC // 2
    rows = x_ref.shape[0]
    q1, q2, q3 = rows // 2, rows // 4, rows // 8
    n_units = 2 * n_f
    last_oth = OWN_FIRST + n_f - 1
    held = n_units - HELD

    ty = lax.axis_index("ty")
    t = lax.axis_index("tx")
    c = lax.rem(t, 2)
    xc = lax.rem(lax.div(t, 2), 2)
    yc = lax.div(t, 4)
    dev_c = (ty, t + 1 - 2 * c)
    dev_x = (ty, t + 2 - 4 * xc)
    dev_y = (ty, t + 4 - 8 * yc)
    dev_z = (1 - ty, t)
    own = pl.ds(mo(ty * rows, rows), rows)
    oth = pl.ds(mo((1 - ty) * rows, rows), rows)

    def remote(src, dst, ssem, rsem, dev):
        return pltpu.make_async_remote_copy(src_ref=src, dst_ref=dst, send_sem=ssem, recv_sem=rsem,
                                            device_id=dev, device_id_type=MESH)

    def f_of(j):
        return lax.rem(j + (n_f - OWN_FIRST), n_f)

    def oth_of(j):
        return lax.rem(lax.div(j + (n_f - OWN_FIRST), n_f), 2)

    def base_of(j):
        k = oth_of(j)
        return (ty + k - 2 * ty * k) * rows

    def fcols(j):
        return pl.ds(mo(f_of(j) * FC, FC), FC)

    def rcols(j, r):
        return pl.ds(mo(f_of(j) * FC + r * half, half), half)

    def trows(j):
        return pl.ds(mo(base_of(j), rows), rows)

    def wcopy(k, i):
        cs = fcols(i)
        if k == 0:
            return pltpu.make_async_copy(wg_hbm.at[:, cs], wg.at[:, cs], wsem.at[0, i])
        if k == 1:
            return pltpu.make_async_copy(wu_hbm.at[:, cs], wu.at[:, cs], wsem.at[1, i])
        return pltpu.make_async_copy(wd_hbm.at[cs, :], wd.at[cs, :], wsem.at[2, i])

    in_dy = pltpu.make_async_copy(dy_hbm, dya_ref.at[own, :], isem.at[0])
    in_x = pltpu.make_async_copy(x_hbm, x_ref, isem.at[1])
    in_gain = pltpu.make_async_copy(gain_hbm, gain_ref, isem.at[2])
    in_x.start()
    in_dy.start()
    in_gain.start()
    for i in range(LEAD):
        wcopy(2, i).start()

    barrier = pltpu.get_barrier_semaphore()
    for o in range(1, 8):
        pl.semaphore_signal(barrier, inc=1, device_id=(ty, lax.rem(t + o, 8)), device_id_type=MESH)
    pl.semaphore_signal(barrier, inc=1, device_id=dev_z, device_id_type=MESH)

    def start_w(i, carry):
        wcopy(0, i).start()
        wcopy(1, i).start()

        @pl.when(i + LEAD < n_f)
        def _():
            wcopy(2, i + LEAD).start()
        return carry

    lax.fori_loop(0, n_f, start_w, 0)

    lane = lax.broadcasted_iota(jnp.int32, (rows, 128), 1)

    def pack_cols(c0, c1):
        both = jnp.where(lane == 0, c0, jnp.where(lane == 1, c1, 0.0))
        return both.T[0:8, :]

    def unpack_cols(packed):
        full = jnp.concatenate([packed, jnp.zeros((rows - 8, 128), jnp.float32)], axis=0).T
        return full[:, 0:1], full[:, 1:2]

    def send_stats(buf, ssem, rsem):
        for o in range(1, 8):
            remote(buf.at[t], buf.at[t], ssem.at[o], rsem.at[o], (ty, lax.rem(t + o, 8))).start()

    def total_stats(buf, ssem, rsem):
        for o in range(1, 8):
            q = lax.rem(t + 8 - o, 8)
            d = remote(buf.at[t], buf.at[q], ssem.at[o], rsem.at[o], (ty, q))
            d.wait_send()
            d.wait_recv()
        s = buf[0]
        for j in range(1, 8):
            s = s + buf[j]
        return unpack_cols(s)

    def seg(base, size):
        return pl.ds(mo(base, size), size)

    own_c = seg(c * q1, q1)
    oth_c = seg((1 - c) * q1, q1)
    keep1 = (seg(c * q1 + xc * q2, q2), seg(c * q1 + yc * q2, q2))
    send1 = (seg(c * q1 + (1 - xc) * q2, q2), seg(c * q1 + (1 - yc) * q2, q2))
    r_keep = (seg(yc * q3, q3), seg(xc * q3, q3))
    r_send = (seg((1 - yc) * q3, q3), seg((1 - xc) * q3, q3))
    lanes = [slice(k * half, (k + 1) * half) for k in range(3)]
    dev1, dev2 = (dev_x, dev_y), (dev_y, dev_x)
    g_c = (c * q1, (1 - c) * q1)
    g_keep1 = (c * q1 + xc * q2, c * q1 + yc * q2)
    g_send1 = (c * q1 + (1 - xc) * q2, c * q1 + (1 - yc) * q2)
    g_fin = (g_keep1[0] + yc * q3, g_keep1[1] + xc * q3)
    g_fin_n = (g_keep1[0] + (1 - yc) * q3, g_keep1[1] + (1 - xc) * q3)

    def grows(j, off, size):
        return pl.ds(mo(base_of(j) + off, size), size)

    def ring(j):
        return lax.rem(j, RING)

    def d_copy(j):
        slot = lax.rem(j, P_SLOTS)
        return remote(part.at[slot, :, :, oth_c, :], dsum.at[lax.rem(j, D_SLOTS)], ds.at[ring(j)], dr.at[ring(j)], dev_c)

    def dd_copy(j):
        slot = lax.rem(j, L_SLOTS)
        return remote(part_d.at[slot, :, oth_c, :], dsum_d.at[slot], dds.at[ring(j)], ddr.at[ring(j)], dev_c)

    def p1_copy(j, r):
        return remote(part.at[lax.rem(j, P_SLOTS), r, :, send1[r], :], r1.at[j, r, 0:2],
                      p1s.at[r, ring(j)], p1r.at[r, ring(j)], dev1[r])

    def pd_copy(j, r):
        return remote(part_d.at[lax.rem(j, L_SLOTS), r, send1[r], :], r1.at[j, r, 2],
                      pds.at[r, ring(j)], pdr.at[r, ring(j)], dev1[r])

    def p2_copy(j, r):
        return remote(r1.at[j, r, :, r_send[r], :], r2.at[j, r], p2s.at[r, ring(j)], p2r.at[r, ring(j)], dev2[r])

    def g1_copy(j, r, off, lo):
        ref = gat.at[f_of(j), r, grows(j, off[r], q3), lo * half:]
        return remote(ref, ref, g1s.at[r, ring(j)], g1r.at[r, ring(j)], dev2[r])

    def g2_copy(j, r, off, lo):
        ref = gat.at[f_of(j), r, grows(j, off[r], q2), lo * half:]
        return remote(ref, ref, g2s.at[r, ring(j)], g2r.at[r, ring(j)], dev1[r])

    def gd_copy(j, off, lo):
        ref = gat.at[f_of(j), :, grows(j, off, q1), lo * half:]
        return remote(ref, ref, gds.at[ring(j)], gdr.at[ring(j)], dev_c)

    def a1_copy(k, r, off):
        ref = gat.at[f_of(held + k), r, grows(held + k, off[r], q3), lanes[0]]
        return remote(ref, ref, a1s.at[r, k], a1r.at[r, k], dev2[r])

    def a2_copy(k, r, off):
        ref = gat.at[f_of(held + k), r, grows(held + k, off[r], q2), lanes[0]]
        return remote(ref, ref, a2s.at[r, k], a2r.at[r, k], dev1[r])

    def ad_copy(k, off):
        ref = gat.at[f_of(held + k), :, grows(held + k, off, q1), lanes[0]]
        return remote(ref, ref, ads.at[k], adr.at[k], dev_c)

    def by_arrays(j, body):
        @pl.when(j < held)
        def _():
            body(0)

        @pl.when(j >= held)
        def _():
            body(1)

    def each_held(body):
        def one(k, carry):
            body(k)
            return carry

        lax.fori_loop(0, HELD, one, 0)

    def da_dot(j):
        for r in range(2):
            part_d[lax.rem(j, L_SLOTS), r] = contract_cols(dya_ref[trows(j), :], wd[rcols(j, r), :])

    def da_product(j):
        da_dot(j)
        dd_copy(j).start()

    def da_pair_sum(j):
        dd_copy(j).wait_recv()
        slot = lax.rem(j, L_SLOTS)
        for r in range(2):
            part_d[slot, r, own_c, :] = part_d[slot, r, own_c, :] + dsum_d[slot, r]
            pd_copy(j, r).start()

    in_dy.wait()
    wcopy(2, 0).wait()
    da_dot(0)
    pl.semaphore_wait(barrier, 8)
    dd_copy(0).start()
    in_x.wait()
    x_own = x_ref[...].astype(jnp.float32)
    st[t] = pack_cols(jnp.sum(x_own, axis=1, keepdims=True), jnp.sum(x_own * x_own, axis=1, keepdims=True))
    send_stats(st, ss, sr)
    zdy = remote(dya_ref.at[own, :], dya_ref.at[own, :], zs.at[0], zr.at[0], dev_z)
    zdy.start()
    for i in range(1, 3):
        wcopy(2, i).wait()
        da_product(i)
    for i in range(LEAD):
        da_pair_sum(i)
        if i + 3 < LEAD:
            wcopy(2, i + 3).wait()
            da_product(i + 3)
    in_gain.wait()
    acc[...] = jnp.zeros_like(acc)

    gain = gain_ref[...]
    c0, c1 = total_stats(st, ss, sr)
    mean_x = c0 / d_model
    inv_std = lax.rsqrt(c1 / d_model - mean_x * mean_x + LN_EPS)
    xhat = (x_ref[...].astype(jnp.float32) - mean_x) * inv_std
    xh[...] = xhat
    h_ref[own, :] = (gain * xhat).astype(jnp.bfloat16)

    def h_copy(block):
        return remote(h_ref.at[own, :], h_ref.at[block, :], zs.at[1], zr.at[1], dev_z)

    h_copy(own).start()

    def m_part(f, rs, j):
        return sum(jnp.dot(gat[f, r, rs, lanes[0]], wd[rcols(j, r), :], preferred_element_type=jnp.float32) for r in range(2))

    z_sum = remote(acc.at[1], zin, zs.at[2], zr.at[2], dev_z)

    def step(i, carry):
        @pl.when(jnp.logical_and(i >= P_SLOTS, i < n_units + P_SLOTS))
        def _():
            j = i - P_SLOTS
            d_copy(j).wait_send()
            dd_copy(j).wait_send()
            for r in range(2):
                p1_copy(j, r).wait_send()
                pd_copy(j, r).wait_send()

        @pl.when(i < n_f)
        def _():
            wcopy(0, i).wait()
            wcopy(1, i).wait()

        @pl.when(i + LEAD < n_f)
        def _():
            wcopy(2, i + LEAD).wait()

        @pl.when(i == OWN_FIRST - LEAD)
        def _():
            remote(dya_ref.at[own, :], dya_ref.at[oth, :], zs.at[0], zr.at[0], dev_z).wait_recv()

        @pl.when(i == OWN_FIRST)
        def _():
            h_copy(oth).wait_recv()
            h_t[...] = h_ref[...].T

        @pl.when(i < n_units)
        def _():
            slot = lax.rem(i, P_SLOTS)
            h = h_ref[trows(i), :]
            for r in range(2):
                part[slot, r, 0] = jnp.dot(h, wg[:, rcols(i, r)], preferred_element_type=jnp.float32)
                part[slot, r, 1] = jnp.dot(h, wu[:, rcols(i, r)], preferred_element_type=jnp.float32)
            d_copy(i).start()

        @pl.when(i + LEAD < n_units)
        def _():
            da_product(i + LEAD)

        @pl.when(jnp.logical_and(i >= STAGES[0], i < n_units + STAGES[0]))
        def _():
            j = i - STAGES[0]
            d_copy(j).wait_recv()
            slot = lax.rem(j, P_SLOTS)
            for r in range(2):
                for k in range(2):
                    part[slot, r, k, own_c, :] = part[slot, r, k, own_c, :] + dsum[lax.rem(j, D_SLOTS), r, k]
                p1_copy(j, r).start()

            @pl.when(j + LEAD < n_units)
            def _():
                da_pair_sum(j + LEAD)

        @pl.when(jnp.logical_and(i >= STAGES[1], i < n_units + STAGES[1]))
        def _():
            j = i - STAGES[1]
            slot = lax.rem(j, P_SLOTS)
            for r in range(2):
                pd_copy(j, r).wait_recv()
                p1_copy(j, r).wait_recv()
                for k in range(2):
                    r1[j, r, k] = r1[j, r, k] + part[slot, r, k, keep1[r], :]
                r1[j, r, 2] = r1[j, r, 2] + part_d[lax.rem(j, L_SLOTS), r, keep1[r], :]
                p2_copy(j, r).start()

        @pl.when(jnp.logical_and(i >= STAGES[2], i < n_units + STAGES[2]))
        def _():
            j = i - STAGES[2]
            for r in range(2):
                p2_copy(j, r).wait_recv()
                u = r1[j, r, 0, r_keep[r], :] + r2[j, r, 0]
                v = r1[j, r, 1, r_keep[r], :] + r2[j, r, 1]
                da = r1[j, r, 2, r_keep[r], :] + r2[j, r, 2]
                sig = jax.nn.sigmoid(u)
                swish = u * sig
                f = f_of(j)
                rs = grows(j, g_fin[r], q3)
                gat[f, r, rs, lanes[0]] = (swish * v).astype(jnp.bfloat16)
                gat[f, r, rs, lanes[1]] = (da * v * sig * (1.0 + u * (1.0 - sig))).astype(jnp.bfloat16)
                gat[f, r, rs, lanes[2]] = (da * swish).astype(jnp.bfloat16)
            by_arrays(j, lambda lo: [g1_copy(j, r, g_fin, lo).start() for r in range(2)])

        @pl.when(jnp.logical_and(i >= STAGES[3], i < n_units + STAGES[3]))
        def _():
            j = i - STAGES[3]

            def forward(lo):
                for r in range(2):
                    g1_copy(j, r, g_fin_n, lo).wait_recv()
                    g2_copy(j, r, g_keep1, lo).start()

            by_arrays(j, forward)

        @pl.when(jnp.logical_and(i >= STAGES[4], i < n_units + STAGES[4]))
        def _():
            j = i - STAGES[4]

            def to_core(lo):
                for r in range(2):
                    g2_copy(j, r, g_send1, lo).wait_recv()
                gd_copy(j, g_c[0], lo).start()

            by_arrays(j, to_core)

        @pl.when(i >= STAGES[5])
        def _():
            j = i - STAGES[5]
            by_arrays(j, lambda lo: gd_copy(j, g_c[1], lo).wait_recv())
            f = f_of(j)
            rs = trows(j)
            side = oth_of(j)

            @pl.when(j < held)
            def _():
                acc[side, 0] += m_part(f, rs, j)

            acc[side, 1] += sum(contract_cols(gat[f, r, rs, lanes[1]], wg[:, rcols(j, r)])
                                + contract_cols(gat[f, r, rs, lanes[2]], wu[:, rcols(j, r)]) for r in range(2))

            def sent(lo):
                for r in range(2):
                    p2_copy(j, r).wait_send()
                    g1_copy(j, r, g_fin, lo).wait_send()
                    g2_copy(j, r, g_keep1, lo).wait_send()
                gd_copy(j, g_c[0], lo).wait_send()

            by_arrays(j, sent)

            @pl.when(j == last_oth)
            def _():
                z_sum.start()

        @pl.when(i == n_units - 1 + STAGES[2])
        def _():
            each_held(lambda k: [a1_copy(k, r, g_fin).start() for r in range(2)])

        @pl.when(i == n_units - 1 + STAGES[3])
        def _():
            def forward(k):
                for r in range(2):
                    a1_copy(k, r, g_fin_n).wait_recv()
                    a2_copy(k, r, g_keep1).start()

            each_held(forward)
        return carry

    lax.fori_loop(0, n_units + STAGES[5], step, 0)

    z_sum.wait()
    d_hnorm = acc[0, 1] + zin[1]
    e = d_hnorm * gain
    rb[t] = pack_cols(jnp.sum(e, axis=1, keepdims=True), jnp.sum(e * xh[...], axis=1, keepdims=True))
    send_stats(rb, bs, br)
    dgs[...] = jnp.broadcast_to(jnp.sum(d_hnorm * xh[...], axis=0, keepdims=True), dgs.shape)
    z_dg = remote(dgs, dgr, zs.at[3], zr.at[3], dev_z)
    z_dg.start()

    def to_core(k):
        for r in range(2):
            a2_copy(k, r, g_send1).wait_recv()
        ad_copy(k, g_c[0]).start()

    each_held(to_core)

    def m_product(k):
        ad_copy(k, g_c[1]).wait_recv()
        acc[0, 0] += m_part(f_of(held + k), own, held + k)
        for r in range(2):
            a1_copy(k, r, g_fin).wait_send()
            a2_copy(k, r, g_keep1).wait_send()
        ad_copy(k, g_c[0]).wait_send()

    each_held(m_product)
    y_ref[...] = (x_ref[...].astype(jnp.float32) + (acc[0, 0] + zin[0])).astype(jnp.bfloat16)
    zdy.wait_send()
    h_copy(own).wait_send()
    c0, c1 = total_stats(rb, bs, br)
    dx_ln = inv_std * (e - c0 / d_model - xh[...] * (c1 / d_model))
    dx_ref[...] = (dya_ref[own, :].astype(jnp.float32) + dx_ln).astype(jnp.bfloat16)
    z_dg.wait()
    dg_ref[...] = dgs[0:1, :] + dgr[0:1, :]


def weight_grad_kernel(gat, h_t, dy_ref, y_in, dx_in, dg_in,
                       dwg_hbm, dwu_hbm, dwd_hbm, y_hbm, dx_hbm, dg_hbm, buf, buf2, bsem, ssem):
    n_f, _, _, width = gat.shape
    n_blocks = 2 * n_f
    wb = width // 3

    def out_copy(b, k):
        cs = pl.ds(mo(b * wb, wb), wb)
        dst = (dwg_hbm.at[:, cs], dwu_hbm.at[:, cs], dwd_hbm.at[cs, :])[k]
        slot = lax.rem(b, W_SLOTS)
        src = buf.at[slot, k] if k < 2 else buf2.at[slot]
        return pltpu.make_async_copy(src, dst, bsem.at[slot, k])

    def block(b, carry):
        slot = lax.rem(b, W_SLOTS)
        for k in range(3):
            @pl.when(b >= W_SLOTS)
            def _():
                out_copy(b - W_SLOTS, k).wait()

            src = gat[lax.div(b, 2), lax.rem(b, 2), :, (k + 1) % 3 * wb:((k + 1) % 3 + 1) * wb]
            if k < 2:
                buf[slot, k] = jnp.dot(h_t[...], src, preferred_element_type=jnp.float32)
            else:
                buf2[slot] = contract_rows(src, dy_ref[...])
            out_copy(b, k).start()
        return carry

    lax.fori_loop(0, n_blocks, block, 0)
    small = [pltpu.make_async_copy(src, dst, ssem.at[k])
             for k, (src, dst) in enumerate(((y_in, y_hbm), (dx_in, dx_hbm), (dg_in, dg_hbm)))]
    for d in small:
        d.start()

    def drain(b, carry):
        for k in range(3):
            out_copy(b, k).wait()
        return carry

    lax.fori_loop(n_blocks - W_SLOTS, n_blocks, drain, 0)
    for d in small:
        d.wait()


def solution(mesh):
    tx_size = mesh.shape["tx"]
    ty_size = mesh.shape["ty"]

    def local_step(x_blk, dy_blk, gain_blk, w_gate_blk, w_up_blk, w_down_blk):
        rows, dl = x_blk.shape
        fl = w_gate_blk.shape[1]
        tok = rows * ty_size
        d_model = dl * tx_size
        n = fl // FC
        half = FC // 2
        f32, bf16 = jnp.float32, jnp.bfloat16
        anyspec = pl.BlockSpec(memory_space=pl.ANY)
        sem = pltpu.SemaphoreType.DMA
        vm = pl.BlockSpec(memory_space=pltpu.VMEM)
        S = jax.ShapeDtypeStruct
        V = pltpu.VMEM
        small = [((rows, dl), bf16), ((rows, dl), bf16), ((1, dl), f32)]
        outs = pl.pallas_call(
            functools.partial(branch_kernel, d_model, n),
            out_shape=[V((n, 2, tok, 3 * half), bf16), V((dl, tok), bf16), V((tok, dl), bf16)] + [V(*s) for s in small],
            in_specs=[anyspec] * 6,
            out_specs=[vm] * 6,
            scratch_shapes=[
                V((rows, dl), bf16), V((1, dl), f32), V((tok, dl), bf16),
                V((dl, fl), bf16), V((dl, fl), bf16), V((fl, dl), bf16),
                V((rows, dl), f32),
                V((P_SLOTS, 2, 2, rows, half), f32), V((L_SLOTS, 2, rows, half), f32),
                V((D_SLOTS, 2, 2, rows // 2, half), f32), V((L_SLOTS, 2, rows // 2, half), f32),
                V((2 * n, 2, 3, rows // 4, half), f32), V((2 * n, 2, 3, rows // 8, half), f32),
                V((2, 2, rows, dl), f32), V((2, rows, dl), f32),
                V((8, 8, 128), f32), V((8, 8, 128), f32), V((8, dl), f32), V((8, dl), f32),
                sem((3, n)), sem((3,)), sem((4,)), sem((4,)), sem((8,)), sem((8,)), sem((8,)), sem((8,)),
                sem((RING,)), sem((RING,)), sem((RING,)), sem((RING,)),
                *[sem((2, RING)) for _ in range(10)],
                sem((RING,)), sem((RING,)),
                *[sem((2, HELD)) for _ in range(4)], sem((HELD,)), sem((HELD,)),
            ],
            compiler_params=pltpu.CompilerParams(collective_id=0, has_side_effects=True, vmem_limit_bytes=VMEM_LIMIT),
            cost_estimate=pl.CostEstimate(flops=12 * tok * dl * fl, bytes_accessed=6 * dl * fl + 6 * tok * fl, transcendentals=0),
        )(x_blk, dy_blk, gain_blk[None, :], w_gate_blk, w_up_blk, w_down_blk)

        dwg, dwu, dwd, y_blk, dx_blk, dg = pl.pallas_call(
            weight_grad_kernel,
            out_shape=[S((dl, fl), f32)] * 2 + [S((fl, dl), f32)] + [S(*s) for s in small],
            in_specs=[vm] * 6,
            out_specs=[anyspec] * 6,
            scratch_shapes=[
                V((W_SLOTS, 2, dl, half), f32), V((W_SLOTS, half, dl), f32), sem((W_SLOTS, 3)), sem((3,)),
            ],
            compiler_params=pltpu.CompilerParams(vmem_limit_bytes=VMEM_LIMIT),
            cost_estimate=pl.CostEstimate(flops=6 * tok * dl * fl, bytes_accessed=12 * dl * fl + 6 * tok * fl, transcendentals=0),
        )(*[pltpu.with_memory_space_constraint(o, pltpu.VMEM) for o in outs])
        return (y_blk, dx_blk, dwg, dwu, dwd, dg[0])

    return jax.shard_map(
        local_step, mesh=mesh,
        in_specs=(P("ty", "tx"), P("ty", "tx"), P("tx"), P("tx", "ty"), P("tx", "ty"), P("ty", "tx")),
        out_specs=(P("ty", "tx"), P("ty", "tx"), P("tx", "ty"), P("tx", "ty"), P("ty", "tx"), P("tx")),
        check_vma=False)
```

```python
import functools

import jax
import jax.numpy as jnp
from jax import lax
from jax.experimental import pallas as pl
from jax.experimental.pallas import tpu as pltpu
from jax.sharding import PartitionSpec as P

LN_EPS = 1e-6
MESH = pl.DeviceIdType.MESH
FC = 512
OWN_FIRST = 8
LEAD = 8
P_SLOTS = 4
L_SLOTS = LEAD + P_SLOTS
HELD = 8
RING = 16
STAGES = (1, 3, 6, 9, 13, 14)
W_SLOTS = 3
VMEM_LIMIT = 48 * 1024 * 1024


def contract_rows(left_op, right_op):
    return lax.dot_general(left_op, right_op, (((0,), (0,)), ((), ())), preferred_element_type=jnp.float32)


def contract_cols(left_op, right_op):
    return lax.dot_general(left_op, right_op, (((1,), (1,)), ((), ())), preferred_element_type=jnp.float32)


def mo(value, multiple):
    return pl.multiple_of(value, multiple)


def branch_kernel(d_model, n_f,
                  x_hbm, dy_hbm, gain_hbm, wg_hbm, wu_hbm, wd_hbm,
                  gat, h_t, dya_ref, y_ref, dx_ref, dg_ref,
                  x_ref, gain_ref, h_ref,
                  wg, wu, wd, xh, part, part_d, dsum, dsum_d, r1, r2, acc, zin, st, rb, dgs, dgr,
                  wsem, isem, zs, zr, ss, sr, bs, br, ds, dr, dds, ddr, p1s, p1r, pds, pdr, p2s, p2r,
                  g1s, g1r, g2s, g2r, gds, gdr, a1s, a1r, a2s, a2r, ads, adr):
    half = FC // 2
    rows = x_ref.shape[0]
    q1, q2, q3 = rows // 2, rows // 4, rows // 8
    n_units = 2 * n_f
    last_oth = OWN_FIRST + n_f - 1
    held = n_units - HELD

    ty = lax.axis_index("ty")
    t = lax.axis_index("tx")
    c = lax.rem(t, 2)
    xc = lax.rem(lax.div(t, 2), 2)
    yc = lax.div(t, 4)
    dev_c = (ty, t + 1 - 2 * c)
    dev_x = (ty, t + 2 - 4 * xc)
    dev_y = (ty, t + 4 - 8 * yc)
    dev_z = (1 - ty, t)
    own = pl.ds(mo(ty * rows, rows), rows)
    oth = pl.ds(mo((1 - ty) * rows, rows), rows)

    def remote(src, dst, ssem, rsem, dev):
        return pltpu.make_async_remote_copy(src_ref=src, dst_ref=dst, send_sem=ssem, recv_sem=rsem,
                                            device_id=dev, device_id_type=MESH)

    def f_of(j):
        return lax.rem(j + (n_f - OWN_FIRST), n_f)

    def oth_of(j):
        return lax.rem(lax.div(j + (n_f - OWN_FIRST), n_f), 2)

    def base_of(j):
        k = oth_of(j)
        return (ty + k - 2 * ty * k) * rows

    def fcols(j):
        return pl.ds(mo(f_of(j) * FC, FC), FC)

    def rcols(j, r):
        return pl.ds(mo(f_of(j) * FC + r * half, half), half)

    def trows(j):
        return pl.ds(mo(base_of(j), rows), rows)

    def wcopy(k, i):
        cs = fcols(i)
        if k == 0:
            return pltpu.make_async_copy(wg_hbm.at[:, cs], wg.at[:, cs], wsem.at[0, i])
        if k == 1:
            return pltpu.make_async_copy(wu_hbm.at[:, cs], wu.at[:, cs], wsem.at[1, i])
        return pltpu.make_async_copy(wd_hbm.at[cs, :], wd.at[cs, :], wsem.at[2, i])

    in_dy = pltpu.make_async_copy(dy_hbm, dya_ref.at[own, :], isem.at[0])
    in_x = pltpu.make_async_copy(x_hbm, x_ref, isem.at[1])
    in_gain = pltpu.make_async_copy(gain_hbm, gain_ref, isem.at[2])
    in_x.start()
    in_dy.start()
    in_gain.start()
    for i in range(LEAD):
        wcopy(2, i).start()

    barrier = pltpu.get_barrier_semaphore()
    for o in range(1, 8):
        pl.semaphore_signal(barrier, inc=1, device_id=(ty, lax.rem(t + o, 8)), device_id_type=MESH)
    pl.semaphore_signal(barrier, inc=1, device_id=dev_z, device_id_type=MESH)

    def start_w(i, carry):
        wcopy(0, i).start()
        wcopy(1, i).start()

        @pl.when(i + LEAD < n_f)
        def _():
            wcopy(2, i + LEAD).start()
        return carry

    lax.fori_loop(0, n_f, start_w, 0)

    lane = lax.broadcasted_iota(jnp.int32, (rows, 128), 1)

    def pack_cols(c0, c1):
        both = jnp.where(lane == 0, c0, jnp.where(lane == 1, c1, 0.0))
        return both.T[0:8, :]

    def unpack_cols(packed):
        full = jnp.concatenate([packed, jnp.zeros((rows - 8, 128), jnp.float32)], axis=0).T
        return full[:, 0:1], full[:, 1:2]

    def send_stats(buf, ssem, rsem):
        for o in range(1, 8):
            remote(buf.at[t], buf.at[t], ssem.at[o], rsem.at[o], (ty, lax.rem(t + o, 8))).start()

    def total_stats(buf, ssem, rsem):
        for o in range(1, 8):
            q = lax.rem(t + 8 - o, 8)
            d = remote(buf.at[t], buf.at[q], ssem.at[o], rsem.at[o], (ty, q))
            d.wait_send()
            d.wait_recv()
        s = buf[0]
        for j in range(1, 8):
            s = s + buf[j]
        return unpack_cols(s)

    def seg(base, size):
        return pl.ds(mo(base, size), size)

    own_c = seg(c * q1, q1)
    oth_c = seg((1 - c) * q1, q1)
    keep1 = (seg(c * q1 + xc * q2, q2), seg(c * q1 + yc * q2, q2))
    send1 = (seg(c * q1 + (1 - xc) * q2, q2), seg(c * q1 + (1 - yc) * q2, q2))
    r_keep = (seg(yc * q3, q3), seg(xc * q3, q3))
    r_send = (seg((1 - yc) * q3, q3), seg((1 - xc) * q3, q3))
    lanes = [slice(k * half, (k + 1) * half) for k in range(3)]
    dev1, dev2 = (dev_x, dev_y), (dev_y, dev_x)
    g_c = (c * q1, (1 - c) * q1)
    g_keep1 = (c * q1 + xc * q2, c * q1 + yc * q2)
    g_send1 = (c * q1 + (1 - xc) * q2, c * q1 + (1 - yc) * q2)
    g_fin = (g_keep1[0] + yc * q3, g_keep1[1] + xc * q3)
    g_fin_n = (g_keep1[0] + (1 - yc) * q3, g_keep1[1] + (1 - xc) * q3)

    def grows(j, off, size):
        return pl.ds(mo(base_of(j) + off, size), size)

    def ring(j):
        return lax.rem(j, RING)

    def d_copy(j):
        slot = lax.rem(j, P_SLOTS)
        return remote(part.at[slot, :, :, oth_c, :], dsum.at[slot], ds.at[ring(j)], dr.at[ring(j)], dev_c)

    def dd_copy(j):
        slot = lax.rem(j, L_SLOTS)
        return remote(part_d.at[slot, :, oth_c, :], dsum_d.at[slot], dds.at[ring(j)], ddr.at[ring(j)], dev_c)

    def p1_copy(j, r):
        return remote(part.at[lax.rem(j, P_SLOTS), r, :, send1[r], :], r1.at[j, r, 0:2],
                      p1s.at[r, ring(j)], p1r.at[r, ring(j)], dev1[r])

    def pd_copy(j, r):
        return remote(part_d.at[lax.rem(j, L_SLOTS), r, send1[r], :], r1.at[j, r, 2],
                      pds.at[r, ring(j)], pdr.at[r, ring(j)], dev1[r])

    def p2_copy(j, r):
        return remote(r1.at[j, r, :, r_send[r], :], r2.at[j, r], p2s.at[r, ring(j)], p2r.at[r, ring(j)], dev2[r])

    def g1_copy(j, r, off, lo):
        ref = gat.at[f_of(j), r, grows(j, off[r], q3), lo * half:]
        return remote(ref, ref, g1s.at[r, ring(j)], g1r.at[r, ring(j)], dev2[r])

    def g2_copy(j, r, off, lo):
        ref = gat.at[f_of(j), r, grows(j, off[r], q2), lo * half:]
        return remote(ref, ref, g2s.at[r, ring(j)], g2r.at[r, ring(j)], dev1[r])

    def gd_copy(j, off, lo):
        ref = gat.at[f_of(j), :, grows(j, off, q1), lo * half:]
        return remote(ref, ref, gds.at[ring(j)], gdr.at[ring(j)], dev_c)

    def a1_copy(k, r, off):
        ref = gat.at[f_of(held + k), r, grows(held + k, off[r], q3), lanes[0]]
        return remote(ref, ref, a1s.at[r, k], a1r.at[r, k], dev2[r])

    def a2_copy(k, r, off):
        ref = gat.at[f_of(held + k), r, grows(held + k, off[r], q2), lanes[0]]
        return remote(ref, ref, a2s.at[r, k], a2r.at[r, k], dev1[r])

    def ad_copy(k, off):
        ref = gat.at[f_of(held + k), :, grows(held + k, off, q1), lanes[0]]
        return remote(ref, ref, ads.at[k], adr.at[k], dev_c)

    def by_arrays(j, body):
        @pl.when(j < held)
        def _():
            body(0)

        @pl.when(j >= held)
        def _():
            body(1)

    def each_held(body):
        def one(k, carry):
            body(k)
            return carry

        lax.fori_loop(0, HELD, one, 0)

    def da_dot(j):
        for r in range(2):
            part_d[lax.rem(j, L_SLOTS), r] = contract_cols(dya_ref[trows(j), :], wd[rcols(j, r), :])

    def da_product(j):
        da_dot(j)
        dd_copy(j).start()

    def da_pair_sum(j):
        dd_copy(j).wait_recv()
        slot = lax.rem(j, L_SLOTS)
        for r in range(2):
            part_d[slot, r, own_c, :] = part_d[slot, r, own_c, :] + dsum_d[slot, r]
            pd_copy(j, r).start()

    in_dy.wait()
    wcopy(2, 0).wait()
    da_dot(0)
    pl.semaphore_wait(barrier, 8)
    dd_copy(0).start()
    in_x.wait()
    x_own = x_ref[...].astype(jnp.float32)
    st[t] = pack_cols(jnp.sum(x_own, axis=1, keepdims=True), jnp.sum(x_own * x_own, axis=1, keepdims=True))
    send_stats(st, ss, sr)
    zdy = remote(dya_ref.at[own, :], dya_ref.at[own, :], zs.at[0], zr.at[0], dev_z)
    zdy.start()
    for i in range(1, 3):
        wcopy(2, i).wait()
        da_product(i)
    for i in range(LEAD):
        da_pair_sum(i)
        if i + 3 < LEAD:
            wcopy(2, i + 3).wait()
            da_product(i + 3)
    in_gain.wait()
    acc[...] = jnp.zeros_like(acc)

    gain = gain_ref[...]
    c0, c1 = total_stats(st, ss, sr)
    mean_x = c0 / d_model
    inv_std = lax.rsqrt(c1 / d_model - mean_x * mean_x + LN_EPS)
    xhat = (x_ref[...].astype(jnp.float32) - mean_x) * inv_std
    xh[...] = xhat
    h_ref[own, :] = (gain * xhat).astype(jnp.bfloat16)

    def h_copy(block):
        return remote(h_ref.at[own, :], h_ref.at[block, :], zs.at[1], zr.at[1], dev_z)

    h_copy(own).start()

    def m_part(f, rs, j):
        return sum(jnp.dot(gat[f, r, rs, lanes[0]], wd[rcols(j, r), :], preferred_element_type=jnp.float32) for r in range(2))

    z_sum = remote(acc.at[1], zin, zs.at[2], zr.at[2], dev_z)

    def step(i, carry):
        @pl.when(jnp.logical_and(i >= P_SLOTS, i < n_units + P_SLOTS))
        def _():
            j = i - P_SLOTS
            d_copy(j).wait_send()
            dd_copy(j).wait_send()
            for r in range(2):
                p1_copy(j, r).wait_send()
                pd_copy(j, r).wait_send()

        @pl.when(i < n_f)
        def _():
            wcopy(0, i).wait()
            wcopy(1, i).wait()

        @pl.when(i + LEAD < n_f)
        def _():
            wcopy(2, i + LEAD).wait()

        @pl.when(i == OWN_FIRST - LEAD)
        def _():
            remote(dya_ref.at[own, :], dya_ref.at[oth, :], zs.at[0], zr.at[0], dev_z).wait_recv()

        @pl.when(i == OWN_FIRST)
        def _():
            h_copy(oth).wait_recv()
            h_t[...] = h_ref[...].T

        @pl.when(i < n_units)
        def _():
            slot = lax.rem(i, P_SLOTS)
            h = h_ref[trows(i), :]
            for r in range(2):
                part[slot, r, 0] = jnp.dot(h, wg[:, rcols(i, r)], preferred_element_type=jnp.float32)
                part[slot, r, 1] = jnp.dot(h, wu[:, rcols(i, r)], preferred_element_type=jnp.float32)
            d_copy(i).start()

        @pl.when(i + LEAD < n_units)
        def _():
            da_product(i + LEAD)

        @pl.when(jnp.logical_and(i >= STAGES[0], i < n_units + STAGES[0]))
        def _():
            j = i - STAGES[0]
            d_copy(j).wait_recv()
            slot = lax.rem(j, P_SLOTS)
            for r in range(2):
                for k in range(2):
                    part[slot, r, k, own_c, :] = part[slot, r, k, own_c, :] + dsum[slot, r, k]
                p1_copy(j, r).start()

            @pl.when(j + LEAD < n_units)
            def _():
                da_pair_sum(j + LEAD)

        @pl.when(jnp.logical_and(i >= STAGES[1], i < n_units + STAGES[1]))
        def _():
            j = i - STAGES[1]
            slot = lax.rem(j, P_SLOTS)
            for r in range(2):
                pd_copy(j, r).wait_recv()
                p1_copy(j, r).wait_recv()
                for k in range(2):
                    r1[j, r, k] = r1[j, r, k] + part[slot, r, k, keep1[r], :]
                r1[j, r, 2] = r1[j, r, 2] + part_d[lax.rem(j, L_SLOTS), r, keep1[r], :]
                p2_copy(j, r).start()

        @pl.when(jnp.logical_and(i >= STAGES[2], i < n_units + STAGES[2]))
        def _():
            j = i - STAGES[2]
            for r in range(2):
                p2_copy(j, r).wait_recv()
                u = r1[j, r, 0, r_keep[r], :] + r2[j, r, 0]
                v = r1[j, r, 1, r_keep[r], :] + r2[j, r, 1]
                da = r1[j, r, 2, r_keep[r], :] + r2[j, r, 2]
                sig = jax.nn.sigmoid(u)
                swish = u * sig
                f = f_of(j)
                rs = grows(j, g_fin[r], q3)
                gat[f, r, rs, lanes[0]] = (swish * v).astype(jnp.bfloat16)
                gat[f, r, rs, lanes[1]] = (da * v * sig * (1.0 + u * (1.0 - sig))).astype(jnp.bfloat16)
                gat[f, r, rs, lanes[2]] = (da * swish).astype(jnp.bfloat16)
            by_arrays(j, lambda lo: [g1_copy(j, r, g_fin, lo).start() for r in range(2)])

        @pl.when(jnp.logical_and(i >= STAGES[3], i < n_units + STAGES[3]))
        def _():
            j = i - STAGES[3]

            def forward(lo):
                for r in range(2):
                    g1_copy(j, r, g_fin_n, lo).wait_recv()
                    g2_copy(j, r, g_keep1, lo).start()

            by_arrays(j, forward)

        @pl.when(jnp.logical_and(i >= STAGES[4], i < n_units + STAGES[4]))
        def _():
            j = i - STAGES[4]

            def to_core(lo):
                for r in range(2):
                    g2_copy(j, r, g_send1, lo).wait_recv()
                gd_copy(j, g_c[0], lo).start()

            by_arrays(j, to_core)

        @pl.when(i >= STAGES[5])
        def _():
            j = i - STAGES[5]
            by_arrays(j, lambda lo: gd_copy(j, g_c[1], lo).wait_recv())
            f = f_of(j)
            rs = trows(j)
            side = oth_of(j)

            @pl.when(j < held)
            def _():
                acc[side, 0] += m_part(f, rs, j)

            acc[side, 1] += sum(contract_cols(gat[f, r, rs, lanes[1]], wg[:, rcols(j, r)])
                                + contract_cols(gat[f, r, rs, lanes[2]], wu[:, rcols(j, r)]) for r in range(2))

            def sent(lo):
                for r in range(2):
                    p2_copy(j, r).wait_send()
                    g1_copy(j, r, g_fin, lo).wait_send()
                    g2_copy(j, r, g_keep1, lo).wait_send()
                gd_copy(j, g_c[0], lo).wait_send()

            by_arrays(j, sent)

            @pl.when(j == last_oth)
            def _():
                z_sum.start()

        @pl.when(i == n_units - 1 + STAGES[2])
        def _():
            each_held(lambda k: [a1_copy(k, r, g_fin).start() for r in range(2)])

        @pl.when(i == n_units - 1 + STAGES[3])
        def _():
            def forward(k):
                for r in range(2):
                    a1_copy(k, r, g_fin_n).wait_recv()
                    a2_copy(k, r, g_keep1).start()

            each_held(forward)
        return carry

    lax.fori_loop(0, n_units + STAGES[5], step, 0)

    z_sum.wait()
    d_hnorm = acc[0, 1] + zin[1]
    e = d_hnorm * gain
    rb[t] = pack_cols(jnp.sum(e, axis=1, keepdims=True), jnp.sum(e * xh[...], axis=1, keepdims=True))
    send_stats(rb, bs, br)
    dgs[...] = jnp.broadcast_to(jnp.sum(d_hnorm * xh[...], axis=0, keepdims=True), dgs.shape)
    z_dg = remote(dgs, dgr, zs.at[3], zr.at[3], dev_z)
    z_dg.start()

    def to_core(k):
        for r in range(2):
            a2_copy(k, r, g_send1).wait_recv()
        ad_copy(k, g_c[0]).start()

    each_held(to_core)

    def m_product(k):
        ad_copy(k, g_c[1]).wait_recv()
        acc[0, 0] += m_part(f_of(held + k), own, held + k)
        for r in range(2):
            a1_copy(k, r, g_fin).wait_send()
            a2_copy(k, r, g_keep1).wait_send()
        ad_copy(k, g_c[0]).wait_send()

    each_held(m_product)
    y_ref[...] = (x_ref[...].astype(jnp.float32) + (acc[0, 0] + zin[0])).astype(jnp.bfloat16)
    zdy.wait_send()
    h_copy(own).wait_send()
    c0, c1 = total_stats(rb, bs, br)
    dx_ln = inv_std * (e - c0 / d_model - xh[...] * (c1 / d_model))
    dx_ref[...] = (dya_ref[own, :].astype(jnp.float32) + dx_ln).astype(jnp.bfloat16)
    z_dg.wait()
    dg_ref[...] = dgs[0:1, :] + dgr[0:1, :]


def weight_grad_kernel(gat, h_t, dy_ref, y_in, dx_in, dg_in,
                       dwg_hbm, dwu_hbm, dwd_hbm, y_hbm, dx_hbm, dg_hbm, buf, bsem, ssem):
    n_blocks, _, _, width = gat.shape
    half = width // 3
    WB = 2 * half

    def out_copy(b, k):
        cs = pl.ds(mo(b * WB, WB), WB)
        dst = (dwg_hbm.at[:, cs], dwu_hbm.at[:, cs], dwd_hbm.at[cs, :])[k]
        slot = lax.rem(b, W_SLOTS)
        return pltpu.make_async_copy(buf.at[slot, k], dst, bsem.at[slot, k])

    def block(b, carry):
        slot = lax.rem(b, W_SLOTS)
        for k in range(3):
            @pl.when(b >= W_SLOTS)
            def _():
                out_copy(b - W_SLOTS, k).wait()

            for r in range(2):
                rs = slice(r * half, (r + 1) * half)
                src = gat[b, r, :, (k + 1) % 3 * half:((k + 1) % 3 + 1) * half]
                if k < 2:
                    buf[slot, k, :, rs] = jnp.dot(h_t[...], src, preferred_element_type=jnp.float32)
                else:
                    buf[slot, k, rs, :] = contract_rows(src, dy_ref[...])
            out_copy(b, k).start()
        return carry

    lax.fori_loop(0, n_blocks, block, 0)
    small = [pltpu.make_async_copy(src, dst, ssem.at[k])
             for k, (src, dst) in enumerate(((y_in, y_hbm), (dx_in, dx_hbm), (dg_in, dg_hbm)))]
    for d in small:
        d.start()

    def drain(b, carry):
        for k in range(3):
            out_copy(b, k).wait()
        return carry

    lax.fori_loop(n_blocks - W_SLOTS, n_blocks, drain, 0)
    for d in small:
        d.wait()


def solution(mesh):
    tx_size = mesh.shape["tx"]
    ty_size = mesh.shape["ty"]

    def local_step(x_blk, dy_blk, gain_blk, w_gate_blk, w_up_blk, w_down_blk):
        rows, dl = x_blk.shape
        fl = w_gate_blk.shape[1]
        tok = rows * ty_size
        d_model = dl * tx_size
        n = fl // FC
        half = FC // 2
        f32, bf16 = jnp.float32, jnp.bfloat16
        anyspec = pl.BlockSpec(memory_space=pl.ANY)
        sem = pltpu.SemaphoreType.DMA
        vm = pl.BlockSpec(memory_space=pltpu.VMEM)
        S = jax.ShapeDtypeStruct
        V = pltpu.VMEM
        small = [((rows, dl), bf16), ((rows, dl), bf16), ((1, dl), f32)]
        outs = pl.pallas_call(
            functools.partial(branch_kernel, d_model, n),
            out_shape=[V((n, 2, tok, 3 * half), bf16), V((dl, tok), bf16), V((tok, dl), bf16)] + [V(*s) for s in small],
            in_specs=[anyspec] * 6,
            out_specs=[vm] * 6,
            scratch_shapes=[
                V((rows, dl), bf16), V((1, dl), f32), V((tok, dl), bf16),
                V((dl, fl), bf16), V((dl, fl), bf16), V((fl, dl), bf16),
                V((rows, dl), f32),
                V((P_SLOTS, 2, 2, rows, half), f32), V((L_SLOTS, 2, rows, half), f32),
                V((P_SLOTS, 2, 2, rows // 2, half), f32), V((L_SLOTS, 2, rows // 2, half), f32),
                V((2 * n, 2, 3, rows // 4, half), f32), V((2 * n, 2, 3, rows // 8, half), f32),
                V((2, 2, rows, dl), f32), V((2, rows, dl), f32),
                V((8, 8, 128), f32), V((8, 8, 128), f32), V((8, dl), f32), V((8, dl), f32),
                sem((3, n)), sem((3,)), sem((4,)), sem((4,)), sem((8,)), sem((8,)), sem((8,)), sem((8,)),
                sem((RING,)), sem((RING,)), sem((RING,)), sem((RING,)),
                *[sem((2, RING)) for _ in range(10)],
                sem((RING,)), sem((RING,)),
                *[sem((2, HELD)) for _ in range(4)], sem((HELD,)), sem((HELD,)),
            ],
            compiler_params=pltpu.CompilerParams(collective_id=0, has_side_effects=True, vmem_limit_bytes=VMEM_LIMIT),
            cost_estimate=pl.CostEstimate(flops=12 * tok * dl * fl, bytes_accessed=6 * dl * fl + 6 * tok * fl, transcendentals=0),
        )(x_blk, dy_blk, gain_blk[None, :], w_gate_blk, w_up_blk, w_down_blk)

        dwg, dwu, dwd, y_blk, dx_blk, dg = pl.pallas_call(
            weight_grad_kernel,
            out_shape=[S((dl, fl), f32)] * 2 + [S((fl, dl), f32)] + [S(*s) for s in small],
            in_specs=[vm] * 6,
            out_specs=[anyspec] * 6,
            scratch_shapes=[
                V((W_SLOTS, 3, dl, FC), f32), sem((W_SLOTS, 3)), sem((3,)),
            ],
            compiler_params=pltpu.CompilerParams(vmem_limit_bytes=VMEM_LIMIT),
            cost_estimate=pl.CostEstimate(flops=6 * tok * dl * fl, bytes_accessed=12 * dl * fl + 6 * tok * fl, transcendentals=0),
        )(*[pltpu.with_memory_space_constraint(o, pltpu.VMEM) for o in outs])
        return (y_blk, dx_blk, dwg, dwu, dwd, dg[0])

    return jax.shard_map(
        local_step, mesh=mesh,
        in_specs=(P("ty", "tx"), P("ty", "tx"), P("tx"), P("tx", "ty"), P("tx", "ty"), P("ty", "tx")),
        out_specs=(P("ty", "tx"), P("ty", "tx"), P("tx", "ty"), P("tx", "ty"), P("ty", "tx"), P("tx")),
        check_vma=False)
```

```python
import functools

import jax
import jax.numpy as jnp
from jax import lax
from jax.experimental import pallas as pl
from jax.experimental.pallas import tpu as pltpu
from jax.sharding import PartitionSpec as P

LN_EPS = 1e-6
MESH = pl.DeviceIdType.MESH
FC = 512
OWN_FIRST = 8
LEAD = 8
P_SLOTS = 5
D_SLOTS = 6
L_SLOTS = LEAD + P_SLOTS
HELD = 8
RING = 16
STAGES = (2, 4, 6, 8, 10, 12)
W_SLOTS = 6
VMEM_LIMIT = 48 * 1024 * 1024


def contract_rows(left_op, right_op):
    return lax.dot_general(left_op, right_op, (((0,), (0,)), ((), ())), preferred_element_type=jnp.float32)


def contract_cols(left_op, right_op):
    return lax.dot_general(left_op, right_op, (((1,), (1,)), ((), ())), preferred_element_type=jnp.float32)


def mo(value, multiple):
    return pl.multiple_of(value, multiple)


def branch_kernel(d_model, n_f,
                  x_hbm, dy_hbm, gain_hbm, wg_hbm, wu_hbm, wd_hbm,
                  gat, h_t, dya_ref, y_ref, dx_ref, dg_ref,
                  x_ref, gain_ref, h_ref,
                  wg, wu, wd, xh, part, part_d, dsum, dsum_d, r1, r2, acc, zin, st, rb, dgs, dgr,
                  wsem, isem, zs, zr, ss, sr, bs, br, ds, dr, dds, ddr, p1s, p1r, pds, pdr, p2s, p2r,
                  g1s, g1r, g2s, g2r, gds, gdr, a1s, a1r, a2s, a2r, ads, adr):
    half = FC // 2
    rows = x_ref.shape[0]
    q1, q2, q3 = rows // 2, rows // 4, rows // 8
    n_units = 2 * n_f
    last_oth = OWN_FIRST + n_f - 1
    held = n_units - HELD

    ty = lax.axis_index("ty")
    t = lax.axis_index("tx")
    c = lax.rem(t, 2)
    xc = lax.rem(lax.div(t, 2), 2)
    yc = lax.div(t, 4)
    dev_c = (ty, t + 1 - 2 * c)
    dev_x = (ty, t + 2 - 4 * xc)
    dev_y = (ty, t + 4 - 8 * yc)
    dev_z = (1 - ty, t)
    own = pl.ds(mo(ty * rows, rows), rows)
    oth = pl.ds(mo((1 - ty) * rows, rows), rows)

    def remote(src, dst, ssem, rsem, dev):
        return pltpu.make_async_remote_copy(src_ref=src, dst_ref=dst, send_sem=ssem, recv_sem=rsem,
                                            device_id=dev, device_id_type=MESH)

    def f_of(j):
        return lax.rem(j + (n_f - OWN_FIRST), n_f)

    def oth_of(j):
        return lax.rem(lax.div(j + (n_f - OWN_FIRST), n_f), 2)

    def base_of(j):
        k = oth_of(j)
        return (ty + k - 2 * ty * k) * rows

    def fcols(j):
        return pl.ds(mo(f_of(j) * FC, FC), FC)

    def rcols(j, r):
        return pl.ds(mo(f_of(j) * FC + r * half, half), half)

    def trows(j):
        return pl.ds(mo(base_of(j), rows), rows)

    def wcopy(k, i):
        cs = fcols(i)
        if k == 0:
            return pltpu.make_async_copy(wg_hbm.at[:, cs], wg.at[:, cs], wsem.at[0, i])
        if k == 1:
            return pltpu.make_async_copy(wu_hbm.at[:, cs], wu.at[:, cs], wsem.at[1, i])
        return pltpu.make_async_copy(wd_hbm.at[cs, :], wd.at[cs, :], wsem.at[2, i])

    in_dy = pltpu.make_async_copy(dy_hbm, dya_ref.at[own, :], isem.at[0])
    in_x = pltpu.make_async_copy(x_hbm, x_ref, isem.at[1])
    in_gain = pltpu.make_async_copy(gain_hbm, gain_ref, isem.at[2])
    in_x.start()
    in_dy.start()
    in_gain.start()
    for i in range(LEAD):
        wcopy(2, i).start()

    barrier = pltpu.get_barrier_semaphore()
    for o in range(1, 8):
        pl.semaphore_signal(barrier, inc=1, device_id=(ty, lax.rem(t + o, 8)), device_id_type=MESH)
    pl.semaphore_signal(barrier, inc=1, device_id=dev_z, device_id_type=MESH)

    def start_w(i, carry):
        wcopy(0, i).start()
        wcopy(1, i).start()

        @pl.when(i + LEAD < n_f)
        def _():
            wcopy(2, i + LEAD).start()
        return carry

    lax.fori_loop(0, n_f, start_w, 0)

    lane = lax.broadcasted_iota(jnp.int32, (rows, 128), 1)

    def pack_cols(c0, c1):
        both = jnp.where(lane == 0, c0, jnp.where(lane == 1, c1, 0.0))
        return both.T[0:8, :]

    def unpack_cols(packed):
        full = jnp.concatenate([packed, jnp.zeros((rows - 8, 128), jnp.float32)], axis=0).T
        return full[:, 0:1], full[:, 1:2]

    def send_stats(buf, ssem, rsem):
        for o in range(1, 8):
            remote(buf.at[t], buf.at[t], ssem.at[o], rsem.at[o], (ty, lax.rem(t + o, 8))).start()

    def total_stats(buf, ssem, rsem):
        for o in range(1, 8):
            q = lax.rem(t + 8 - o, 8)
            d = remote(buf.at[t], buf.at[q], ssem.at[o], rsem.at[o], (ty, q))
            d.wait_send()
            d.wait_recv()
        s = buf[0]
        for j in range(1, 8):
            s = s + buf[j]
        return unpack_cols(s)

    def seg(base, size):
        return pl.ds(mo(base, size), size)

    own_c = seg(c * q1, q1)
    oth_c = seg((1 - c) * q1, q1)
    keep1 = (seg(c * q1 + xc * q2, q2), seg(c * q1 + yc * q2, q2))
    send1 = (seg(c * q1 + (1 - xc) * q2, q2), seg(c * q1 + (1 - yc) * q2, q2))
    r_keep = (seg(yc * q3, q3), seg(xc * q3, q3))
    r_send = (seg((1 - yc) * q3, q3), seg((1 - xc) * q3, q3))
    lanes = [slice(k * half, (k + 1) * half) for k in range(3)]
    dev1, dev2 = (dev_x, dev_y), (dev_y, dev_x)
    g_c = (c * q1, (1 - c) * q1)
    g_keep1 = (c * q1 + xc * q2, c * q1 + yc * q2)
    g_send1 = (c * q1 + (1 - xc) * q2, c * q1 + (1 - yc) * q2)
    g_fin = (g_keep1[0] + yc * q3, g_keep1[1] + xc * q3)
    g_fin_n = (g_keep1[0] + (1 - yc) * q3, g_keep1[1] + (1 - xc) * q3)

    def grows(j, off, size):
        return pl.ds(mo(base_of(j) + off, size), size)

    def ring(j):
        return lax.rem(j, RING)

    def d_copy(j):
        slot = lax.rem(j, P_SLOTS)
        return remote(part.at[slot, :, :, oth_c, :], dsum.at[lax.rem(j, D_SLOTS)], ds.at[ring(j)], dr.at[ring(j)], dev_c)

    def dd_copy(j):
        slot = lax.rem(j, L_SLOTS)
        return remote(part_d.at[slot, :, oth_c, :], dsum_d.at[slot], dds.at[ring(j)], ddr.at[ring(j)], dev_c)

    def p1_copy(j, r):
        return remote(part.at[lax.rem(j, P_SLOTS), r, :, send1[r], :], r1.at[j, r, 0:2],
                      p1s.at[r, ring(j)], p1r.at[r, ring(j)], dev1[r])

    def pd_copy(j, r):
        return remote(part_d.at[lax.rem(j, L_SLOTS), r, send1[r], :], r1.at[j, r, 2],
                      pds.at[r, ring(j)], pdr.at[r, ring(j)], dev1[r])

    def p2_copy(j, r):
        return remote(r1.at[j, r, :, r_send[r], :], r2.at[j, r], p2s.at[r, ring(j)], p2r.at[r, ring(j)], dev2[r])

    def g1_copy(j, r, off, lo):
        ref = gat.at[f_of(j), r, grows(j, off[r], q3), lo * half:]
        return remote(ref, ref, g1s.at[r, ring(j)], g1r.at[r, ring(j)], dev2[r])

    def g2_copy(j, r, off, lo):
        ref = gat.at[f_of(j), r, grows(j, off[r], q2), lo * half:]
        return remote(ref, ref, g2s.at[r, ring(j)], g2r.at[r, ring(j)], dev1[r])

    def gd_copy(j, off, lo):
        ref = gat.at[f_of(j), :, grows(j, off, q1), lo * half:]
        return remote(ref, ref, gds.at[ring(j)], gdr.at[ring(j)], dev_c)

    def a1_copy(k, r, off):
        ref = gat.at[f_of(held + k), r, grows(held + k, off[r], q3), lanes[0]]
        return remote(ref, ref, a1s.at[r, k], a1r.at[r, k], dev2[r])

    def a2_copy(k, r, off):
        ref = gat.at[f_of(held + k), r, grows(held + k, off[r], q2), lanes[0]]
        return remote(ref, ref, a2s.at[r, k], a2r.at[r, k], dev1[r])

    def ad_copy(k, off):
        ref = gat.at[f_of(held + k), :, grows(held + k, off, q1), lanes[0]]
        return remote(ref, ref, ads.at[k], adr.at[k], dev_c)

    def by_arrays(j, body):
        @pl.when(j < held)
        def _():
            body(0)

        @pl.when(j >= held)
        def _():
            body(1)

    def each_held(body):
        def one(k, carry):
            body(k)
            return carry

        lax.fori_loop(0, HELD, one, 0)

    def da_dot(j):
        for r in range(2):
            part_d[lax.rem(j, L_SLOTS), r] = contract_cols(dya_ref[trows(j), :], wd[rcols(j, r), :])

    def da_product(j):
        da_dot(j)
        dd_copy(j).start()

    def da_pair_sum(j):
        dd_copy(j).wait_recv()
        slot = lax.rem(j, L_SLOTS)
        for r in range(2):
            part_d[slot, r, own_c, :] = part_d[slot, r, own_c, :] + dsum_d[slot, r]
            pd_copy(j, r).start()

    in_dy.wait()
    wcopy(2, 0).wait()
    da_dot(0)
    pl.semaphore_wait(barrier, 8)
    dd_copy(0).start()
    in_x.wait()
    x_own = x_ref[...].astype(jnp.float32)
    st[t] = pack_cols(jnp.sum(x_own, axis=1, keepdims=True), jnp.sum(x_own * x_own, axis=1, keepdims=True))
    send_stats(st, ss, sr)
    zdy = remote(dya_ref.at[own, :], dya_ref.at[own, :], zs.at[0], zr.at[0], dev_z)
    zdy.start()
    for i in range(1, 3):
        wcopy(2, i).wait()
        da_product(i)
    for i in range(LEAD):
        da_pair_sum(i)
        if i + 3 < LEAD:
            wcopy(2, i + 3).wait()
            da_product(i + 3)
    in_gain.wait()
    acc[...] = jnp.zeros_like(acc)

    gain = gain_ref[...]
    c0, c1 = total_stats(st, ss, sr)
    mean_x = c0 / d_model
    inv_std = lax.rsqrt(c1 / d_model - mean_x * mean_x + LN_EPS)
    xhat = (x_ref[...].astype(jnp.float32) - mean_x) * inv_std
    xh[...] = xhat
    h_ref[own, :] = (gain * xhat).astype(jnp.bfloat16)

    def h_copy(block):
        return remote(h_ref.at[own, :], h_ref.at[block, :], zs.at[1], zr.at[1], dev_z)

    h_copy(own).start()

    def m_part(f, rs, j):
        return sum(jnp.dot(gat[f, r, rs, lanes[0]], wd[rcols(j, r), :], preferred_element_type=jnp.float32) for r in range(2))

    z_sum = remote(acc.at[1], zin, zs.at[2], zr.at[2], dev_z)

    def step(i, carry):
        @pl.when(jnp.logical_and(i >= P_SLOTS, i < n_units + P_SLOTS))
        def _():
            j = i - P_SLOTS
            d_copy(j).wait_send()
            dd_copy(j).wait_send()
            for r in range(2):
                p1_copy(j, r).wait_send()
                pd_copy(j, r).wait_send()

        @pl.when(i < n_f)
        def _():
            wcopy(0, i).wait()
            wcopy(1, i).wait()

        @pl.when(i + LEAD < n_f)
        def _():
            wcopy(2, i + LEAD).wait()

        @pl.when(i == OWN_FIRST - LEAD)
        def _():
            remote(dya_ref.at[own, :], dya_ref.at[oth, :], zs.at[0], zr.at[0], dev_z).wait_recv()

        @pl.when(i == OWN_FIRST)
        def _():
            h_copy(oth).wait_recv()
            h_t[...] = h_ref[...].T

        @pl.when(i < n_units)
        def _():
            slot = lax.rem(i, P_SLOTS)
            h = h_ref[trows(i), :]
            for r in range(2):
                part[slot, r, 0] = jnp.dot(h, wg[:, rcols(i, r)], preferred_element_type=jnp.float32)
                part[slot, r, 1] = jnp.dot(h, wu[:, rcols(i, r)], preferred_element_type=jnp.float32)
            d_copy(i).start()

        @pl.when(i + LEAD < n_units)
        def _():
            da_product(i + LEAD)

        @pl.when(jnp.logical_and(i >= STAGES[0], i < n_units + STAGES[0]))
        def _():
            j = i - STAGES[0]
            d_copy(j).wait_recv()
            slot = lax.rem(j, P_SLOTS)
            for r in range(2):
                for k in range(2):
                    part[slot, r, k, own_c, :] = part[slot, r, k, own_c, :] + dsum[lax.rem(j, D_SLOTS), r, k]
                p1_copy(j, r).start()

            @pl.when(j + LEAD < n_units)
            def _():
                da_pair_sum(j + LEAD)

        @pl.when(jnp.logical_and(i >= STAGES[1], i < n_units + STAGES[1]))
        def _():
            j = i - STAGES[1]
            slot = lax.rem(j, P_SLOTS)
            for r in range(2):
                pd_copy(j, r).wait_recv()
                p1_copy(j, r).wait_recv()
                for k in range(2):
                    r1[j, r, k] = r1[j, r, k] + part[slot, r, k, keep1[r], :]
                r1[j, r, 2] = r1[j, r, 2] + part_d[lax.rem(j, L_SLOTS), r, keep1[r], :]
                p2_copy(j, r).start()

        @pl.when(jnp.logical_and(i >= STAGES[2], i < n_units + STAGES[2]))
        def _():
            j = i - STAGES[2]
            for r in range(2):
                p2_copy(j, r).wait_recv()
                u = r1[j, r, 0, r_keep[r], :] + r2[j, r, 0]
                v = r1[j, r, 1, r_keep[r], :] + r2[j, r, 1]
                da = r1[j, r, 2, r_keep[r], :] + r2[j, r, 2]
                sig = jax.nn.sigmoid(u)
                swish = u * sig
                f = f_of(j)
                rs = grows(j, g_fin[r], q3)
                gat[f, r, rs, lanes[0]] = (swish * v).astype(jnp.bfloat16)
                gat[f, r, rs, lanes[1]] = (da * v * sig * (1.0 + u * (1.0 - sig))).astype(jnp.bfloat16)
                gat[f, r, rs, lanes[2]] = (da * swish).astype(jnp.bfloat16)
            by_arrays(j, lambda lo: [g1_copy(j, r, g_fin, lo).start() for r in range(2)])

        @pl.when(jnp.logical_and(i >= STAGES[3], i < n_units + STAGES[3]))
        def _():
            j = i - STAGES[3]

            def forward(lo):
                for r in range(2):
                    g1_copy(j, r, g_fin_n, lo).wait_recv()
                    g2_copy(j, r, g_keep1, lo).start()

            by_arrays(j, forward)

        @pl.when(jnp.logical_and(i >= STAGES[4], i < n_units + STAGES[4]))
        def _():
            j = i - STAGES[4]

            def to_core(lo):
                for r in range(2):
                    g2_copy(j, r, g_send1, lo).wait_recv()
                gd_copy(j, g_c[0], lo).start()

            by_arrays(j, to_core)

        @pl.when(i >= STAGES[5])
        def _():
            j = i - STAGES[5]
            by_arrays(j, lambda lo: gd_copy(j, g_c[1], lo).wait_recv())
            f = f_of(j)
            rs = trows(j)
            side = oth_of(j)

            @pl.when(j < held)
            def _():
                acc[side, 0] += m_part(f, rs, j)

            acc[side, 1] += sum(contract_cols(gat[f, r, rs, lanes[1]], wg[:, rcols(j, r)])
                                + contract_cols(gat[f, r, rs, lanes[2]], wu[:, rcols(j, r)]) for r in range(2))

            def sent(lo):
                for r in range(2):
                    p2_copy(j, r).wait_send()
                    g1_copy(j, r, g_fin, lo).wait_send()
                    g2_copy(j, r, g_keep1, lo).wait_send()
                gd_copy(j, g_c[0], lo).wait_send()

            by_arrays(j, sent)

            @pl.when(j == last_oth)
            def _():
                z_sum.start()

        @pl.when(i == n_units - 1 + STAGES[2])
        def _():
            each_held(lambda k: [a1_copy(k, r, g_fin).start() for r in range(2)])

        @pl.when(i == n_units - 1 + STAGES[3])
        def _():
            def forward(k):
                for r in range(2):
                    a1_copy(k, r, g_fin_n).wait_recv()
                    a2_copy(k, r, g_keep1).start()

            each_held(forward)
        return carry

    lax.fori_loop(0, n_units + STAGES[5], step, 0)

    z_sum.wait()
    d_hnorm = acc[0, 1] + zin[1]
    e = d_hnorm * gain
    rb[t] = pack_cols(jnp.sum(e, axis=1, keepdims=True), jnp.sum(e * xh[...], axis=1, keepdims=True))
    send_stats(rb, bs, br)
    dgs[...] = jnp.broadcast_to(jnp.sum(d_hnorm * xh[...], axis=0, keepdims=True), dgs.shape)
    z_dg = remote(dgs, dgr, zs.at[3], zr.at[3], dev_z)
    z_dg.start()

    def to_core(k):
        for r in range(2):
            a2_copy(k, r, g_send1).wait_recv()
        ad_copy(k, g_c[0]).start()

    each_held(to_core)

    def m_product(k):
        ad_copy(k, g_c[1]).wait_recv()
        acc[0, 0] += m_part(f_of(held + k), own, held + k)
        for r in range(2):
            a1_copy(k, r, g_fin).wait_send()
            a2_copy(k, r, g_keep1).wait_send()
        ad_copy(k, g_c[0]).wait_send()

    each_held(m_product)
    y_ref[...] = (x_ref[...].astype(jnp.float32) + (acc[0, 0] + zin[0])).astype(jnp.bfloat16)
    zdy.wait_send()
    h_copy(own).wait_send()
    c0, c1 = total_stats(rb, bs, br)
    dx_ln = inv_std * (e - c0 / d_model - xh[...] * (c1 / d_model))
    dx_ref[...] = (dya_ref[own, :].astype(jnp.float32) + dx_ln).astype(jnp.bfloat16)
    z_dg.wait()
    dg_ref[...] = dgs[0:1, :] + dgr[0:1, :]


def weight_grad_kernel(gat, h_t, dy_ref, y_in, dx_in, dg_in,
                       dwg_hbm, dwu_hbm, dwd_hbm, y_hbm, dx_hbm, dg_hbm, buf, buf2, bsem, ssem):
    n_f, _, _, width = gat.shape
    n_blocks = 2 * n_f
    wb = width // 3

    def out_copy(b, k):
        cs = pl.ds(mo(b * wb, wb), wb)
        dst = (dwg_hbm.at[:, cs], dwu_hbm.at[:, cs], dwd_hbm.at[cs, :])[k]
        slot = lax.rem(b, W_SLOTS)
        src = buf.at[slot, k] if k < 2 else buf2.at[slot]
        return pltpu.make_async_copy(src, dst, bsem.at[slot, k])

    def block(b, carry):
        slot = lax.rem(b, W_SLOTS)
        for k in range(3):
            @pl.when(b >= W_SLOTS)
            def _():
                out_copy(b - W_SLOTS, k).wait()

            src = gat[lax.div(b, 2), lax.rem(b, 2), :, (k + 1) % 3 * wb:((k + 1) % 3 + 1) * wb]
            if k < 2:
                buf[slot, k] = jnp.dot(h_t[...], src, preferred_element_type=jnp.float32)
            else:
                buf2[slot] = contract_rows(src, dy_ref[...])
            out_copy(b, k).start()
        return carry

    lax.fori_loop(0, n_blocks, block, 0)
    small = [pltpu.make_async_copy(src, dst, ssem.at[k])
             for k, (src, dst) in enumerate(((y_in, y_hbm), (dx_in, dx_hbm), (dg_in, dg_hbm)))]
    for d in small:
        d.start()

    def drain(b, carry):
        for k in range(3):
            out_copy(b, k).wait()
        return carry

    lax.fori_loop(n_blocks - W_SLOTS, n_blocks, drain, 0)
    for d in small:
        d.wait()


def solution(mesh):
    tx_size = mesh.shape["tx"]
    ty_size = mesh.shape["ty"]

    def local_step(x_blk, dy_blk, gain_blk, w_gate_blk, w_up_blk, w_down_blk):
        rows, dl = x_blk.shape
        fl = w_gate_blk.shape[1]
        tok = rows * ty_size
        d_model = dl * tx_size
        n = fl // FC
        half = FC // 2
        f32, bf16 = jnp.float32, jnp.bfloat16
        anyspec = pl.BlockSpec(memory_space=pl.ANY)
        sem = pltpu.SemaphoreType.DMA
        vm = pl.BlockSpec(memory_space=pltpu.VMEM)
        S = jax.ShapeDtypeStruct
        V = pltpu.VMEM
        small = [((rows, dl), bf16), ((rows, dl), bf16), ((1, dl), f32)]
        outs = pl.pallas_call(
            functools.partial(branch_kernel, d_model, n),
            out_shape=[V((n, 2, tok, 3 * half), bf16), V((dl, tok), bf16), V((tok, dl), bf16)] + [V(*s) for s in small],
            in_specs=[anyspec] * 6,
            out_specs=[vm] * 6,
            scratch_shapes=[
                V((rows, dl), bf16), V((1, dl), f32), V((tok, dl), bf16),
                V((dl, fl), bf16), V((dl, fl), bf16), V((fl, dl), bf16),
                V((rows, dl), f32),
                V((P_SLOTS, 2, 2, rows, half), f32), V((L_SLOTS, 2, rows, half), f32),
                V((D_SLOTS, 2, 2, rows // 2, half), f32), V((L_SLOTS, 2, rows // 2, half), f32),
                V((2 * n, 2, 3, rows // 4, half), f32), V((2 * n, 2, 3, rows // 8, half), f32),
                V((2, 2, rows, dl), f32), V((2, rows, dl), f32),
                V((8, 8, 128), f32), V((8, 8, 128), f32), V((8, dl), f32), V((8, dl), f32),
                sem((3, n)), sem((3,)), sem((4,)), sem((4,)), sem((8,)), sem((8,)), sem((8,)), sem((8,)),
                sem((RING,)), sem((RING,)), sem((RING,)), sem((RING,)),
                *[sem((2, RING)) for _ in range(10)],
                sem((RING,)), sem((RING,)),
                *[sem((2, HELD)) for _ in range(4)], sem((HELD,)), sem((HELD,)),
            ],
            compiler_params=pltpu.CompilerParams(collective_id=0, has_side_effects=True, vmem_limit_bytes=VMEM_LIMIT),
            cost_estimate=pl.CostEstimate(flops=12 * tok * dl * fl, bytes_accessed=6 * dl * fl + 6 * tok * fl, transcendentals=0),
        )(x_blk, dy_blk, gain_blk[None, :], w_gate_blk, w_up_blk, w_down_blk)

        dwg, dwu, dwd, y_blk, dx_blk, dg = pl.pallas_call(
            weight_grad_kernel,
            out_shape=[S((dl, fl), f32)] * 2 + [S((fl, dl), f32)] + [S(*s) for s in small],
            in_specs=[vm] * 6,
            out_specs=[anyspec] * 6,
            scratch_shapes=[
                V((W_SLOTS, 2, dl, half), f32), V((W_SLOTS, half, dl), f32), sem((W_SLOTS, 3)), sem((3,)),
            ],
            compiler_params=pltpu.CompilerParams(vmem_limit_bytes=VMEM_LIMIT),
            cost_estimate=pl.CostEstimate(flops=6 * tok * dl * fl, bytes_accessed=12 * dl * fl + 6 * tok * fl, transcendentals=0),
        )(*[pltpu.with_memory_space_constraint(o, pltpu.VMEM) for o in outs])
        return (y_blk, dx_blk, dwg, dwu, dwd, dg[0])

    return jax.shard_map(
        local_step, mesh=mesh,
        in_specs=(P("ty", "tx"), P("ty", "tx"), P("tx"), P("tx", "ty"), P("tx", "ty"), P("ty", "tx")),
        out_specs=(P("ty", "tx"), P("ty", "tx"), P("tx", "ty"), P("tx", "ty"), P("ty", "tx"), P("tx")),
        check_vma=False)
```

```python
import functools

import jax
import jax.numpy as jnp
from jax import lax
from jax.experimental import pallas as pl
from jax.experimental.pallas import tpu as pltpu
from jax.sharding import PartitionSpec as P

LN_EPS = 1e-6
MESH = pl.DeviceIdType.MESH
FC = 512
OWN_FIRST = 8
LEAD = 8
P_SLOTS = 4
L_SLOTS = LEAD + P_SLOTS
HELD = 8
RING = 16
STAGES = (1, 2, 4, 5, 7, 8)
W_SLOTS = 2
W_UNITS = 2
VMEM_LIMIT = 48 * 1024 * 1024


def contract_rows(left_op, right_op):
    return lax.dot_general(left_op, right_op, (((0,), (0,)), ((), ())), preferred_element_type=jnp.float32)


def contract_cols(left_op, right_op):
    return lax.dot_general(left_op, right_op, (((1,), (1,)), ((), ())), preferred_element_type=jnp.float32)


def mo(value, multiple):
    return pl.multiple_of(value, multiple)


def branch_kernel(d_model, n_f,
                  x_hbm, dy_hbm, gain_hbm, wg_hbm, wu_hbm, wd_hbm,
                  gat, h_t, dya_ref, y_ref, dx_ref, dg_ref,
                  x_ref, gain_ref, h_ref,
                  wg, wu, wd, xh, part, part_d, dsum, dsum_d, r1, r2, acc, zin, st, rb, dgs, dgr,
                  wsem, isem, zs, zr, ss, sr, bs, br, ds, dr, dds, ddr, p1s, p1r, pds, pdr, p2s, p2r,
                  g1s, g1r, g2s, g2r, gds, gdr, a1s, a1r, a2s, a2r, ads, adr):
    half = FC // 2
    rows = x_ref.shape[0]
    q1, q2, q3 = rows // 2, rows // 4, rows // 8
    n_units = 2 * n_f
    last_oth = OWN_FIRST + n_f - 1
    held = n_units - HELD

    ty = lax.axis_index("ty")
    t = lax.axis_index("tx")
    c = lax.rem(t, 2)
    xc = lax.rem(lax.div(t, 2), 2)
    yc = lax.div(t, 4)
    dev_c = (ty, t + 1 - 2 * c)
    dev_x = (ty, t + 2 - 4 * xc)
    dev_y = (ty, t + 4 - 8 * yc)
    dev_z = (1 - ty, t)
    own = pl.ds(mo(ty * rows, rows), rows)
    oth = pl.ds(mo((1 - ty) * rows, rows), rows)

    def remote(src, dst, ssem, rsem, dev):
        return pltpu.make_async_remote_copy(src_ref=src, dst_ref=dst, send_sem=ssem, recv_sem=rsem,
                                            device_id=dev, device_id_type=MESH)

    def f_of(j):
        return lax.rem(j + (n_f - OWN_FIRST), n_f)

    def oth_of(j):
        return lax.rem(lax.div(j + (n_f - OWN_FIRST), n_f), 2)

    def base_of(j):
        k = oth_of(j)
        return (ty + k - 2 * ty * k) * rows

    def fcols(j):
        return pl.ds(mo(f_of(j) * FC, FC), FC)

    def rcols(j, r):
        return pl.ds(mo(f_of(j) * FC + r * half, half), half)

    def trows(j):
        return pl.ds(mo(base_of(j), rows), rows)

    def wcopy(k, i):
        cs = fcols(i)
        if k == 0:
            return pltpu.make_async_copy(wg_hbm.at[:, cs], wg.at[:, cs], wsem.at[0, i])
        if k == 1:
            return pltpu.make_async_copy(wu_hbm.at[:, cs], wu.at[:, cs], wsem.at[1, i])
        return pltpu.make_async_copy(wd_hbm.at[cs, :], wd.at[cs, :], wsem.at[2, i])

    in_dy = pltpu.make_async_copy(dy_hbm, dya_ref.at[own, :], isem.at[0])
    in_x = pltpu.make_async_copy(x_hbm, x_ref, isem.at[1])
    in_gain = pltpu.make_async_copy(gain_hbm, gain_ref, isem.at[2])
    in_x.start()
    in_dy.start()
    in_gain.start()
    for i in range(LEAD):
        wcopy(2, i).start()

    barrier = pltpu.get_barrier_semaphore()
    for o in range(1, 8):
        pl.semaphore_signal(barrier, inc=1, device_id=(ty, lax.rem(t + o, 8)), device_id_type=MESH)
    pl.semaphore_signal(barrier, inc=1, device_id=dev_z, device_id_type=MESH)

    def start_w(i, carry):
        wcopy(0, i).start()
        wcopy(1, i).start()

        @pl.when(i + LEAD < n_f)
        def _():
            wcopy(2, i + LEAD).start()
        return carry

    lax.fori_loop(0, n_f, start_w, 0)

    lane = lax.broadcasted_iota(jnp.int32, (rows, 128), 1)

    def pack_cols(c0, c1):
        both = jnp.where(lane == 0, c0, jnp.where(lane == 1, c1, 0.0))
        return both.T[0:8, :]

    def unpack_cols(packed):
        full = jnp.concatenate([packed, jnp.zeros((rows - 8, 128), jnp.float32)], axis=0).T
        return full[:, 0:1], full[:, 1:2]

    def send_stats(buf, ssem, rsem):
        for o in range(1, 8):
            remote(buf.at[t], buf.at[t], ssem.at[o], rsem.at[o], (ty, lax.rem(t + o, 8))).start()

    def total_stats(buf, ssem, rsem):
        for o in range(1, 8):
            q = lax.rem(t + 8 - o, 8)
            d = remote(buf.at[t], buf.at[q], ssem.at[o], rsem.at[o], (ty, q))
            d.wait_send()
            d.wait_recv()
        s = buf[0]
        for j in range(1, 8):
            s = s + buf[j]
        return unpack_cols(s)

    def seg(base, size):
        return pl.ds(mo(base, size), size)

    own_c = seg(c * q1, q1)
    oth_c = seg((1 - c) * q1, q1)
    keep1 = (seg(c * q1 + xc * q2, q2), seg(c * q1 + yc * q2, q2))
    send1 = (seg(c * q1 + (1 - xc) * q2, q2), seg(c * q1 + (1 - yc) * q2, q2))
    r_keep = (seg(yc * q3, q3), seg(xc * q3, q3))
    r_send = (seg((1 - yc) * q3, q3), seg((1 - xc) * q3, q3))
    lanes = [slice(k * half, (k + 1) * half) for k in range(3)]
    dev1, dev2 = (dev_x, dev_y), (dev_y, dev_x)
    g_c = (c * q1, (1 - c) * q1)
    g_keep1 = (c * q1 + xc * q2, c * q1 + yc * q2)
    g_send1 = (c * q1 + (1 - xc) * q2, c * q1 + (1 - yc) * q2)
    g_fin = (g_keep1[0] + yc * q3, g_keep1[1] + xc * q3)
    g_fin_n = (g_keep1[0] + (1 - yc) * q3, g_keep1[1] + (1 - xc) * q3)

    def grows(j, off, size):
        return pl.ds(mo(base_of(j) + off, size), size)

    def ring(j):
        return lax.rem(j, RING)

    def d_copy(j):
        slot = lax.rem(j, P_SLOTS)
        return remote(part.at[slot, :, :, oth_c, :], dsum.at[slot], ds.at[ring(j)], dr.at[ring(j)], dev_c)

    def dd_copy(j):
        slot = lax.rem(j, L_SLOTS)
        return remote(part_d.at[slot, :, oth_c, :], dsum_d.at[slot], dds.at[ring(j)], ddr.at[ring(j)], dev_c)

    def p1_copy(j, r):
        return remote(part.at[lax.rem(j, P_SLOTS), r, :, send1[r], :], r1.at[j, r, 0:2],
                      p1s.at[r, ring(j)], p1r.at[r, ring(j)], dev1[r])

    def pd_copy(j, r):
        return remote(part_d.at[lax.rem(j, L_SLOTS), r, send1[r], :], r1.at[j, r, 2],
                      pds.at[r, ring(j)], pdr.at[r, ring(j)], dev1[r])

    def p2_copy(j, r):
        return remote(r1.at[j, r, :, r_send[r], :], r2.at[j, r], p2s.at[r, ring(j)], p2r.at[r, ring(j)], dev2[r])

    def g1_copy(j, r, off, lo):
        ref = gat.at[f_of(j), r, grows(j, off[r], q3), lo * half:]
        return remote(ref, ref, g1s.at[r, ring(j)], g1r.at[r, ring(j)], dev2[r])

    def g2_copy(j, r, off, lo):
        ref = gat.at[f_of(j), r, grows(j, off[r], q2), lo * half:]
        return remote(ref, ref, g2s.at[r, ring(j)], g2r.at[r, ring(j)], dev1[r])

    def gd_copy(j, off, lo):
        ref = gat.at[f_of(j), :, grows(j, off, q1), lo * half:]
        return remote(ref, ref, gds.at[ring(j)], gdr.at[ring(j)], dev_c)

    def a1_copy(k, r, off):
        ref = gat.at[f_of(held + k), r, grows(held + k, off[r], q3), lanes[0]]
        return remote(ref, ref, a1s.at[r, k], a1r.at[r, k], dev2[r])

    def a2_copy(k, r, off):
        ref = gat.at[f_of(held + k), r, grows(held + k, off[r], q2), lanes[0]]
        return remote(ref, ref, a2s.at[r, k], a2r.at[r, k], dev1[r])

    def ad_copy(k, off):
        ref = gat.at[f_of(held + k), :, grows(held + k, off, q1), lanes[0]]
        return remote(ref, ref, ads.at[k], adr.at[k], dev_c)

    def by_arrays(j, body):
        @pl.when(j < held)
        def _():
            body(0)

        @pl.when(j >= held)
        def _():
            body(1)

    def each_held(body):
        def one(k, carry):
            body(k)
            return carry

        lax.fori_loop(0, HELD, one, 0)

    def da_dot(j):
        for r in range(2):
            part_d[lax.rem(j, L_SLOTS), r] = contract_cols(dya_ref[trows(j), :], wd[rcols(j, r), :])

    def da_product(j):
        da_dot(j)
        dd_copy(j).start()

    def da_pair_sum(j):
        dd_copy(j).wait_recv()
        slot = lax.rem(j, L_SLOTS)
        for r in range(2):
            part_d[slot, r, own_c, :] = part_d[slot, r, own_c, :] + dsum_d[slot, r]
            pd_copy(j, r).start()

    in_dy.wait()
    wcopy(2, 0).wait()
    da_dot(0)
    pl.semaphore_wait(barrier, 8)
    dd_copy(0).start()
    in_x.wait()
    x_own = x_ref[...].astype(jnp.float32)
    st[t] = pack_cols(jnp.sum(x_own, axis=1, keepdims=True), jnp.sum(x_own * x_own, axis=1, keepdims=True))
    send_stats(st, ss, sr)
    zdy = remote(dya_ref.at[own, :], dya_ref.at[own, :], zs.at[0], zr.at[0], dev_z)
    zdy.start()
    for i in range(1, 3):
        wcopy(2, i).wait()
        da_product(i)
    for i in range(LEAD):
        da_pair_sum(i)
        if i + 3 < LEAD:
            wcopy(2, i + 3).wait()
            da_product(i + 3)
    in_gain.wait()
    acc[...] = jnp.zeros_like(acc)

    gain = gain_ref[...]
    c0, c1 = total_stats(st, ss, sr)
    mean_x = c0 / d_model
    inv_std = lax.rsqrt(c1 / d_model - mean_x * mean_x + LN_EPS)
    xhat = (x_ref[...].astype(jnp.float32) - mean_x) * inv_std
    xh[...] = xhat
    h_ref[own, :] = (gain * xhat).astype(jnp.bfloat16)

    def h_copy(block):
        return remote(h_ref.at[own, :], h_ref.at[block, :], zs.at[1], zr.at[1], dev_z)

    h_copy(own).start()

    def m_part(f, rs, j):
        return sum(jnp.dot(gat[f, r, rs, lanes[0]], wd[rcols(j, r), :], preferred_element_type=jnp.float32) for r in range(2))

    z_sum = remote(acc.at[1], zin, zs.at[2], zr.at[2], dev_z)

    def step(i, carry):
        @pl.when(jnp.logical_and(i >= P_SLOTS, i < n_units + P_SLOTS))
        def _():
            j = i - P_SLOTS
            d_copy(j).wait_send()
            dd_copy(j).wait_send()
            for r in range(2):
                p1_copy(j, r).wait_send()
                pd_copy(j, r).wait_send()

        @pl.when(i < n_f)
        def _():
            wcopy(0, i).wait()
            wcopy(1, i).wait()

        @pl.when(i + LEAD < n_f)
        def _():
            wcopy(2, i + LEAD).wait()

        @pl.when(i == OWN_FIRST - LEAD)
        def _():
            remote(dya_ref.at[own, :], dya_ref.at[oth, :], zs.at[0], zr.at[0], dev_z).wait_recv()

        @pl.when(i == OWN_FIRST)
        def _():
            h_copy(oth).wait_recv()
            h_t[...] = h_ref[...].T

        @pl.when(i < n_units)
        def _():
            slot = lax.rem(i, P_SLOTS)
            h = h_ref[trows(i), :]
            for r in range(2):
                part[slot, r, 0] = jnp.dot(h, wg[:, rcols(i, r)], preferred_element_type=jnp.float32)
                part[slot, r, 1] = jnp.dot(h, wu[:, rcols(i, r)], preferred_element_type=jnp.float32)
            d_copy(i).start()

        @pl.when(i + LEAD < n_units)
        def _():
            da_product(i + LEAD)

        @pl.when(jnp.logical_and(i >= STAGES[0], i < n_units + STAGES[0]))
        def _():
            j = i - STAGES[0]
            d_copy(j).wait_recv()
            slot = lax.rem(j, P_SLOTS)
            for r in range(2):
                for k in range(2):
                    part[slot, r, k, own_c, :] = part[slot, r, k, own_c, :] + dsum[slot, r, k]
                p1_copy(j, r).start()

            @pl.when(j + LEAD < n_units)
            def _():
                da_pair_sum(j + LEAD)

        @pl.when(jnp.logical_and(i >= STAGES[1], i < n_units + STAGES[1]))
        def _():
            j = i - STAGES[1]
            slot = lax.rem(j, P_SLOTS)
            for r in range(2):
                pd_copy(j, r).wait_recv()
                p1_copy(j, r).wait_recv()
                for k in range(2):
                    r1[j, r, k] = r1[j, r, k] + part[slot, r, k, keep1[r], :]
                r1[j, r, 2] = r1[j, r, 2] + part_d[lax.rem(j, L_SLOTS), r, keep1[r], :]
                p2_copy(j, r).start()

        @pl.when(jnp.logical_and(i >= STAGES[2], i < n_units + STAGES[2]))
        def _():
            j = i - STAGES[2]
            for r in range(2):
                p2_copy(j, r).wait_recv()
                u = r1[j, r, 0, r_keep[r], :] + r2[j, r, 0]
                v = r1[j, r, 1, r_keep[r], :] + r2[j, r, 1]
                da = r1[j, r, 2, r_keep[r], :] + r2[j, r, 2]
                sig = jax.nn.sigmoid(u)
                swish = u * sig
                f = f_of(j)
                rs = grows(j, g_fin[r], q3)
                gat[f, r, rs, lanes[0]] = (swish * v).astype(jnp.bfloat16)
                gat[f, r, rs, lanes[1]] = (da * v * sig * (1.0 + u * (1.0 - sig))).astype(jnp.bfloat16)
                gat[f, r, rs, lanes[2]] = (da * swish).astype(jnp.bfloat16)
            by_arrays(j, lambda lo: [g1_copy(j, r, g_fin, lo).start() for r in range(2)])

        @pl.when(jnp.logical_and(i >= STAGES[3], i < n_units + STAGES[3]))
        def _():
            j = i - STAGES[3]

            def forward(lo):
                for r in range(2):
                    g1_copy(j, r, g_fin_n, lo).wait_recv()
                    g2_copy(j, r, g_keep1, lo).start()

            by_arrays(j, forward)

        @pl.when(jnp.logical_and(i >= STAGES[4], i < n_units + STAGES[4]))
        def _():
            j = i - STAGES[4]

            def to_core(lo):
                for r in range(2):
                    g2_copy(j, r, g_send1, lo).wait_recv()
                gd_copy(j, g_c[0], lo).start()

            by_arrays(j, to_core)

        @pl.when(i >= STAGES[5])
        def _():
            j = i - STAGES[5]
            by_arrays(j, lambda lo: gd_copy(j, g_c[1], lo).wait_recv())
            f = f_of(j)
            rs = trows(j)
            side = oth_of(j)

            @pl.when(j < held)
            def _():
                acc[side, 0] += m_part(f, rs, j)

            acc[side, 1] += sum(contract_cols(gat[f, r, rs, lanes[1]], wg[:, rcols(j, r)])
                                + contract_cols(gat[f, r, rs, lanes[2]], wu[:, rcols(j, r)]) for r in range(2))

            def sent(lo):
                for r in range(2):
                    p2_copy(j, r).wait_send()
                    g1_copy(j, r, g_fin, lo).wait_send()
                    g2_copy(j, r, g_keep1, lo).wait_send()
                gd_copy(j, g_c[0], lo).wait_send()

            by_arrays(j, sent)

            @pl.when(j == last_oth)
            def _():
                z_sum.start()

        @pl.when(i == n_units - 1 + STAGES[2])
        def _():
            each_held(lambda k: [a1_copy(k, r, g_fin).start() for r in range(2)])

        @pl.when(i == n_units - 1 + STAGES[3])
        def _():
            def forward(k):
                for r in range(2):
                    a1_copy(k, r, g_fin_n).wait_recv()
                    a2_copy(k, r, g_keep1).start()

            each_held(forward)
        return carry

    lax.fori_loop(0, n_units + STAGES[5], step, 0)

    z_sum.wait()
    d_hnorm = acc[0, 1] + zin[1]
    e = d_hnorm * gain
    rb[t] = pack_cols(jnp.sum(e, axis=1, keepdims=True), jnp.sum(e * xh[...], axis=1, keepdims=True))
    send_stats(rb, bs, br)
    dgs[...] = jnp.broadcast_to(jnp.sum(d_hnorm * xh[...], axis=0, keepdims=True), dgs.shape)
    z_dg = remote(dgs, dgr, zs.at[3], zr.at[3], dev_z)
    z_dg.start()

    def to_core(k):
        for r in range(2):
            a2_copy(k, r, g_send1).wait_recv()
        ad_copy(k, g_c[0]).start()

    each_held(to_core)

    def m_product(k):
        ad_copy(k, g_c[1]).wait_recv()
        acc[0, 0] += m_part(f_of(held + k), own, held + k)
        for r in range(2):
            a1_copy(k, r, g_fin).wait_send()
            a2_copy(k, r, g_keep1).wait_send()
        ad_copy(k, g_c[0]).wait_send()

    each_held(m_product)
    y_ref[...] = (x_ref[...].astype(jnp.float32) + (acc[0, 0] + zin[0])).astype(jnp.bfloat16)
    zdy.wait_send()
    h_copy(own).wait_send()
    c0, c1 = total_stats(rb, bs, br)
    dx_ln = inv_std * (e - c0 / d_model - xh[...] * (c1 / d_model))
    dx_ref[...] = (dya_ref[own, :].astype(jnp.float32) + dx_ln).astype(jnp.bfloat16)
    z_dg.wait()
    dg_ref[...] = dgs[0:1, :] + dgr[0:1, :]


def weight_grad_kernel(gat, h_t, dy_ref, y_in, dx_in, dg_in,
                       dwg_hbm, dwu_hbm, dwd_hbm, y_hbm, dx_hbm, dg_hbm, buf, buf2, bsem, ssem):
    n_f, _, _, width = gat.shape
    n_blocks = n_f // W_UNITS
    half = width // 3
    wb = 2 * half * W_UNITS

    def out_copy(b, k):
        cs = pl.ds(mo(b * wb, wb), wb)
        dst = (dwg_hbm.at[:, cs], dwu_hbm.at[:, cs], dwd_hbm.at[cs, :])[k]
        slot = lax.rem(b, W_SLOTS)
        src = buf.at[slot, k] if k < 2 else buf2.at[slot]
        return pltpu.make_async_copy(src, dst, bsem.at[slot, k])

    def block(b, carry):
        slot = lax.rem(b, W_SLOTS)
        for k in range(3):
            @pl.when(b >= W_SLOTS)
            def _():
                out_copy(b - W_SLOTS, k).wait()

            for q in range(2 * W_UNITS):
                rs = slice(q * half, (q + 1) * half)
                lane = (k + 1) % 3 * half
                src = gat[b * W_UNITS + q // 2, q % 2, :, lane:lane + half]
                if k < 2:
                    buf[slot, k, :, rs] = jnp.dot(h_t[...], src, preferred_element_type=jnp.float32)
                else:
                    buf2[slot, rs, :] = contract_rows(src, dy_ref[...])
            out_copy(b, k).start()
        return carry

    lax.fori_loop(0, n_blocks, block, 0)
    small = [pltpu.make_async_copy(src, dst, ssem.at[k])
             for k, (src, dst) in enumerate(((y_in, y_hbm), (dx_in, dx_hbm), (dg_in, dg_hbm)))]
    for d in small:
        d.start()

    def drain(b, carry):
        for k in range(3):
            out_copy(b, k).wait()
        return carry

    lax.fori_loop(n_blocks - W_SLOTS, n_blocks, drain, 0)
    for d in small:
        d.wait()


def solution(mesh):
    tx_size = mesh.shape["tx"]
    ty_size = mesh.shape["ty"]

    def local_step(x_blk, dy_blk, gain_blk, w_gate_blk, w_up_blk, w_down_blk):
        rows, dl = x_blk.shape
        fl = w_gate_blk.shape[1]
        tok = rows * ty_size
        d_model = dl * tx_size
        n = fl // FC
        half = FC // 2
        f32, bf16 = jnp.float32, jnp.bfloat16
        anyspec = pl.BlockSpec(memory_space=pl.ANY)
        sem = pltpu.SemaphoreType.DMA
        vm = pl.BlockSpec(memory_space=pltpu.VMEM)
        S = jax.ShapeDtypeStruct
        V = pltpu.VMEM
        small = [((rows, dl), bf16), ((rows, dl), bf16), ((1, dl), f32)]
        outs = pl.pallas_call(
            functools.partial(branch_kernel, d_model, n),
            out_shape=[V((n, 2, tok, 3 * half), bf16), V((dl, tok), bf16), V((tok, dl), bf16)] + [V(*s) for s in small],
            in_specs=[anyspec] * 6,
            out_specs=[vm] * 6,
            scratch_shapes=[
                V((rows, dl), bf16), V((1, dl), f32), V((tok, dl), bf16),
                V((dl, fl), bf16), V((dl, fl), bf16), V((fl, dl), bf16),
                V((rows, dl), f32),
                V((P_SLOTS, 2, 2, rows, half), f32), V((L_SLOTS, 2, rows, half), f32),
                V((P_SLOTS, 2, 2, rows // 2, half), f32), V((L_SLOTS, 2, rows // 2, half), f32),
                V((2 * n, 2, 3, rows // 4, half), f32), V((2 * n, 2, 3, rows // 8, half), f32),
                V((2, 2, rows, dl), f32), V((2, rows, dl), f32),
                V((8, 8, 128), f32), V((8, 8, 128), f32), V((8, dl), f32), V((8, dl), f32),
                sem((3, n)), sem((3,)), sem((4,)), sem((4,)), sem((8,)), sem((8,)), sem((8,)), sem((8,)),
                sem((RING,)), sem((RING,)), sem((RING,)), sem((RING,)),
                *[sem((2, RING)) for _ in range(10)],
                sem((RING,)), sem((RING,)),
                *[sem((2, HELD)) for _ in range(4)], sem((HELD,)), sem((HELD,)),
            ],
            compiler_params=pltpu.CompilerParams(collective_id=0, has_side_effects=True, vmem_limit_bytes=VMEM_LIMIT),
            cost_estimate=pl.CostEstimate(flops=12 * tok * dl * fl, bytes_accessed=6 * dl * fl + 6 * tok * fl, transcendentals=0),
        )(x_blk, dy_blk, gain_blk[None, :], w_gate_blk, w_up_blk, w_down_blk)

        dwg, dwu, dwd, y_blk, dx_blk, dg = pl.pallas_call(
            weight_grad_kernel,
            out_shape=[S((dl, fl), f32)] * 2 + [S((fl, dl), f32)] + [S(*s) for s in small],
            in_specs=[vm] * 6,
            out_specs=[anyspec] * 6,
            scratch_shapes=[
                V((W_SLOTS, 2, dl, FC * W_UNITS), f32), V((W_SLOTS, FC * W_UNITS, dl), f32), sem((W_SLOTS, 3)), sem((3,)),
            ],
            compiler_params=pltpu.CompilerParams(vmem_limit_bytes=VMEM_LIMIT),
            cost_estimate=pl.CostEstimate(flops=6 * tok * dl * fl, bytes_accessed=12 * dl * fl + 6 * tok * fl, transcendentals=0),
        )(*[pltpu.with_memory_space_constraint(o, pltpu.VMEM) for o in outs])
        return (y_blk, dx_blk, dwg, dwu, dwd, dg[0])

    return jax.shard_map(
        local_step, mesh=mesh,
        in_specs=(P("ty", "tx"), P("ty", "tx"), P("tx"), P("tx", "ty"), P("tx", "ty"), P("ty", "tx")),
        out_specs=(P("ty", "tx"), P("ty", "tx"), P("tx", "ty"), P("tx", "ty"), P("ty", "tx"), P("tx")),
        check_vma=False)
```

```python
import functools

import jax
import jax.numpy as jnp
from jax import lax
from jax.experimental import pallas as pl
from jax.experimental.pallas import tpu as pltpu
from jax.sharding import PartitionSpec as P

LN_EPS = 1e-6
MESH = pl.DeviceIdType.MESH
FC = 512
OWN_FIRST = 8
LEAD = 8
P_SLOTS = 4
L_SLOTS = LEAD + P_SLOTS
HELD = 8
RING = 16
STAGES = (1, 3, 5, 7, 8, 9)
W_SLOTS = 3
VMEM_LIMIT = 48 * 1024 * 1024


def contract_rows(left_op, right_op):
    return lax.dot_general(left_op, right_op, (((0,), (0,)), ((), ())), preferred_element_type=jnp.float32)


def contract_cols(left_op, right_op):
    return lax.dot_general(left_op, right_op, (((1,), (1,)), ((), ())), preferred_element_type=jnp.float32)


def mo(value, multiple):
    return pl.multiple_of(value, multiple)


def branch_kernel(d_model, n_f,
                  x_hbm, dy_hbm, gain_hbm, wg_hbm, wu_hbm, wd_hbm,
                  gat, h_t, dya_ref, y_ref, dx_ref, dg_ref,
                  x_ref, gain_ref, h_ref,
                  wg, wu, wd, xh, part, part_d, dsum, dsum_d, r1, r2, acc, zin, st, rb, dgs, dgr,
                  wsem, isem, zs, zr, ss, sr, bs, br, ds, dr, dds, ddr, p1s, p1r, pds, pdr, p2s, p2r,
                  g1s, g1r, g2s, g2r, gds, gdr, a1s, a1r, a2s, a2r, ads, adr):
    half = FC // 2
    rows = x_ref.shape[0]
    q1, q2, q3 = rows // 2, rows // 4, rows // 8
    n_units = 2 * n_f
    last_oth = OWN_FIRST + n_f - 1
    held = n_units - HELD

    ty = lax.axis_index("ty")
    t = lax.axis_index("tx")
    c = lax.rem(t, 2)
    xc = lax.rem(lax.div(t, 2), 2)
    yc = lax.div(t, 4)
    dev_c = (ty, t + 1 - 2 * c)
    dev_x = (ty, t + 2 - 4 * xc)
    dev_y = (ty, t + 4 - 8 * yc)
    dev_z = (1 - ty, t)
    own = pl.ds(mo(ty * rows, rows), rows)
    oth = pl.ds(mo((1 - ty) * rows, rows), rows)

    def remote(src, dst, ssem, rsem, dev):
        return pltpu.make_async_remote_copy(src_ref=src, dst_ref=dst, send_sem=ssem, recv_sem=rsem,
                                            device_id=dev, device_id_type=MESH)

    def f_of(j):
        return lax.rem(j + (n_f - OWN_FIRST), n_f)

    def oth_of(j):
        return lax.rem(lax.div(j + (n_f - OWN_FIRST), n_f), 2)

    def base_of(j):
        k = oth_of(j)
        return (ty + k - 2 * ty * k) * rows

    def fcols(j):
        return pl.ds(mo(f_of(j) * FC, FC), FC)

    def rcols(j, r):
        return pl.ds(mo(f_of(j) * FC + r * half, half), half)

    def trows(j):
        return pl.ds(mo(base_of(j), rows), rows)

    def wcopy(k, i):
        cs = fcols(i)
        if k == 0:
            return pltpu.make_async_copy(wg_hbm.at[:, cs], wg.at[:, cs], wsem.at[0, i])
        if k == 1:
            return pltpu.make_async_copy(wu_hbm.at[:, cs], wu.at[:, cs], wsem.at[1, i])
        return pltpu.make_async_copy(wd_hbm.at[cs, :], wd.at[cs, :], wsem.at[2, i])

    in_dy = pltpu.make_async_copy(dy_hbm, dya_ref.at[own, :], isem.at[0])
    in_x = pltpu.make_async_copy(x_hbm, x_ref, isem.at[1])
    in_gain = pltpu.make_async_copy(gain_hbm, gain_ref, isem.at[2])
    in_x.start()
    in_dy.start()
    in_gain.start()
    for i in range(LEAD):
        wcopy(2, i).start()

    barrier = pltpu.get_barrier_semaphore()
    for o in range(1, 8):
        pl.semaphore_signal(barrier, inc=1, device_id=(ty, lax.rem(t + o, 8)), device_id_type=MESH)
    pl.semaphore_signal(barrier, inc=1, device_id=dev_z, device_id_type=MESH)

    def start_w(i, carry):
        wcopy(0, i).start()
        wcopy(1, i).start()

        @pl.when(i + LEAD < n_f)
        def _():
            wcopy(2, i + LEAD).start()
        return carry

    lax.fori_loop(0, n_f, start_w, 0)

    lane = lax.broadcasted_iota(jnp.int32, (rows, 128), 1)

    def pack_cols(c0, c1):
        both = jnp.where(lane == 0, c0, jnp.where(lane == 1, c1, 0.0))
        return both.T[0:8, :]

    def unpack_cols(packed):
        full = jnp.concatenate([packed, jnp.zeros((rows - 8, 128), jnp.float32)], axis=0).T
        return full[:, 0:1], full[:, 1:2]

    def send_stats(buf, ssem, rsem):
        for o in range(1, 8):
            remote(buf.at[t], buf.at[t], ssem.at[o], rsem.at[o], (ty, lax.rem(t + o, 8))).start()

    def total_stats(buf, ssem, rsem):
        for o in range(1, 8):
            q = lax.rem(t + 8 - o, 8)
            d = remote(buf.at[t], buf.at[q], ssem.at[o], rsem.at[o], (ty, q))
            d.wait_send()
            d.wait_recv()
        s = buf[0]
        for j in range(1, 8):
            s = s + buf[j]
        return unpack_cols(s)

    def seg(base, size):
        return pl.ds(mo(base, size), size)

    own_c = seg(c * q1, q1)
    oth_c = seg((1 - c) * q1, q1)
    keep1 = (seg(c * q1 + xc * q2, q2), seg(c * q1 + yc * q2, q2))
    send1 = (seg(c * q1 + (1 - xc) * q2, q2), seg(c * q1 + (1 - yc) * q2, q2))
    r_keep = (seg(yc * q3, q3), seg(xc * q3, q3))
    r_send = (seg((1 - yc) * q3, q3), seg((1 - xc) * q3, q3))
    lanes = [slice(k * half, (k + 1) * half) for k in range(3)]
    dev1, dev2 = (dev_x, dev_y), (dev_y, dev_x)
    g_c = (c * q1, (1 - c) * q1)
    g_keep1 = (c * q1 + xc * q2, c * q1 + yc * q2)
    g_send1 = (c * q1 + (1 - xc) * q2, c * q1 + (1 - yc) * q2)
    g_fin = (g_keep1[0] + yc * q3, g_keep1[1] + xc * q3)
    g_fin_n = (g_keep1[0] + (1 - yc) * q3, g_keep1[1] + (1 - xc) * q3)

    def grows(j, off, size):
        return pl.ds(mo(base_of(j) + off, size), size)

    def ring(j):
        return lax.rem(j, RING)

    def d_copy(j):
        slot = lax.rem(j, P_SLOTS)
        return remote(part.at[slot, :, :, oth_c, :], dsum.at[slot], ds.at[ring(j)], dr.at[ring(j)], dev_c)

    def dd_copy(j):
        slot = lax.rem(j, L_SLOTS)
        return remote(part_d.at[slot, :, oth_c, :], dsum_d.at[slot], dds.at[ring(j)], ddr.at[ring(j)], dev_c)

    def p1_copy(j, r):
        return remote(part.at[lax.rem(j, P_SLOTS), r, :, send1[r], :], r1.at[j, r, 0:2],
                      p1s.at[r, ring(j)], p1r.at[r, ring(j)], dev1[r])

    def pd_copy(j, r):
        return remote(part_d.at[lax.rem(j, L_SLOTS), r, send1[r], :], r1.at[j, r, 2],
                      pds.at[r, ring(j)], pdr.at[r, ring(j)], dev1[r])

    def p2_copy(j, r):
        return remote(r1.at[j, r, :, r_send[r], :], r2.at[j, r], p2s.at[r, ring(j)], p2r.at[r, ring(j)], dev2[r])

    def g1_copy(j, r, off, lo):
        ref = gat.at[f_of(j), r, grows(j, off[r], q3), lo * half:]
        return remote(ref, ref, g1s.at[r, ring(j)], g1r.at[r, ring(j)], dev2[r])

    def g2_copy(j, r, off, lo):
        ref = gat.at[f_of(j), r, grows(j, off[r], q2), lo * half:]
        return remote(ref, ref, g2s.at[r, ring(j)], g2r.at[r, ring(j)], dev1[r])

    def gd_copy(j, off, lo):
        ref = gat.at[f_of(j), :, grows(j, off, q1), lo * half:]
        return remote(ref, ref, gds.at[ring(j)], gdr.at[ring(j)], dev_c)

    def a1_copy(k, r, off):
        ref = gat.at[f_of(held + k), r, grows(held + k, off[r], q3), lanes[0]]
        return remote(ref, ref, a1s.at[r, k], a1r.at[r, k], dev2[r])

    def a2_copy(k, r, off):
        ref = gat.at[f_of(held + k), r, grows(held + k, off[r], q2), lanes[0]]
        return remote(ref, ref, a2s.at[r, k], a2r.at[r, k], dev1[r])

    def ad_copy(k, off):
        ref = gat.at[f_of(held + k), :, grows(held + k, off, q1), lanes[0]]
        return remote(ref, ref, ads.at[k], adr.at[k], dev_c)

    def by_arrays(j, body):
        @pl.when(j < held)
        def _():
            body(0)

        @pl.when(j >= held)
        def _():
            body(1)

    def each_held(body):
        def one(k, carry):
            body(k)
            return carry

        lax.fori_loop(0, HELD, one, 0)

    def da_dot(j):
        for r in range(2):
            part_d[lax.rem(j, L_SLOTS), r] = contract_cols(dya_ref[trows(j), :], wd[rcols(j, r), :])

    def da_product(j):
        da_dot(j)
        dd_copy(j).start()

    def da_pair_sum(j):
        dd_copy(j).wait_recv()
        slot = lax.rem(j, L_SLOTS)
        for r in range(2):
            part_d[slot, r, own_c, :] = part_d[slot, r, own_c, :] + dsum_d[slot, r]
            pd_copy(j, r).start()

    in_dy.wait()
    wcopy(2, 0).wait()
    da_dot(0)
    pl.semaphore_wait(barrier, 8)
    dd_copy(0).start()
    in_x.wait()
    x_own = x_ref[...].astype(jnp.float32)
    st[t] = pack_cols(jnp.sum(x_own, axis=1, keepdims=True), jnp.sum(x_own * x_own, axis=1, keepdims=True))
    send_stats(st, ss, sr)
    zdy = remote(dya_ref.at[own, :], dya_ref.at[own, :], zs.at[0], zr.at[0], dev_z)
    zdy.start()
    for i in range(1, 3):
        wcopy(2, i).wait()
        da_product(i)
    for i in range(LEAD):
        da_pair_sum(i)
        if i + 3 < LEAD:
            wcopy(2, i + 3).wait()
            da_product(i + 3)
    in_gain.wait()
    acc[...] = jnp.zeros_like(acc)

    gain = gain_ref[...]
    c0, c1 = total_stats(st, ss, sr)
    mean_x = c0 / d_model
    inv_std = lax.rsqrt(c1 / d_model - mean_x * mean_x + LN_EPS)
    xhat = (x_ref[...].astype(jnp.float32) - mean_x) * inv_std
    xh[...] = xhat
    h_ref[own, :] = (gain * xhat).astype(jnp.bfloat16)

    def h_copy(block):
        return remote(h_ref.at[own, :], h_ref.at[block, :], zs.at[1], zr.at[1], dev_z)

    h_copy(own).start()

    def m_part(f, rs, j):
        return sum(jnp.dot(gat[f, r, rs, lanes[0]], wd[rcols(j, r), :], preferred_element_type=jnp.float32) for r in range(2))

    z_sum = remote(acc.at[1], zin, zs.at[2], zr.at[2], dev_z)

    def step(i, carry):
        @pl.when(jnp.logical_and(i >= P_SLOTS, i < n_units + P_SLOTS))
        def _():
            j = i - P_SLOTS
            d_copy(j).wait_send()
            dd_copy(j).wait_send()
            for r in range(2):
                p1_copy(j, r).wait_send()
                pd_copy(j, r).wait_send()

        @pl.when(i < n_f)
        def _():
            wcopy(0, i).wait()
            wcopy(1, i).wait()

        @pl.when(i + LEAD < n_f)
        def _():
            wcopy(2, i + LEAD).wait()

        @pl.when(i == OWN_FIRST - LEAD)
        def _():
            remote(dya_ref.at[own, :], dya_ref.at[oth, :], zs.at[0], zr.at[0], dev_z).wait_recv()

        @pl.when(i == OWN_FIRST)
        def _():
            h_copy(oth).wait_recv()
            h_t[...] = h_ref[...].T

        @pl.when(i < n_units)
        def _():
            slot = lax.rem(i, P_SLOTS)
            h = h_ref[trows(i), :]
            for r in range(2):
                part[slot, r, 0] = jnp.dot(h, wg[:, rcols(i, r)], preferred_element_type=jnp.float32)
                part[slot, r, 1] = jnp.dot(h, wu[:, rcols(i, r)], preferred_element_type=jnp.float32)
            d_copy(i).start()

        @pl.when(i + LEAD < n_units)
        def _():
            da_product(i + LEAD)

        @pl.when(jnp.logical_and(i >= STAGES[0], i < n_units + STAGES[0]))
        def _():
            j = i - STAGES[0]
            d_copy(j).wait_recv()
            slot = lax.rem(j, P_SLOTS)
            for r in range(2):
                for k in range(2):
                    part[slot, r, k, own_c, :] = part[slot, r, k, own_c, :] + dsum[slot, r, k]
                p1_copy(j, r).start()

            @pl.when(j + LEAD < n_units)
            def _():
                da_pair_sum(j + LEAD)

        @pl.when(jnp.logical_and(i >= STAGES[1], i < n_units + STAGES[1]))
        def _():
            j = i - STAGES[1]
            slot = lax.rem(j, P_SLOTS)
            for r in range(2):
                pd_copy(j, r).wait_recv()
                p1_copy(j, r).wait_recv()
                for k in range(2):
                    r1[j, r, k] = r1[j, r, k] + part[slot, r, k, keep1[r], :]
                r1[j, r, 2] = r1[j, r, 2] + part_d[lax.rem(j, L_SLOTS), r, keep1[r], :]
                p2_copy(j, r).start()

        @pl.when(jnp.logical_and(i >= STAGES[2], i < n_units + STAGES[2]))
        def _():
            j = i - STAGES[2]
            for r in range(2):
                p2_copy(j, r).wait_recv()
                u = r1[j, r, 0, r_keep[r], :] + r2[j, r, 0]
                v = r1[j, r, 1, r_keep[r], :] + r2[j, r, 1]
                da = r1[j, r, 2, r_keep[r], :] + r2[j, r, 2]
                sig = jax.nn.sigmoid(u)
                swish = u * sig
                f = f_of(j)
                rs = grows(j, g_fin[r], q3)
                gat[f, r, rs, lanes[0]] = (swish * v).astype(jnp.bfloat16)
                gat[f, r, rs, lanes[1]] = (da * v * sig * (1.0 + u * (1.0 - sig))).astype(jnp.bfloat16)
                gat[f, r, rs, lanes[2]] = (da * swish).astype(jnp.bfloat16)
            by_arrays(j, lambda lo: [g1_copy(j, r, g_fin, lo).start() for r in range(2)])

        @pl.when(jnp.logical_and(i >= STAGES[3], i < n_units + STAGES[3]))
        def _():
            j = i - STAGES[3]

            def forward(lo):
                for r in range(2):
                    g1_copy(j, r, g_fin_n, lo).wait_recv()
                    g2_copy(j, r, g_keep1, lo).start()

            by_arrays(j, forward)

        @pl.when(jnp.logical_and(i >= STAGES[4], i < n_units + STAGES[4]))
        def _():
            j = i - STAGES[4]

            def to_core(lo):
                for r in range(2):
                    g2_copy(j, r, g_send1, lo).wait_recv()
                gd_copy(j, g_c[0], lo).start()

            by_arrays(j, to_core)

        @pl.when(i >= STAGES[5])
        def _():
            j = i - STAGES[5]
            by_arrays(j, lambda lo: gd_copy(j, g_c[1], lo).wait_recv())
            f = f_of(j)
            rs = trows(j)
            side = oth_of(j)

            @pl.when(j < held)
            def _():
                acc[side, 0] += m_part(f, rs, j)

            acc[side, 1] += sum(contract_cols(gat[f, r, rs, lanes[1]], wg[:, rcols(j, r)])
                                + contract_cols(gat[f, r, rs, lanes[2]], wu[:, rcols(j, r)]) for r in range(2))

            def sent(lo):
                for r in range(2):
                    p2_copy(j, r).wait_send()
                    g1_copy(j, r, g_fin, lo).wait_send()
                    g2_copy(j, r, g_keep1, lo).wait_send()
                gd_copy(j, g_c[0], lo).wait_send()

            by_arrays(j, sent)

            @pl.when(j == last_oth)
            def _():
                z_sum.start()

        @pl.when(i == n_units - 1 + STAGES[2])
        def _():
            each_held(lambda k: [a1_copy(k, r, g_fin).start() for r in range(2)])

        @pl.when(i == n_units - 1 + STAGES[3])
        def _():
            def forward(k):
                for r in range(2):
                    a1_copy(k, r, g_fin_n).wait_recv()
                    a2_copy(k, r, g_keep1).start()

            each_held(forward)
        return carry

    lax.fori_loop(0, n_units + STAGES[5], step, 0)

    z_sum.wait()
    d_hnorm = acc[0, 1] + zin[1]
    e = d_hnorm * gain
    rb[t] = pack_cols(jnp.sum(e, axis=1, keepdims=True), jnp.sum(e * xh[...], axis=1, keepdims=True))
    send_stats(rb, bs, br)
    dgs[...] = jnp.broadcast_to(jnp.sum(d_hnorm * xh[...], axis=0, keepdims=True), dgs.shape)
    z_dg = remote(dgs, dgr, zs.at[3], zr.at[3], dev_z)
    z_dg.start()

    def to_core(k):
        for r in range(2):
            a2_copy(k, r, g_send1).wait_recv()
        ad_copy(k, g_c[0]).start()

    each_held(to_core)

    def m_product(k):
        ad_copy(k, g_c[1]).wait_recv()
        acc[0, 0] += m_part(f_of(held + k), own, held + k)
        for r in range(2):
            a1_copy(k, r, g_fin).wait_send()
            a2_copy(k, r, g_keep1).wait_send()
        ad_copy(k, g_c[0]).wait_send()

    each_held(m_product)
    y_ref[...] = (x_ref[...].astype(jnp.float32) + (acc[0, 0] + zin[0])).astype(jnp.bfloat16)
    zdy.wait_send()
    h_copy(own).wait_send()
    c0, c1 = total_stats(rb, bs, br)
    dx_ln = inv_std * (e - c0 / d_model - xh[...] * (c1 / d_model))
    dx_ref[...] = (dya_ref[own, :].astype(jnp.float32) + dx_ln).astype(jnp.bfloat16)
    z_dg.wait()
    dg_ref[...] = dgs[0:1, :] + dgr[0:1, :]


def weight_grad_kernel(gat, h_t, dy_ref, y_in, dx_in, dg_in,
                       dwg_hbm, dwu_hbm, dwd_hbm, y_hbm, dx_hbm, dg_hbm, buf, bsem, ssem):
    n_blocks, _, _, width = gat.shape
    half = width // 3
    WB = 2 * half

    def out_copy(b, k):
        cs = pl.ds(mo(b * WB, WB), WB)
        dst = (dwg_hbm.at[:, cs], dwu_hbm.at[:, cs], dwd_hbm.at[cs, :])[k]
        slot = lax.rem(b, W_SLOTS)
        return pltpu.make_async_copy(buf.at[slot, k], dst, bsem.at[slot, k])

    def block(b, carry):
        slot = lax.rem(b, W_SLOTS)
        for k in range(3):
            @pl.when(b >= W_SLOTS)
            def _():
                out_copy(b - W_SLOTS, k).wait()

            for r in range(2):
                rs = slice(r * half, (r + 1) * half)
                src = gat[b, r, :, (k + 1) % 3 * half:((k + 1) % 3 + 1) * half]
                if k < 2:
                    buf[slot, k, :, rs] = jnp.dot(h_t[...], src, preferred_element_type=jnp.float32)
                else:
                    buf[slot, k, rs, :] = contract_rows(src, dy_ref[...])
            out_copy(b, k).start()
        return carry

    lax.fori_loop(0, n_blocks, block, 0)
    small = [pltpu.make_async_copy(src, dst, ssem.at[k])
             for k, (src, dst) in enumerate(((y_in, y_hbm), (dx_in, dx_hbm), (dg_in, dg_hbm)))]
    for d in small:
        d.start()

    def drain(b, carry):
        for k in range(3):
            out_copy(b, k).wait()
        return carry

    lax.fori_loop(n_blocks - W_SLOTS, n_blocks, drain, 0)
    for d in small:
        d.wait()


def solution(mesh):
    tx_size = mesh.shape["tx"]
    ty_size = mesh.shape["ty"]

    def local_step(x_blk, dy_blk, gain_blk, w_gate_blk, w_up_blk, w_down_blk):
        rows, dl = x_blk.shape
        fl = w_gate_blk.shape[1]
        tok = rows * ty_size
        d_model = dl * tx_size
        n = fl // FC
        half = FC // 2
        f32, bf16 = jnp.float32, jnp.bfloat16
        anyspec = pl.BlockSpec(memory_space=pl.ANY)
        sem = pltpu.SemaphoreType.DMA
        vm = pl.BlockSpec(memory_space=pltpu.VMEM)
        S = jax.ShapeDtypeStruct
        V = pltpu.VMEM
        small = [((rows, dl), bf16), ((rows, dl), bf16), ((1, dl), f32)]
        outs = pl.pallas_call(
            functools.partial(branch_kernel, d_model, n),
            out_shape=[V((n, 2, tok, 3 * half), bf16), V((dl, tok), bf16), V((tok, dl), bf16)] + [V(*s) for s in small],
            in_specs=[anyspec] * 6,
            out_specs=[vm] * 6,
            scratch_shapes=[
                V((rows, dl), bf16), V((1, dl), f32), V((tok, dl), bf16),
                V((dl, fl), bf16), V((dl, fl), bf16), V((fl, dl), bf16),
                V((rows, dl), f32),
                V((P_SLOTS, 2, 2, rows, half), f32), V((L_SLOTS, 2, rows, half), f32),
                V((P_SLOTS, 2, 2, rows // 2, half), f32), V((L_SLOTS, 2, rows // 2, half), f32),
                V((2 * n, 2, 3, rows // 4, half), f32), V((2 * n, 2, 3, rows // 8, half), f32),
                V((2, 2, rows, dl), f32), V((2, rows, dl), f32),
                V((8, 8, 128), f32), V((8, 8, 128), f32), V((8, dl), f32), V((8, dl), f32),
                sem((3, n)), sem((3,)), sem((4,)), sem((4,)), sem((8,)), sem((8,)), sem((8,)), sem((8,)),
                sem((RING,)), sem((RING,)), sem((RING,)), sem((RING,)),
                *[sem((2, RING)) for _ in range(10)],
                sem((RING,)), sem((RING,)),
                *[sem((2, HELD)) for _ in range(4)], sem((HELD,)), sem((HELD,)),
            ],
            compiler_params=pltpu.CompilerParams(collective_id=0, has_side_effects=True, vmem_limit_bytes=VMEM_LIMIT),
            cost_estimate=pl.CostEstimate(flops=12 * tok * dl * fl, bytes_accessed=6 * dl * fl + 6 * tok * fl, transcendentals=0),
        )(x_blk, dy_blk, gain_blk[None, :], w_gate_blk, w_up_blk, w_down_blk)

        dwg, dwu, dwd, y_blk, dx_blk, dg = pl.pallas_call(
            weight_grad_kernel,
            out_shape=[S((dl, fl), f32)] * 2 + [S((fl, dl), f32)] + [S(*s) for s in small],
            in_specs=[vm] * 6,
            out_specs=[anyspec] * 6,
            scratch_shapes=[
                V((W_SLOTS, 3, dl, FC), f32), sem((W_SLOTS, 3)), sem((3,)),
            ],
            compiler_params=pltpu.CompilerParams(vmem_limit_bytes=VMEM_LIMIT),
            cost_estimate=pl.CostEstimate(flops=6 * tok * dl * fl, bytes_accessed=12 * dl * fl + 6 * tok * fl, transcendentals=0),
        )(*[pltpu.with_memory_space_constraint(o, pltpu.VMEM) for o in outs])
        return (y_blk, dx_blk, dwg, dwu, dwd, dg[0])

    return jax.shard_map(
        local_step, mesh=mesh,
        in_specs=(P("ty", "tx"), P("ty", "tx"), P("tx"), P("tx", "ty"), P("tx", "ty"), P("ty", "tx")),
        out_specs=(P("ty", "tx"), P("ty", "tx"), P("tx", "ty"), P("tx", "ty"), P("ty", "tx"), P("tx")),
        check_vma=False)
```

```python
import functools

import jax
import jax.numpy as jnp
from jax import lax
from jax.experimental import pallas as pl
from jax.experimental.pallas import tpu as pltpu
from jax.sharding import PartitionSpec as P

LN_EPS = 1e-6
MESH = pl.DeviceIdType.MESH
FC = 512
OWN_FIRST = 8
LEAD = 8
P_SLOTS = 4
L_SLOTS = LEAD + P_SLOTS
HELD = 8
RING = 16
STAGES = (1, 3, 5, 7, 9, 10)
W_SLOTS = 3
VMEM_LIMIT = 48 * 1024 * 1024


def contract_rows(left_op, right_op):
    return lax.dot_general(left_op, right_op, (((0,), (0,)), ((), ())), preferred_element_type=jnp.float32)


def contract_cols(left_op, right_op):
    return lax.dot_general(left_op, right_op, (((1,), (1,)), ((), ())), preferred_element_type=jnp.float32)


def mo(value, multiple):
    return pl.multiple_of(value, multiple)


def branch_kernel(d_model, n_f,
                  x_hbm, dy_hbm, gain_hbm, wg_hbm, wu_hbm, wd_hbm,
                  gat, h_t, dya_ref, y_ref, dx_ref, dg_ref,
                  x_ref, gain_ref, h_ref,
                  wg, wu, wd, xh, part, part_d, dsum, dsum_d, r1, r2, ga, acc, zin, st, rb, dgs, dgr,
                  wsem, isem, zs, zr, ss, sr, bs, br, ds, dr, dds, ddr, p1s, p1r, pds, pdr, p2s, p2r,
                  g1s, g1r, g2s, g2r, gds, gdr, a1s, a1r, a2s, a2r, ads, adr):
    half = FC // 2
    rows = x_ref.shape[0]
    q1, q2, q3 = rows // 2, rows // 4, rows // 8
    n_units = 2 * n_f
    last_oth = OWN_FIRST + n_f - 1
    held = n_units - HELD

    ty = lax.axis_index("ty")
    t = lax.axis_index("tx")
    c = lax.rem(t, 2)
    xc = lax.rem(lax.div(t, 2), 2)
    yc = lax.div(t, 4)
    dev_c = (ty, t + 1 - 2 * c)
    dev_x = (ty, t + 2 - 4 * xc)
    dev_y = (ty, t + 4 - 8 * yc)
    dev_z = (1 - ty, t)
    own = pl.ds(mo(ty * rows, rows), rows)
    oth = pl.ds(mo((1 - ty) * rows, rows), rows)

    def remote(src, dst, ssem, rsem, dev):
        return pltpu.make_async_remote_copy(src_ref=src, dst_ref=dst, send_sem=ssem, recv_sem=rsem,
                                            device_id=dev, device_id_type=MESH)

    def f_of(j):
        return lax.rem(j + (n_f - OWN_FIRST), n_f)

    def oth_of(j):
        return lax.rem(lax.div(j + (n_f - OWN_FIRST), n_f), 2)

    def base_of(j):
        k = oth_of(j)
        return (ty + k - 2 * ty * k) * rows

    def fcols(j):
        return pl.ds(mo(f_of(j) * FC, FC), FC)

    def rcols(j, r):
        return pl.ds(mo(f_of(j) * FC + r * half, half), half)

    def trows(j):
        return pl.ds(mo(base_of(j), rows), rows)

    def wcopy(k, i):
        cs = fcols(i)
        if k == 0:
            return pltpu.make_async_copy(wg_hbm.at[:, cs], wg.at[:, cs], wsem.at[0, i])
        if k == 1:
            return pltpu.make_async_copy(wu_hbm.at[:, cs], wu.at[:, cs], wsem.at[1, i])
        return pltpu.make_async_copy(wd_hbm.at[cs, :], wd.at[cs, :], wsem.at[2, i])

    in_dy = pltpu.make_async_copy(dy_hbm, dya_ref.at[own, :], isem.at[0])
    in_x = pltpu.make_async_copy(x_hbm, x_ref, isem.at[1])
    in_gain = pltpu.make_async_copy(gain_hbm, gain_ref, isem.at[2])
    in_x.start()
    in_dy.start()
    in_gain.start()
    for i in range(LEAD):
        wcopy(2, i).start()

    barrier = pltpu.get_barrier_semaphore()
    for o in range(1, 8):
        pl.semaphore_signal(barrier, inc=1, device_id=(ty, lax.rem(t + o, 8)), device_id_type=MESH)
    pl.semaphore_signal(barrier, inc=1, device_id=dev_z, device_id_type=MESH)

    def start_w(i, carry):
        wcopy(0, i).start()
        wcopy(1, i).start()

        @pl.when(i + LEAD < n_f)
        def _():
            wcopy(2, i + LEAD).start()
        return carry

    lax.fori_loop(0, n_f, start_w, 0)

    lane = lax.broadcasted_iota(jnp.int32, (rows, 128), 1)

    def pack_cols(c0, c1):
        both = jnp.where(lane == 0, c0, jnp.where(lane == 1, c1, 0.0))
        return both.T[0:8, :]

    def unpack_cols(packed):
        full = jnp.concatenate([packed, jnp.zeros((rows - 8, 128), jnp.float32)], axis=0).T
        return full[:, 0:1], full[:, 1:2]

    def send_stats(buf, ssem, rsem):
        for o in range(1, 8):
            remote(buf.at[t], buf.at[t], ssem.at[o], rsem.at[o], (ty, lax.rem(t + o, 8))).start()

    def total_stats(buf, ssem, rsem):
        for o in range(1, 8):
            q = lax.rem(t + 8 - o, 8)
            d = remote(buf.at[t], buf.at[q], ssem.at[o], rsem.at[o], (ty, q))
            d.wait_send()
            d.wait_recv()
        s = buf[0]
        for j in range(1, 8):
            s = s + buf[j]
        return unpack_cols(s)

    def seg(base, size):
        return pl.ds(mo(base, size), size)

    own_c = seg(c * q1, q1)
    oth_c = seg((1 - c) * q1, q1)
    keep1 = (seg(c * q1 + xc * q2, q2), seg(c * q1 + yc * q2, q2))
    send1 = (seg(c * q1 + (1 - xc) * q2, q2), seg(c * q1 + (1 - yc) * q2, q2))
    r_keep = (seg(yc * q3, q3), seg(xc * q3, q3))
    r_send = (seg((1 - yc) * q3, q3), seg((1 - xc) * q3, q3))
    lanes = [slice(k * half, (k + 1) * half) for k in range(3)]
    dev1, dev2 = (dev_x, dev_y), (dev_y, dev_x)
    g_c = (c * q1, (1 - c) * q1)
    g_keep1 = (c * q1 + xc * q2, c * q1 + yc * q2)
    g_send1 = (c * q1 + (1 - xc) * q2, c * q1 + (1 - yc) * q2)
    g_fin = (g_keep1[0] + yc * q3, g_keep1[1] + xc * q3)
    g_fin_n = (g_keep1[0] + (1 - yc) * q3, g_keep1[1] + (1 - xc) * q3)

    def grows(j, off, size):
        return pl.ds(mo(base_of(j) + off, size), size)

    def ring(j):
        return lax.rem(j, RING)

    def d_copy(j):
        slot = lax.rem(j, P_SLOTS)
        return remote(part.at[slot, :, :, oth_c, :], dsum.at[slot], ds.at[ring(j)], dr.at[ring(j)], dev_c)

    def dd_copy(j):
        slot = lax.rem(j, L_SLOTS)
        return remote(part_d.at[slot, :, oth_c, :], dsum_d.at[slot], dds.at[ring(j)], ddr.at[ring(j)], dev_c)

    def p1_copy(j, r):
        return remote(part.at[lax.rem(j, P_SLOTS), r, :, send1[r], :], r1.at[j, r, 0:2],
                      p1s.at[r, ring(j)], p1r.at[r, ring(j)], dev1[r])

    def pd_copy(j, r):
        return remote(part_d.at[lax.rem(j, L_SLOTS), r, send1[r], :], r1.at[j, r, 2],
                      pds.at[r, ring(j)], pdr.at[r, ring(j)], dev1[r])

    def p2_copy(j, r):
        return remote(r1.at[j, r, :, r_send[r], :], r2.at[j, r], p2s.at[r, ring(j)], p2r.at[r, ring(j)], dev2[r])

    def g1_copy(j, r, off, lo):
        ref = gat.at[f_of(j), r, grows(j, off[r], q3), lo * half:]
        return remote(ref, ref, g1s.at[r, ring(j)], g1r.at[r, ring(j)], dev2[r])

    def g2_copy(j, r, off, lo):
        ref = gat.at[f_of(j), r, grows(j, off[r], q2), lo * half:]
        return remote(ref, ref, g2s.at[r, ring(j)], g2r.at[r, ring(j)], dev1[r])

    def gd_copy(j, off, lo):
        ref = gat.at[f_of(j), :, grows(j, off, q1), lo * half:]
        return remote(ref, ref, gds.at[ring(j)], gdr.at[ring(j)], dev_c)

    def a1_copy(r, off):
        ref = ga.at[r, seg(off[r], q3), :]
        return remote(ref, ref, a1s.at[r], a1r.at[r], dev2[r])

    def a2_copy(r, off):
        ref = ga.at[r, seg(off[r], q2), :]
        return remote(ref, ref, a2s.at[r], a2r.at[r], dev1[r])

    def ad_copy(off):
        ref = ga.at[:, seg(off, q1), :]
        return remote(ref, ref, ads.at[0], adr.at[0], dev_c)

    def by_arrays(j, body):
        @pl.when(j < held)
        def _():
            body(0)

        @pl.when(j >= held)
        def _():
            body(1)

    def each_held(body):
        def one(k, carry):
            body(k)
            return carry

        lax.fori_loop(0, HELD, one, 0)

    def da_dot(j):
        for r in range(2):
            part_d[lax.rem(j, L_SLOTS), r] = contract_cols(dya_ref[trows(j), :], wd[rcols(j, r), :])

    def da_product(j):
        da_dot(j)
        dd_copy(j).start()

    def da_pair_sum(j):
        dd_copy(j).wait_recv()
        slot = lax.rem(j, L_SLOTS)
        for r in range(2):
            part_d[slot, r, own_c, :] = part_d[slot, r, own_c, :] + dsum_d[slot, r]
            pd_copy(j, r).start()

    in_dy.wait()
    wcopy(2, 0).wait()
    da_dot(0)
    pl.semaphore_wait(barrier, 8)
    dd_copy(0).start()
    in_x.wait()
    x_own = x_ref[...].astype(jnp.float32)
    st[t] = pack_cols(jnp.sum(x_own, axis=1, keepdims=True), jnp.sum(x_own * x_own, axis=1, keepdims=True))
    send_stats(st, ss, sr)
    zdy = remote(dya_ref.at[own, :], dya_ref.at[own, :], zs.at[0], zr.at[0], dev_z)
    zdy.start()
    for i in range(1, 3):
        wcopy(2, i).wait()
        da_product(i)
    for i in range(LEAD):
        da_pair_sum(i)
        if i + 3 < LEAD:
            wcopy(2, i + 3).wait()
            da_product(i + 3)
    in_gain.wait()
    acc[...] = jnp.zeros_like(acc)

    gain = gain_ref[...]
    c0, c1 = total_stats(st, ss, sr)
    mean_x = c0 / d_model
    inv_std = lax.rsqrt(c1 / d_model - mean_x * mean_x + LN_EPS)
    xhat = (x_ref[...].astype(jnp.float32) - mean_x) * inv_std
    xh[...] = xhat
    h_ref[own, :] = (gain * xhat).astype(jnp.bfloat16)

    def h_copy(block):
        return remote(h_ref.at[own, :], h_ref.at[block, :], zs.at[1], zr.at[1], dev_z)

    h_copy(own).start()

    def m_part(f, rs, j):
        return sum(jnp.dot(gat[f, r, rs, lanes[0]], wd[rcols(j, r), :], preferred_element_type=jnp.float32) for r in range(2))

    z_sum = remote(acc.at[1], zin, zs.at[2], zr.at[2], dev_z)

    def step(i, carry):
        @pl.when(jnp.logical_and(i >= P_SLOTS, i < n_units + P_SLOTS))
        def _():
            j = i - P_SLOTS
            d_copy(j).wait_send()
            dd_copy(j).wait_send()
            for r in range(2):
                p1_copy(j, r).wait_send()
                pd_copy(j, r).wait_send()

        @pl.when(i < n_f)
        def _():
            wcopy(0, i).wait()
            wcopy(1, i).wait()

        @pl.when(i + LEAD < n_f)
        def _():
            wcopy(2, i + LEAD).wait()

        @pl.when(i == OWN_FIRST - LEAD)
        def _():
            remote(dya_ref.at[own, :], dya_ref.at[oth, :], zs.at[0], zr.at[0], dev_z).wait_recv()

        @pl.when(i == OWN_FIRST)
        def _():
            h_copy(oth).wait_recv()
            h_t[...] = h_ref[...].T

        @pl.when(i < n_units)
        def _():
            slot = lax.rem(i, P_SLOTS)
            h = h_ref[trows(i), :]
            for r in range(2):
                part[slot, r, 0] = jnp.dot(h, wg[:, rcols(i, r)], preferred_element_type=jnp.float32)
                part[slot, r, 1] = jnp.dot(h, wu[:, rcols(i, r)], preferred_element_type=jnp.float32)
            d_copy(i).start()

        @pl.when(i + LEAD < n_units)
        def _():
            da_product(i + LEAD)

        @pl.when(jnp.logical_and(i >= STAGES[0], i < n_units + STAGES[0]))
        def _():
            j = i - STAGES[0]
            d_copy(j).wait_recv()
            slot = lax.rem(j, P_SLOTS)
            for r in range(2):
                for k in range(2):
                    part[slot, r, k, own_c, :] = part[slot, r, k, own_c, :] + dsum[slot, r, k]
                p1_copy(j, r).start()

            @pl.when(j + LEAD < n_units)
            def _():
                da_pair_sum(j + LEAD)

        @pl.when(jnp.logical_and(i >= STAGES[1], i < n_units + STAGES[1]))
        def _():
            j = i - STAGES[1]
            slot = lax.rem(j, P_SLOTS)
            for r in range(2):
                pd_copy(j, r).wait_recv()
                p1_copy(j, r).wait_recv()
                for k in range(2):
                    r1[j, r, k] = r1[j, r, k] + part[slot, r, k, keep1[r], :]
                r1[j, r, 2] = r1[j, r, 2] + part_d[lax.rem(j, L_SLOTS), r, keep1[r], :]
                p2_copy(j, r).start()

        @pl.when(jnp.logical_and(i >= STAGES[2], i < n_units + STAGES[2]))
        def _():
            j = i - STAGES[2]
            for r in range(2):
                p2_copy(j, r).wait_recv()
                u = r1[j, r, 0, r_keep[r], :] + r2[j, r, 0]
                v = r1[j, r, 1, r_keep[r], :] + r2[j, r, 1]
                da = r1[j, r, 2, r_keep[r], :] + r2[j, r, 2]
                sig = jax.nn.sigmoid(u)
                swish = u * sig
                f = f_of(j)
                rs = grows(j, g_fin[r], q3)
                act = (swish * v).astype(jnp.bfloat16)

                @pl.when(j < held)
                def _():
                    gat[f, r, rs, lanes[0]] = act

                @pl.when(j >= held)
                def _():
                    ga[r, seg(g_fin[r], q3), pl.ds(mo((j - held) * half, half), half)] = act

                gat[f, r, rs, lanes[1]] = (da * v * sig * (1.0 + u * (1.0 - sig))).astype(jnp.bfloat16)
                gat[f, r, rs, lanes[2]] = (da * swish).astype(jnp.bfloat16)
            by_arrays(j, lambda lo: [g1_copy(j, r, g_fin, lo).start() for r in range(2)])

        @pl.when(jnp.logical_and(i >= STAGES[3], i < n_units + STAGES[3]))
        def _():
            j = i - STAGES[3]

            def forward(lo):
                for r in range(2):
                    g1_copy(j, r, g_fin_n, lo).wait_recv()
                    g2_copy(j, r, g_keep1, lo).start()

            by_arrays(j, forward)

        @pl.when(jnp.logical_and(i >= STAGES[4], i < n_units + STAGES[4]))
        def _():
            j = i - STAGES[4]

            def to_core(lo):
                for r in range(2):
                    g2_copy(j, r, g_send1, lo).wait_recv()
                gd_copy(j, g_c[0], lo).start()

            by_arrays(j, to_core)

        @pl.when(i >= STAGES[5])
        def _():
            j = i - STAGES[5]
            by_arrays(j, lambda lo: gd_copy(j, g_c[1], lo).wait_recv())
            f = f_of(j)
            rs = trows(j)
            side = oth_of(j)

            @pl.when(j < held)
            def _():
                acc[side, 0] += m_part(f, rs, j)

            acc[side, 1] += sum(contract_cols(gat[f, r, rs, lanes[1]], wg[:, rcols(j, r)])
                                + contract_cols(gat[f, r, rs, lanes[2]], wu[:, rcols(j, r)]) for r in range(2))

            def sent(lo):
                for r in range(2):
                    p2_copy(j, r).wait_send()
                    g1_copy(j, r, g_fin, lo).wait_send()
                    g2_copy(j, r, g_keep1, lo).wait_send()
                gd_copy(j, g_c[0], lo).wait_send()

            by_arrays(j, sent)

            @pl.when(j == last_oth)
            def _():
                z_sum.start()

        @pl.when(i == n_units - 1 + STAGES[2])
        def _():
            for r in range(2):
                a1_copy(r, g_fin).start()

        @pl.when(i == n_units - 1 + STAGES[3])
        def _():
            for r in range(2):
                a1_copy(r, g_fin_n).wait_recv()
                a2_copy(r, g_keep1).start()
        return carry

    lax.fori_loop(0, n_units + STAGES[5], step, 0)

    z_sum.wait()
    d_hnorm = acc[0, 1] + zin[1]
    e = d_hnorm * gain
    rb[t] = pack_cols(jnp.sum(e, axis=1, keepdims=True), jnp.sum(e * xh[...], axis=1, keepdims=True))
    send_stats(rb, bs, br)
    dgs[...] = jnp.broadcast_to(jnp.sum(d_hnorm * xh[...], axis=0, keepdims=True), dgs.shape)
    z_dg = remote(dgs, dgr, zs.at[3], zr.at[3], dev_z)
    z_dg.start()

    for r in range(2):
        a2_copy(r, g_send1).wait_recv()
    ad_copy(g_c[0]).start()
    for r in range(2):
        a1_copy(r, g_fin).wait_send()
        a2_copy(r, g_keep1).wait_send()
    ad_copy(g_c[1]).wait_recv()
    ad_copy(g_c[0]).wait_send()

    def m_product(k):
        j = held + k
        for r in range(2):
            act = ga[r, :, pl.ds(mo(k * half, half), half)]
            gat[f_of(j), r, own, lanes[0]] = act
            acc[0, 0] += jnp.dot(act, wd[rcols(j, r), :], preferred_element_type=jnp.float32)

    each_held(m_product)
    y_ref[...] = (x_ref[...].astype(jnp.float32) + (acc[0, 0] + zin[0])).astype(jnp.bfloat16)
    zdy.wait_send()
    h_copy(own).wait_send()
    c0, c1 = total_stats(rb, bs, br)
    dx_ln = inv_std * (e - c0 / d_model - xh[...] * (c1 / d_model))
    dx_ref[...] = (dya_ref[own, :].astype(jnp.float32) + dx_ln).astype(jnp.bfloat16)
    z_dg.wait()
    dg_ref[...] = dgs[0:1, :] + dgr[0:1, :]


def weight_grad_kernel(gat, h_t, dy_ref, y_in, dx_in, dg_in,
                       dwg_hbm, dwu_hbm, dwd_hbm, y_hbm, dx_hbm, dg_hbm, buf, bsem, ssem):
    n_blocks, _, _, width = gat.shape
    half = width // 3
    WB = 2 * half

    def out_copy(b, k):
        cs = pl.ds(mo(b * WB, WB), WB)
        dst = (dwg_hbm.at[:, cs], dwu_hbm.at[:, cs], dwd_hbm.at[cs, :])[k]
        slot = lax.rem(b, W_SLOTS)
        return pltpu.make_async_copy(buf.at[slot, k], dst, bsem.at[slot, k])

    def block(b, carry):
        slot = lax.rem(b, W_SLOTS)
        for k in range(3):
            @pl.when(b >= W_SLOTS)
            def _():
                out_copy(b - W_SLOTS, k).wait()

            for r in range(2):
                rs = slice(r * half, (r + 1) * half)
                src = gat[b, r, :, (k + 1) % 3 * half:((k + 1) % 3 + 1) * half]
                if k < 2:
                    buf[slot, k, :, rs] = jnp.dot(h_t[...], src, preferred_element_type=jnp.float32)
                else:
                    buf[slot, k, rs, :] = contract_rows(src, dy_ref[...])
            out_copy(b, k).start()
        return carry

    lax.fori_loop(0, n_blocks, block, 0)
    small = [pltpu.make_async_copy(src, dst, ssem.at[k])
             for k, (src, dst) in enumerate(((y_in, y_hbm), (dx_in, dx_hbm), (dg_in, dg_hbm)))]
    for d in small:
        d.start()

    def drain(b, carry):
        for k in range(3):
            out_copy(b, k).wait()
        return carry

    lax.fori_loop(n_blocks - W_SLOTS, n_blocks, drain, 0)
    for d in small:
        d.wait()


def solution(mesh):
    tx_size = mesh.shape["tx"]
    ty_size = mesh.shape["ty"]

    def local_step(x_blk, dy_blk, gain_blk, w_gate_blk, w_up_blk, w_down_blk):
        rows, dl = x_blk.shape
        fl = w_gate_blk.shape[1]
        tok = rows * ty_size
        d_model = dl * tx_size
        n = fl // FC
        half = FC // 2
        f32, bf16 = jnp.float32, jnp.bfloat16
        anyspec = pl.BlockSpec(memory_space=pl.ANY)
        sem = pltpu.SemaphoreType.DMA
        vm = pl.BlockSpec(memory_space=pltpu.VMEM)
        S = jax.ShapeDtypeStruct
        V = pltpu.VMEM
        small = [((rows, dl), bf16), ((rows, dl), bf16), ((1, dl), f32)]
        outs = pl.pallas_call(
            functools.partial(branch_kernel, d_model, n),
            out_shape=[V((n, 2, tok, 3 * half), bf16), V((dl, tok), bf16), V((tok, dl), bf16)] + [V(*s) for s in small],
            in_specs=[anyspec] * 6,
            out_specs=[vm] * 6,
            scratch_shapes=[
                V((rows, dl), bf16), V((1, dl), f32), V((tok, dl), bf16),
                V((dl, fl), bf16), V((dl, fl), bf16), V((fl, dl), bf16),
                V((rows, dl), f32),
                V((P_SLOTS, 2, 2, rows, half), f32), V((L_SLOTS, 2, rows, half), f32),
                V((P_SLOTS, 2, 2, rows // 2, half), f32), V((L_SLOTS, 2, rows // 2, half), f32),
                V((2 * n, 2, 3, rows // 4, half), f32), V((2 * n, 2, 3, rows // 8, half), f32),
                V((2, rows, HELD * half), bf16),
                V((2, 2, rows, dl), f32), V((2, rows, dl), f32),
                V((8, 8, 128), f32), V((8, 8, 128), f32), V((8, dl), f32), V((8, dl), f32),
                sem((3, n)), sem((3,)), sem((4,)), sem((4,)), sem((8,)), sem((8,)), sem((8,)), sem((8,)),
                sem((RING,)), sem((RING,)), sem((RING,)), sem((RING,)),
                *[sem((2, RING)) for _ in range(10)],
                sem((RING,)), sem((RING,)),
                *[sem((2,)) for _ in range(4)], sem((1,)), sem((1,)),
            ],
            compiler_params=pltpu.CompilerParams(collective_id=0, has_side_effects=True, vmem_limit_bytes=VMEM_LIMIT),
            cost_estimate=pl.CostEstimate(flops=12 * tok * dl * fl, bytes_accessed=6 * dl * fl + 6 * tok * fl, transcendentals=0),
        )(x_blk, dy_blk, gain_blk[None, :], w_gate_blk, w_up_blk, w_down_blk)

        dwg, dwu, dwd, y_blk, dx_blk, dg = pl.pallas_call(
            weight_grad_kernel,
            out_shape=[S((dl, fl), f32)] * 2 + [S((fl, dl), f32)] + [S(*s) for s in small],
            in_specs=[vm] * 6,
            out_specs=[anyspec] * 6,
            scratch_shapes=[
                V((W_SLOTS, 3, dl, FC), f32), sem((W_SLOTS, 3)), sem((3,)),
            ],
            compiler_params=pltpu.CompilerParams(vmem_limit_bytes=VMEM_LIMIT),
            cost_estimate=pl.CostEstimate(flops=6 * tok * dl * fl, bytes_accessed=12 * dl * fl + 6 * tok * fl, transcendentals=0),
        )(*[pltpu.with_memory_space_constraint(o, pltpu.VMEM) for o in outs])
        return (y_blk, dx_blk, dwg, dwu, dwd, dg[0])

    return jax.shard_map(
        local_step, mesh=mesh,
        in_specs=(P("ty", "tx"), P("ty", "tx"), P("tx"), P("tx", "ty"), P("tx", "ty"), P("ty", "tx")),
        out_specs=(P("ty", "tx"), P("ty", "tx"), P("tx", "ty"), P("tx", "ty"), P("ty", "tx"), P("tx")),
        check_vma=False)
```

```python
import functools

import jax
import jax.numpy as jnp
from jax import lax
from jax.experimental import pallas as pl
from jax.experimental.pallas import tpu as pltpu
from jax.sharding import PartitionSpec as P

LN_EPS = 1e-6
MESH = pl.DeviceIdType.MESH
FC = 512
OWN_FIRST = 8
LEAD = 8
P_SLOTS = 4
L_SLOTS = LEAD + P_SLOTS
HELD = 6
RING = 16
STAGES = (1, 3, 5, 7, 9, 10)
WB = 512
W_SLOTS = 4
VMEM_LIMIT = 48 * 1024 * 1024


def contract_rows(left_op, right_op):
    return lax.dot_general(left_op, right_op, (((0,), (0,)), ((), ())), preferred_element_type=jnp.float32)


def contract_cols(left_op, right_op):
    return lax.dot_general(left_op, right_op, (((1,), (1,)), ((), ())), preferred_element_type=jnp.float32)


def mo(value, multiple):
    return pl.multiple_of(value, multiple)


def branch_kernel(d_model, n_f,
                  x_hbm, dy_hbm, gain_hbm, wg_hbm, wu_hbm, wd_hbm,
                  gat, h_t, dya_ref, y_ref, dx_ref, dg_ref,
                  x_ref, gain_ref, h_ref,
                  wg, wu, wd, xh, part, part_d, dsum, dsum_d, r1, r2, acc, zin, st, rb, dgs, dgr,
                  wsem, isem, zs, zr, ss, sr, bs, br, ds, dr, dds, ddr, p1s, p1r, pds, pdr, p2s, p2r,
                  g1s, g1r, g2s, g2r, gds, gdr, a1s, a1r, a2s, a2r, ads, adr):
    half = FC // 2
    rows = x_ref.shape[0]
    q1, q2, q3 = rows // 2, rows // 4, rows // 8
    n_units = 2 * n_f
    last_oth = OWN_FIRST + n_f - 1
    held = n_units - HELD

    ty = lax.axis_index("ty")
    t = lax.axis_index("tx")
    c = lax.rem(t, 2)
    xc = lax.rem(lax.div(t, 2), 2)
    yc = lax.div(t, 4)
    dev_c = (ty, t + 1 - 2 * c)
    dev_x = (ty, t + 2 - 4 * xc)
    dev_y = (ty, t + 4 - 8 * yc)
    dev_z = (1 - ty, t)
    own = pl.ds(mo(ty * rows, rows), rows)
    oth = pl.ds(mo((1 - ty) * rows, rows), rows)

    def remote(src, dst, ssem, rsem, dev):
        return pltpu.make_async_remote_copy(src_ref=src, dst_ref=dst, send_sem=ssem, recv_sem=rsem,
                                            device_id=dev, device_id_type=MESH)

    def f_of(j):
        return lax.rem(j + (n_f - OWN_FIRST), n_f)

    def oth_of(j):
        return lax.rem(lax.div(j + (n_f - OWN_FIRST), n_f), 2)

    def base_of(j):
        k = oth_of(j)
        return (ty + k - 2 * ty * k) * rows

    def fcols(j):
        return pl.ds(mo(f_of(j) * FC, FC), FC)

    def trows(j):
        return pl.ds(mo(base_of(j), rows), rows)

    def wcopy(k, i):
        cs = fcols(i)
        if k == 0:
            return pltpu.make_async_copy(wg_hbm.at[:, cs], wg.at[:, cs], wsem.at[0, i])
        if k == 1:
            return pltpu.make_async_copy(wu_hbm.at[:, cs], wu.at[:, cs], wsem.at[1, i])
        return pltpu.make_async_copy(wd_hbm.at[cs, :], wd.at[cs, :], wsem.at[2, i])

    in_dy = pltpu.make_async_copy(dy_hbm, dya_ref.at[own, :], isem.at[0])
    in_x = pltpu.make_async_copy(x_hbm, x_ref, isem.at[1])
    in_gain = pltpu.make_async_copy(gain_hbm, gain_ref, isem.at[2])
    in_x.start()
    in_dy.start()
    in_gain.start()
    for i in range(LEAD):
        wcopy(2, i).start()

    barrier = pltpu.get_barrier_semaphore()
    for o in range(1, 8):
        pl.semaphore_signal(barrier, inc=1, device_id=(ty, lax.rem(t + o, 8)), device_id_type=MESH)
    pl.semaphore_signal(barrier, inc=1, device_id=dev_z, device_id_type=MESH)

    def start_w(i, carry):
        wcopy(0, i).start()
        wcopy(1, i).start()

        @pl.when(i + LEAD < n_f)
        def _():
            wcopy(2, i + LEAD).start()
        return carry

    lax.fori_loop(0, n_f, start_w, 0)

    lane = lax.broadcasted_iota(jnp.int32, (rows, 128), 1)

    def pack_cols(c0, c1):
        both = jnp.where(lane == 0, c0, jnp.where(lane == 1, c1, 0.0))
        return both.T[0:8, :]

    def unpack_cols(packed):
        full = jnp.concatenate([packed, jnp.zeros((rows - 8, 128), jnp.float32)], axis=0).T
        return full[:, 0:1], full[:, 1:2]

    def send_stats(buf, ssem, rsem):
        for o in range(1, 8):
            remote(buf.at[t], buf.at[t], ssem.at[o], rsem.at[o], (ty, lax.rem(t + o, 8))).start()

    def total_stats(buf, ssem, rsem):
        for o in range(1, 8):
            q = lax.rem(t + 8 - o, 8)
            d = remote(buf.at[t], buf.at[q], ssem.at[o], rsem.at[o], (ty, q))
            d.wait_send()
            d.wait_recv()
        s = buf[0]
        for j in range(1, 8):
            s = s + buf[j]
        return unpack_cols(s)

    def seg(base, size):
        return pl.ds(mo(base, size), size)

    own_c = seg(c * q1, q1)
    oth_c = seg((1 - c) * q1, q1)
    keep1 = (seg(c * q1 + xc * q2, q2), seg(c * q1 + yc * q2, q2))
    send1 = (seg(c * q1 + (1 - xc) * q2, q2), seg(c * q1 + (1 - yc) * q2, q2))
    r_keep = (seg(yc * q3, q3), seg(xc * q3, q3))
    r_send = (seg((1 - yc) * q3, q3), seg((1 - xc) * q3, q3))
    colw = (slice(0, half), slice(half, FC))
    dev1, dev2 = (dev_x, dev_y), (dev_y, dev_x)
    g_c = (c * q1, (1 - c) * q1)
    g_keep1 = (c * q1 + xc * q2, c * q1 + yc * q2)
    g_send1 = (c * q1 + (1 - xc) * q2, c * q1 + (1 - yc) * q2)
    g_fin = (g_keep1[0] + yc * q3, g_keep1[1] + xc * q3)
    g_fin_n = (g_keep1[0] + (1 - yc) * q3, g_keep1[1] + (1 - xc) * q3)

    def gcols(j, r):
        return pl.ds(mo(f_of(j) * FC + r * half, half), half)

    def grows(j, off, size):
        return pl.ds(mo(base_of(j) + off, size), size)

    def ring(j):
        return lax.rem(j, RING)

    def d_copy(j):
        slot = lax.rem(j, P_SLOTS)
        return remote(part.at[slot, :, oth_c, :], dsum.at[slot], ds.at[ring(j)], dr.at[ring(j)], dev_c)

    def dd_copy(j):
        slot = lax.rem(j, L_SLOTS)
        return remote(part_d.at[slot, oth_c, :], dsum_d.at[slot], dds.at[ring(j)], ddr.at[ring(j)], dev_c)

    def p1_copy(j, r):
        return remote(part.at[lax.rem(j, P_SLOTS), :, send1[r], colw[r]], r1.at[j, r, 0:2],
                      p1s.at[r, ring(j)], p1r.at[r, ring(j)], dev1[r])

    def pd_copy(j, r):
        return remote(part_d.at[lax.rem(j, L_SLOTS), send1[r], colw[r]], r1.at[j, r, 2],
                      pds.at[r, ring(j)], pdr.at[r, ring(j)], dev1[r])

    def p2_copy(j, r):
        return remote(r1.at[j, r, :, r_send[r], :], r2.at[j, r], p2s.at[r, ring(j)], p2r.at[r, ring(j)], dev2[r])

    def g1_copy(j, r, off, lo):
        ref = gat.at[lo:3, grows(j, off[r], q3), gcols(j, r)]
        return remote(ref, ref, g1s.at[r, ring(j)], g1r.at[r, ring(j)], dev2[r])

    def g2_copy(j, r, off, lo):
        ref = gat.at[lo:3, grows(j, off[r], q2), gcols(j, r)]
        return remote(ref, ref, g2s.at[r, ring(j)], g2r.at[r, ring(j)], dev1[r])

    def gd_copy(j, off, lo):
        ref = gat.at[lo:3, grows(j, off, q1), fcols(j)]
        return remote(ref, ref, gds.at[ring(j)], gdr.at[ring(j)], dev_c)

    def a1_copy(k, r, off):
        ref = gat.at[0, grows(held + k, off[r], q3), gcols(held + k, r)]
        return remote(ref, ref, a1s.at[r, k], a1r.at[r, k], dev2[r])

    def a2_copy(k, r, off):
        ref = gat.at[0, grows(held + k, off[r], q2), gcols(held + k, r)]
        return remote(ref, ref, a2s.at[r, k], a2r.at[r, k], dev1[r])

    def ad_copy(k, off):
        ref = gat.at[0, grows(held + k, off, q1), fcols(held + k)]
        return remote(ref, ref, ads.at[k], adr.at[k], dev_c)

    def by_arrays(j, body):
        @pl.when(j < held)
        def _():
            body(0)

        @pl.when(j >= held)
        def _():
            body(1)

    def each_held(body):
        def one(k, carry):
            body(k)
            return carry

        lax.fori_loop(0, HELD, one, 0)

    def da_dot(j):
        part_d[lax.rem(j, L_SLOTS)] = contract_cols(dya_ref[trows(j), :], wd[fcols(j), :])

    def da_product(j):
        da_dot(j)
        dd_copy(j).start()

    def da_pair_sum(j):
        dd_copy(j).wait_recv()
        slot = lax.rem(j, L_SLOTS)
        part_d[slot, own_c, :] = part_d[slot, own_c, :] + dsum_d[slot]
        for r in range(2):
            pd_copy(j, r).start()

    in_dy.wait()
    wcopy(2, 0).wait()
    da_dot(0)
    pl.semaphore_wait(barrier, 8)
    dd_copy(0).start()
    in_x.wait()
    x_own = x_ref[...].astype(jnp.float32)
    st[t] = pack_cols(jnp.sum(x_own, axis=1, keepdims=True), jnp.sum(x_own * x_own, axis=1, keepdims=True))
    send_stats(st, ss, sr)
    zdy = remote(dya_ref.at[own, :], dya_ref.at[own, :], zs.at[0], zr.at[0], dev_z)
    zdy.start()
    for i in range(1, 3):
        wcopy(2, i).wait()
        da_product(i)
    for i in range(LEAD):
        da_pair_sum(i)
        if i + 3 < LEAD:
            wcopy(2, i + 3).wait()
            da_product(i + 3)
    in_gain.wait()
    acc[...] = jnp.zeros_like(acc)

    gain = gain_ref[...]
    c0, c1 = total_stats(st, ss, sr)
    mean_x = c0 / d_model
    inv_std = lax.rsqrt(c1 / d_model - mean_x * mean_x + LN_EPS)
    xhat = (x_ref[...].astype(jnp.float32) - mean_x) * inv_std
    xh[...] = xhat
    h_ref[own, :] = (gain * xhat).astype(jnp.bfloat16)

    def h_copy(block):
        return remote(h_ref.at[own, :], h_ref.at[block, :], zs.at[1], zr.at[1], dev_z)

    h_copy(own).start()

    z_sum = remote(acc.at[1], zin, zs.at[2], zr.at[2], dev_z)

    def step(i, carry):
        @pl.when(jnp.logical_and(i >= P_SLOTS, i < n_units + P_SLOTS))
        def _():
            j = i - P_SLOTS
            d_copy(j).wait_send()
            dd_copy(j).wait_send()
            for r in range(2):
                p1_copy(j, r).wait_send()
                pd_copy(j, r).wait_send()

        @pl.when(i < n_f)
        def _():
            wcopy(0, i).wait()
            wcopy(1, i).wait()

        @pl.when(i + LEAD < n_f)
        def _():
            wcopy(2, i + LEAD).wait()

        @pl.when(i == OWN_FIRST - LEAD)
        def _():
            remote(dya_ref.at[own, :], dya_ref.at[oth, :], zs.at[0], zr.at[0], dev_z).wait_recv()

        @pl.when(i == OWN_FIRST)
        def _():
            h_copy(oth).wait_recv()
            h_t[...] = h_ref[...].T

        @pl.when(i < n_units)
        def _():
            cs = fcols(i)
            slot = lax.rem(i, P_SLOTS)
            h = h_ref[trows(i), :]
            part[slot, 0] = jnp.dot(h, wg[:, cs], preferred_element_type=jnp.float32)
            part[slot, 1] = jnp.dot(h, wu[:, cs], preferred_element_type=jnp.float32)
            d_copy(i).start()

        @pl.when(i + LEAD < n_units)
        def _():
            da_product(i + LEAD)

        @pl.when(jnp.logical_and(i >= STAGES[0], i < n_units + STAGES[0]))
        def _():
            j = i - STAGES[0]
            d_copy(j).wait_recv()
            slot = lax.rem(j, P_SLOTS)
            for k in range(2):
                part[slot, k, own_c, :] = part[slot, k, own_c, :] + dsum[slot, k]
            for r in range(2):
                p1_copy(j, r).start()

            @pl.when(j + LEAD < n_units)
            def _():
                da_pair_sum(j + LEAD)

        @pl.when(jnp.logical_and(i >= STAGES[1], i < n_units + STAGES[1]))
        def _():
            j = i - STAGES[1]
            slot = lax.rem(j, P_SLOTS)
            for r in range(2):
                pd_copy(j, r).wait_recv()
                p1_copy(j, r).wait_recv()
                for k in range(2):
                    r1[j, r, k] = r1[j, r, k] + part[slot, k, keep1[r], colw[r]]
                r1[j, r, 2] = r1[j, r, 2] + part_d[lax.rem(j, L_SLOTS), keep1[r], colw[r]]
                p2_copy(j, r).start()

        @pl.when(jnp.logical_and(i >= STAGES[2], i < n_units + STAGES[2]))
        def _():
            j = i - STAGES[2]
            for r in range(2):
                p2_copy(j, r).wait_recv()
                u = r1[j, r, 0, r_keep[r], :] + r2[j, r, 0]
                v = r1[j, r, 1, r_keep[r], :] + r2[j, r, 1]
                da = r1[j, r, 2, r_keep[r], :] + r2[j, r, 2]
                sig = jax.nn.sigmoid(u)
                swish = u * sig
                cs = gcols(j, r)
                rs = grows(j, g_fin[r], q3)
                gat[0, rs, cs] = (swish * v).astype(jnp.bfloat16)
                gat[1, rs, cs] = (da * v * sig * (1.0 + u * (1.0 - sig))).astype(jnp.bfloat16)
                gat[2, rs, cs] = (da * swish).astype(jnp.bfloat16)
            by_arrays(j, lambda lo: [g1_copy(j, r, g_fin, lo).start() for r in range(2)])

        @pl.when(jnp.logical_and(i >= STAGES[3], i < n_units + STAGES[3]))
        def _():
            j = i - STAGES[3]

            def forward(lo):
                for r in range(2):
                    g1_copy(j, r, g_fin_n, lo).wait_recv()
                    g2_copy(j, r, g_keep1, lo).start()

            by_arrays(j, forward)

        @pl.when(jnp.logical_and(i >= STAGES[4], i < n_units + STAGES[4]))
        def _():
            j = i - STAGES[4]

            def to_core(lo):
                for r in range(2):
                    g2_copy(j, r, g_send1, lo).wait_recv()
                gd_copy(j, g_c[0], lo).start()

            by_arrays(j, to_core)

        @pl.when(i >= STAGES[5])
        def _():
            j = i - STAGES[5]
            by_arrays(j, lambda lo: gd_copy(j, g_c[1], lo).wait_recv())
            cs = fcols(j)
            rs = trows(j)
            side = oth_of(j)

            @pl.when(j < held)
            def _():
                acc[side, 0] += jnp.dot(gat[0, rs, cs], wd[cs, :], preferred_element_type=jnp.float32)

            acc[side, 1] += contract_cols(gat[1, rs, cs], wg[:, cs]) + contract_cols(gat[2, rs, cs], wu[:, cs])

            def sent(lo):
                for r in range(2):
                    p2_copy(j, r).wait_send()
                    g1_copy(j, r, g_fin, lo).wait_send()
                    g2_copy(j, r, g_keep1, lo).wait_send()
                gd_copy(j, g_c[0], lo).wait_send()

            by_arrays(j, sent)

            @pl.when(j == last_oth)
            def _():
                z_sum.start()

        @pl.when(i == n_units - 1 + STAGES[2])
        def _():
            each_held(lambda k: [a1_copy(k, r, g_fin).start() for r in range(2)])

        @pl.when(i == n_units - 1 + STAGES[3])
        def _():
            def forward(k):
                for r in range(2):
                    a1_copy(k, r, g_fin_n).wait_recv()
                    a2_copy(k, r, g_keep1).start()

            each_held(forward)
        return carry

    lax.fori_loop(0, n_units + STAGES[5], step, 0)

    z_sum.wait()
    d_hnorm = acc[0, 1] + zin[1]
    e = d_hnorm * gain
    rb[t] = pack_cols(jnp.sum(e, axis=1, keepdims=True), jnp.sum(e * xh[...], axis=1, keepdims=True))
    send_stats(rb, bs, br)
    dgs[...] = jnp.broadcast_to(jnp.sum(d_hnorm * xh[...], axis=0, keepdims=True), dgs.shape)
    z_dg = remote(dgs, dgr, zs.at[3], zr.at[3], dev_z)
    z_dg.start()

    def to_core(k):
        for r in range(2):
            a2_copy(k, r, g_send1).wait_recv()
        ad_copy(k, g_c[0]).start()

    each_held(to_core)

    def m_product(k):
        ad_copy(k, g_c[1]).wait_recv()
        cs = fcols(held + k)
        acc[0, 0] += jnp.dot(gat[0, own, cs], wd[cs, :], preferred_element_type=jnp.float32)
        for r in range(2):
            a1_copy(k, r, g_fin).wait_send()
            a2_copy(k, r, g_keep1).wait_send()
        ad_copy(k, g_c[0]).wait_send()

    each_held(m_product)
    y_ref[...] = (x_ref[...].astype(jnp.float32) + (acc[0, 0] + zin[0])).astype(jnp.bfloat16)
    zdy.wait_send()
    h_copy(own).wait_send()
    c0, c1 = total_stats(rb, bs, br)
    dx_ln = inv_std * (e - c0 / d_model - xh[...] * (c1 / d_model))
    dx_ref[...] = (dya_ref[own, :].astype(jnp.float32) + dx_ln).astype(jnp.bfloat16)
    z_dg.wait()
    dg_ref[...] = dgs[0:1, :] + dgr[0:1, :]


def weight_grad_kernel(gat, h_t, dy_ref, y_in, dx_in, dg_in,
                       dwg_hbm, dwu_hbm, dwd_hbm, y_hbm, dx_hbm, dg_hbm, buf, bsem, ssem):
    n_blocks = gat.shape[2] // WB

    def out_copy(b, k):
        cs = pl.ds(mo(b * WB, WB), WB)
        dst = (dwg_hbm.at[:, cs], dwu_hbm.at[:, cs], dwd_hbm.at[cs, :])[k]
        slot = lax.rem(b, W_SLOTS)
        return pltpu.make_async_copy(buf.at[slot, k], dst, bsem.at[slot, k])

    def block(b, carry):
        cs = pl.ds(mo(b * WB, WB), WB)
        slot = lax.rem(b, W_SLOTS)
        for k in range(3):
            @pl.when(b >= W_SLOTS)
            def _():
                out_copy(b - W_SLOTS, k).wait()

            if k < 2:
                buf[slot, k] = jnp.dot(h_t[...], gat[k + 1, :, cs], preferred_element_type=jnp.float32)
            else:
                buf[slot, k] = contract_rows(gat[0, :, cs], dy_ref[...])
            out_copy(b, k).start()
        return carry

    lax.fori_loop(0, n_blocks, block, 0)
    small = [pltpu.make_async_copy(src, dst, ssem.at[k])
             for k, (src, dst) in enumerate(((y_in, y_hbm), (dx_in, dx_hbm), (dg_in, dg_hbm)))]
    for d in small:
        d.start()

    def drain(b, carry):
        for k in range(3):
            out_copy(b, k).wait()
        return carry

    lax.fori_loop(n_blocks - W_SLOTS, n_blocks, drain, 0)
    for d in small:
        d.wait()


def solution(mesh):
    tx_size = mesh.shape["tx"]
    ty_size = mesh.shape["ty"]

    def local_step(x_blk, dy_blk, gain_blk, w_gate_blk, w_up_blk, w_down_blk):
        rows, dl = x_blk.shape
        fl = w_gate_blk.shape[1]
        tok = rows * ty_size
        d_model = dl * tx_size
        n = fl // FC
        half = FC // 2
        f32, bf16 = jnp.float32, jnp.bfloat16
        anyspec = pl.BlockSpec(memory_space=pl.ANY)
        sem = pltpu.SemaphoreType.DMA
        vm = pl.BlockSpec(memory_space=pltpu.VMEM)
        S = jax.ShapeDtypeStruct
        V = pltpu.VMEM
        small = [((rows, dl), bf16), ((rows, dl), bf16), ((1, dl), f32)]
        outs = pl.pallas_call(
            functools.partial(branch_kernel, d_model, n),
            out_shape=[V((3, tok, fl), bf16), V((dl, tok), bf16), V((tok, dl), bf16)] + [V(*s) for s in small],
            in_specs=[anyspec] * 6,
            out_specs=[vm] * 6,
            scratch_shapes=[
                V((rows, dl), bf16), V((1, dl), f32), V((tok, dl), bf16),
                V((dl, fl), bf16), V((dl, fl), bf16), V((fl, dl), bf16),
                V((rows, dl), f32),
                V((P_SLOTS, 2, rows, FC), f32), V((L_SLOTS, rows, FC), f32),
                V((P_SLOTS, 2, rows // 2, FC), f32), V((L_SLOTS, rows // 2, FC), f32),
                V((2 * n, 2, 3, rows // 4, half), f32), V((2 * n, 2, 3, rows // 8, half), f32),
                V((2, 2, rows, dl), f32), V((2, rows, dl), f32),
                V((8, 8, 128), f32), V((8, 8, 128), f32), V((8, dl), f32), V((8, dl), f32),
                sem((3, n)), sem((3,)), sem((4,)), sem((4,)), sem((8,)), sem((8,)), sem((8,)), sem((8,)),
                sem((RING,)), sem((RING,)), sem((RING,)), sem((RING,)),
                *[sem((2, RING)) for _ in range(10)],
                sem((RING,)), sem((RING,)),
                *[sem((2, HELD)) for _ in range(4)], sem((HELD,)), sem((HELD,)),
            ],
            compiler_params=pltpu.CompilerParams(collective_id=0, has_side_effects=True, vmem_limit_bytes=VMEM_LIMIT),
            cost_estimate=pl.CostEstimate(flops=12 * tok * dl * fl, bytes_accessed=6 * dl * fl + 6 * tok * fl, transcendentals=0),
        )(x_blk, dy_blk, gain_blk[None, :], w_gate_blk, w_up_blk, w_down_blk)

        dwg, dwu, dwd, y_blk, dx_blk, dg = pl.pallas_call(
            weight_grad_kernel,
            out_shape=[S((dl, fl), f32)] * 2 + [S((fl, dl), f32)] + [S(*s) for s in small],
            in_specs=[vm] * 6,
            out_specs=[anyspec] * 6,
            scratch_shapes=[
                V((W_SLOTS, 3, dl, WB), f32), sem((W_SLOTS, 3)), sem((3,)),
            ],
            compiler_params=pltpu.CompilerParams(vmem_limit_bytes=VMEM_LIMIT),
            cost_estimate=pl.CostEstimate(flops=6 * tok * dl * fl, bytes_accessed=12 * dl * fl + 6 * tok * fl, transcendentals=0),
        )(*[pltpu.with_memory_space_constraint(o, pltpu.VMEM) for o in outs])
        return (y_blk, dx_blk, dwg, dwu, dwd, dg[0])

    return jax.shard_map(
        local_step, mesh=mesh,
        in_specs=(P("ty", "tx"), P("ty", "tx"), P("tx"), P("tx", "ty"), P("tx", "ty"), P("ty", "tx")),
        out_specs=(P("ty", "tx"), P("ty", "tx"), P("tx", "ty"), P("tx", "ty"), P("ty", "tx"), P("tx")),
        check_vma=False)
```
